32 devices in a mesh: expert: 8 (over z, y), shard: 4 (over x, core).
Axes of the slice: x: 2, y: 2, z: 4, core: 2. Of those that a mesh axis runs over, the one named last changes fastest.
Arguments:
- tokens: bfloat16 [4096, 2048], P(('expert', 'shard')), may hold values from -6 to 6
- gain_attn: float32 [2048], replicated, may hold values from 0.1 to 1.9
- w_qkv: bfloat16 [3, 2048, 2048], P(None, 'expert', 'shard'), may hold values from -0.125 to 0.125
- b_qkv: float32 [3, 2048], P(None, 'shard'), may hold values from -9 to 9, as said below
- w_out: bfloat16 [2048, 2048], P('shard', 'expert'), may hold values from -0.5 to 0.5
- gain_ffn: float32 [2048], replicated, may hold values from 0.1 to 1.9
- w_router: bfloat16 [2048, 32], replicated, may hold values from -0.125 to 0.125
- shared_gate: float32 [2048], replicated, may hold values from -0.125 to 0.125
- w_shared_gu: bfloat16 [2, 2048, 5632], P(None, 'expert', 'shard'), may hold values from -0.125 to 0.125
- w_shared_down: bfloat16 [5632, 2048], P('shard', 'expert'), may hold values from -0.078125 to 0.078125
- w_expert_gu: bfloat16 [32, 2, 2048, 1408], P(('expert', 'shard')), may hold values from -0.125 to 0.125
- w_expert_down: bfloat16 [32, 1408, 2048], P(('expert', 'shard')), may hold values from -1.25 to 1.25
- routes: int32 [4096, 4], P(('expert', 'shard')), may hold values from 0 to 31, all different within a row; in each aligned block of 128 rows (0 to 127, 128 to 255, ...) at most 32 rows name the same one
- grad_out: bfloat16 [4096, 2048], P(('expert', 'shard')), may hold values from -6 to 6
Outputs:
- result: bfloat16 [4096, 2048], P(('expert', 'shard'))
- grad_tokens: float32 [4096, 2048], P(('expert', 'shard'))
- grad_gain_attn: float32 [2048], replicated
- grad_w_qkv: float32 [3, 2048, 2048], P(None, 'expert', 'shard')
- grad_b_qkv: float32 [3, 2048], replicated
- grad_w_out: float32 [2048, 2048], P('shard', 'expert')
- grad_gain_ffn: float32 [2048], replicated
- grad_w_router: float32 [2048, 32], replicated
- grad_shared_gate: float32 [2048], replicated
- grad_w_shared_gu: float32 [2, 2048, 5632], P(None, 'expert', 'shard')
- grad_w_shared_down: float32 [5632, 2048], P('shard', 'expert')
- grad_w_expert_gu: float32 [32, 2, 2048, 1408], P(('expert', 'shard'))
- grad_w_expert_down: float32 [32, 1408, 2048], P(('expert', 'shard'))
The draws below stay inside these ranges and needn't reach their ends.
Inputs may be any that keep to these rules, and one draw needn't show every extreme that they name: `routes`: each row names 4 different experts; among the rows of one device no expert is named more than 32 times, a bound that some block reaches. `b_qkv`: biases of the queries, keys and values.
All inputs are finite; a program needn't handle non-finite values.
Results may differ from the reference program's by a relative error of at most 0.018.
The reference program's roundings to bfloat16 on the way count: a program that leaves them out, or rounds other values in their place, can miss the bound.
Values may be sent and summed in bfloat16 or wider, within the bound.
A program may use at most 384 MiB of HBM per device.

```python
import math
import jax
import jax.numpy as jnp
import numpy as np
from jax import lax

D = 2048
HEADS = 16
HEAD_DIM = 128
FF = 1408
SFF = 5632
TOPK = 4
TOK_DEV = 128
SEQ = 512
TOKENS = 4096
EXPERTS = 32
CAP = 32
DEVICES = 32


def draw_b_qkv(key, part):
    first_key = jax.random.fold_in(key, 0)
    base_bias = jnp.clip(jax.random.normal(first_key, (3, D), jnp.float32) * 0.5, -3.0, 3.0)
    return base_bias


def raised(values, own_key, source, target, parts, factor):
    def block_of(dim):
        return (jnp.arange(values.shape[dim]) // (values.shape[dim] // parts)).reshape((-1,) + (1,) * (values.ndim - 1 - dim))

    one_side = jax.random.permutation(own_key, parts)[block_of(target)]
    far = (block_of(target) + parts // 2) % parts
    return jnp.where((block_of(source) == one_side) | (block_of(source) == far), factor * values, values)


def levels(key, extent, pieces, least, top_value):
    loudness = 1.0
    for axis_at, parts in pieces:
        draws = jax.random.uniform(jax.random.fold_in(jax.random.fold_in(key, 6), axis_at), (parts,), jnp.float32, least / len(pieces), top_value / len(pieces))
        loudness = loudness * jnp.repeat(jnp.exp(draws), extent[axis_at] // parts).reshape((-1,) + (1,) * (len(extent) - 1 - axis_at))
    return loudness


def deal_out(key, own, number, rows, amount, top, reach, lean):
    ranking = jax.random.permutation(key, amount)
    crowded, usual = load_shares(amount, rows * top, reach, lean, True), load_shares(amount, rows * top, reach, lean, False)
    places = jnp.arange(amount)

    def named(lengths, rotation):
        used = int((lengths > 0).sum())
        fixed = max(1, used // 4)
        passed = fixed + (places - fixed + rotation * (used - fixed)) % max(1, amount - fixed)
        return jnp.zeros((amount,), jnp.int32).at[ranking[jnp.where(places < fixed, places, passed)]].set(jnp.asarray(lengths, jnp.int32))

    lengths = jnp.where(number % 4 == 0, named(crowded, number // 4), named(usual, number - number // 4 - 1))
    mixed = jax.random.permutation(jax.random.fold_in(own, 3), amount)
    source_of, taker = mixed[0:amount // 2 * 2:2], mixed[1:amount // 2 * 2:2]
    slack = jnp.minimum(lengths[source_of] - 1, reach - lengths[taker]) // 2
    slack = jnp.where((source_of == ranking[0]) | (taker == ranking[0]) | (lengths[taker] == 0), 0, jnp.maximum(slack, 0))
    passed = jax.random.randint(jax.random.fold_in(own, 4), (amount // 2,), 0, 1 << 20) % (slack + 1)
    lengths = lengths.at[source_of].add(-passed).at[taker].add(passed)
    members = jnp.searchsorted(jnp.cumsum(lengths), jnp.arange(rows * top), side="right").astype(jnp.int32)
    listing = members.reshape(top, rows).T
    listing = listing[jax.random.permutation(jax.random.fold_in(own, 1), rows)]
    rotation = jax.random.randint(jax.random.fold_in(own, 2), (rows, 1), 0, top)
    return jnp.take_along_axis(listing, (jnp.arange(top)[None, :] + rotation) % top, axis=1)


def load_shares(count, total, bound, skew, full):
    portions = [(1 << 20) // math.isqrt(grade ** skew) + 1 for grade in range(1, count + 1)]
    largest = bound if full else min(bound, max(-(-total // count), total * portions[0] // sum(portions)))
    least = 1 if total - largest >= count - 1 else 0
    counts, surplus = [largest] + [least] * (count - 1), total - largest - least * (count - 1)
    while surplus > 0:
        free = [i for i in range(1, count) if counts[i] < largest] or [i for i in range(1, count) if counts[i] < bound]
        whole, remaining = sum([portions[i] for i in free]), surplus
        for i in free:
            addition = min(bound - counts[i], max(1, remaining * portions[i] // whole), surplus)
            counts[i] = counts[i] + addition
            surplus = surplus - addition
    return np.array(counts)


def scatter_about(own_key, dims, scale, bound, cuts=(), kind=jnp.bfloat16):
    loudness = levels(own_key, dims, cuts, -0.22, 0.18) if cuts else 1.0
    array = jax.random.normal(own_key, dims, jnp.float32) * scale * loudness
    return jnp.minimum(jnp.maximum(array, -bound), bound).astype(kind)


def heavy_noise(own_key, shape, scale, bound, cuts, heavy, held_as=jnp.bfloat16):
    entries = scale * jax.random.normal(own_key, shape, jnp.float32)
    if cuts:
        entries = entries * levels(own_key, shape, cuts, -0.22, 0.18)
    return jnp.clip(raised(entries, jax.random.fold_in(own_key, 3), *heavy), -bound, bound).astype(held_as)


def setup_inputs(seed: int = 0) -> dict:
    splits = jax.random.split(jax.random.key(seed), 15)
    tokens = heavy_noise(splits[0], (TOKENS, D), 1.0, 6.0, ((0, 32),), (0, 1, 32, 2.75))
    gain_attn = jnp.clip(1.0 + 0.18 * jax.random.normal(splits[1], (D,), jnp.float32), 0.1, 1.9)
    w_qkv = scatter_about(splits[2], (3, D, D), D ** -0.5, 0.125, ((1, 8), (2, 4)))
    b_qkv = draw_b_qkv(jax.random.fold_in(splits[14], 71), 0)
    w_out = scatter_about(splits[4], (D, D), (D // 16) ** -0.5, 0.5, ((0, 4), (1, 8)))
    gain_ffn = jnp.clip(1.0 + 0.18 * jax.random.normal(splits[5], (D,), jnp.float32), 0.1, 1.9)
    w_router = scatter_about(splits[6], (D, EXPERTS), D ** -0.5, 0.125)
    shared_gate = scatter_about(splits[7], (D,), D ** -0.5, 0.125, (), jnp.float32)
    w_shared_gu = scatter_about(splits[8], (2, D, SFF), D ** -0.5, 0.125, ((1, 8), (2, 4)))
    w_shared_down = scatter_about(splits[9], (SFF, D), SFF ** -0.5, 0.078125, ((0, 4), (1, 8)))
    w_expert_gu = scatter_about(splits[10], (EXPERTS, 2, D, FF), D ** -0.5, 0.125, ((0, 32),))
    w_expert_down = scatter_about(splits[11], (EXPERTS, FF, D), (max(FF // 64, 1)) ** -0.5, 1.25, ((0, 32),))
    routes_keys = jax.random.split(jax.random.fold_in(splits[12], 1), TOKENS // TOK_DEV)
    routes_turns = jax.random.permutation(jax.random.fold_in(splits[12], 3), TOKENS // TOK_DEV)
    routes = jax.vmap(lambda own, number: deal_out(jax.random.fold_in(splits[12], 2), own, number, TOK_DEV, EXPERTS, TOPK, CAP, 2))(routes_keys, routes_turns).reshape((TOKENS, TOPK))
    grad_out = heavy_noise(splits[13], (TOKENS, D), 1.0, 6.0, ((0, 32),), (0, 1, 32, 2.75))
    return dict(tokens=tokens, gain_attn=gain_attn, w_qkv=w_qkv, b_qkv=b_qkv, w_out=w_out, gain_ffn=gain_ffn, w_router=w_router, shared_gate=shared_gate, w_shared_gu=w_shared_gu, w_shared_down=w_shared_down, w_expert_gu=w_expert_gu, w_expert_down=w_expert_down, routes=routes, grad_out=grad_out)


eps = 1e-06
rope_base = 1000000.0
highest = lax.Precision.HIGHEST

@jax.custom_vjp
def low(v):
    return lax.optimization_barrier(v.astype(jnp.bfloat16)).astype(jnp.float32)

@jax.custom_vjp
def low_back(v):
    return v

def low_keep(v):
    return (low(v), None)

def low_pass(kept, grad):
    return (grad,)

def back_keep(v):
    return (v, None)

def back_low(kept, grad):
    return (low(grad),)
low.defvjp(low_keep, low_pass)
low_back.defvjp(back_keep, back_low)

def rope_tables(length, head_width):
    half_width = head_width // 2
    inverse = rope_base ** (-(jnp.arange(half_width, dtype=jnp.float32) * 2.0 / head_width))
    angles = jnp.arange(length, dtype=jnp.float32)[:, None] * inverse[None, :]
    angles = jnp.concatenate([angles, angles], axis=1)
    return (jnp.cos(angles), jnp.sin(angles))

def rotate(values, cosine, sine_tab):
    half_width = values.shape[-1] // 2
    turned = jnp.concatenate([-values[..., half_width:], values[..., :half_width]], axis=-1)
    return values * cosine[:, None, :] + turned * sine_tab[:, None, :]

def rms_norm(values, gain_vec):
    scale_rows = lax.rsqrt(lax.optimization_barrier(jnp.mean(values * values, axis=-1, keepdims=True)) + eps)
    return values * scale_rows * gain_vec

def build_slots(routes):
    flat_routes = routes.reshape(DEVICES, TOK_DEV * TOPK).astype(jnp.int32)
    matches = (flat_routes[:, :, None] == jnp.arange(EXPERTS, dtype=jnp.int32)[None, None, :]).astype(jnp.int32)
    ranks = lax.optimization_barrier(jnp.sum((jnp.cumsum(matches, axis=1) - 1) * matches, axis=2))
    device_ids = jnp.arange(DEVICES, dtype=jnp.int32)[:, None]
    places = flat_routes * (DEVICES * CAP) + device_ids * CAP + ranks
    token_ids = device_ids * TOK_DEV + jnp.arange(TOK_DEV * TOPK, dtype=jnp.int32)[None, :] // TOPK
    filled = jnp.full((EXPERTS * DEVICES * CAP,), TOKENS, jnp.int32)
    filled = filled.at[places.reshape(-1)].set(token_ids.reshape(-1).astype(jnp.int32))
    return filled.reshape(EXPERTS, DEVICES * CAP)

def attend(seq_rows, qkv_w, qkv_b, out_w):
    projected = low_back(jnp.einsum('sd,cdh->csh', seq_rows, qkv_w, precision=highest) + qkv_b[:, None, :])
    split_proj = projected.reshape(3, SEQ, HEADS, HEAD_DIM)
    cosine, sine_tab = rope_tables(SEQ, HEAD_DIM)
    queries = low(rotate(split_proj[0], cosine, sine_tab))
    keys_low = low(rotate(split_proj[1], cosine, sine_tab))
    values = low(split_proj[2])
    scores = low_back(jnp.einsum('qhd,khd->hqk', queries, keys_low, precision=highest) * HEAD_DIM ** (-0.5))
    positions = jnp.arange(SEQ, dtype=jnp.int32)
    causal = positions[None, :] <= positions[:, None]
    scores = jnp.where(causal[None], scores, -jnp.inf)
    row_max = lax.optimization_barrier(jnp.max(scores, axis=-1, keepdims=True))
    weights = jnp.exp(scores - row_max)
    soft_probs = low(weights / lax.optimization_barrier(jnp.sum(weights, axis=-1, keepdims=True)))
    mixed_heads = jnp.einsum('hqk,khd->qhd', soft_probs, values, precision=highest).reshape(SEQ, D)
    mixed_heads = low_back(low(mixed_heads))
    return low_back(jnp.dot(mixed_heads, out_w, precision=highest))

def experts(normed_two, router_probs, egu_w, edown_w, slot_table):
    padded = jnp.concatenate([normed_two, jnp.zeros((1, D), jnp.float32)], axis=0)
    prob_pad = jnp.concatenate([router_probs, jnp.zeros((1, EXPERTS), jnp.float32)], axis=0)

    def one_expert(expert_item):
        slots_idx, gu_weight, down_weight, column = expert_item
        rows_in = low_back(padded[slots_idx])
        expert_gu = low_back(jnp.einsum('rd,cdf->crf', rows_in, gu_weight, precision=highest))
        expert_hid = low(jax.nn.silu(expert_gu[0]) * expert_gu[1])
        expert_out = low_back(low(jnp.dot(expert_hid, down_weight, precision=highest)))
        return prob_pad[slots_idx, column][:, None] * expert_out
    weighted = lax.map(jax.checkpoint(one_expert), (slot_table, egu_w, edown_w, jnp.arange(EXPERTS, dtype=jnp.int32)))
    summed = jnp.zeros((TOKENS + 1, D), jnp.float32).at[slot_table.reshape(-1)].add(weighted.reshape(-1, D))
    return summed[:TOKENS]

def reference(tokens, gain_attn, w_qkv, b_qkv, w_out, gain_ffn, w_router, shared_gate, w_shared_gu, w_shared_down, w_expert_gu, w_expert_down, routes, grad_out):
    slot_table = build_slots(routes)

    def forward(x_in, gain_one, qkv_w, qkv_b, out_w, gain_two, router_w, gate_w, sgu_w, sdown_w, egu_w, edown_w):
        normed_one = low(rms_norm(x_in, gain_one))
        sequences = normed_one.reshape(TOKENS // SEQ, SEQ, D)
        attn_out = lax.map(jax.checkpoint(lambda seq_rows: attend(seq_rows, qkv_w, qkv_b, out_w)), sequences).reshape(TOKENS, D)
        hidden = x_in + attn_out
        normed_two = low(rms_norm(hidden, gain_two))
        logits = low_back(jnp.dot(normed_two, router_w, precision=highest))
        router_exp = jnp.exp(logits)
        router_probs = router_exp / lax.optimization_barrier(jnp.sum(router_exp, axis=-1, keepdims=True))
        gate_logit = jnp.dot(normed_two, gate_w, precision=highest)
        shared_gu = low_back(jnp.einsum('td,cdf->ctf', normed_two, sgu_w, precision=highest))
        shared_hid = low(jax.nn.silu(shared_gu[0]) * shared_gu[1])
        shared_out = low_back(jnp.dot(shared_hid, sdown_w, precision=highest))
        expert_sum = experts(normed_two, router_probs, egu_w, edown_w, slot_table)
        return hidden + jax.nn.sigmoid(gate_logit)[:, None] * shared_out + expert_sum
    primals = (tokens.astype(jnp.float32), gain_attn, w_qkv.astype(jnp.float32), b_qkv, w_out.astype(jnp.float32), gain_ffn, w_router.astype(jnp.float32), shared_gate, w_shared_gu.astype(jnp.float32), w_shared_down.astype(jnp.float32), w_expert_gu.astype(jnp.float32), w_expert_down.astype(jnp.float32))
    output, pullback = jax.vjp(forward, *primals)
    grads = pullback(grad_out.astype(jnp.float32))
    return (output.astype(jnp.bfloat16), grads[0], grads[1], grads[2], grads[3], grads[4], grads[5], grads[6], grads[7], grads[8], grads[9], grads[10], grads[11])
```

```python
import functools

import jax
import jax.numpy as jnp
from jax import lax
from jax.experimental import pallas as pl
from jax.experimental.pallas import tpu as pltpu
from jax.sharding import PartitionSpec as P

HEAD_DIM = 128
TOPK = 4
EXPERT = "expert"
SHARD = "shard"
both = (EXPERT, SHARD)
eps = 1e-06
rope_base = 1000000.0
highest = lax.Precision.HIGHEST

MESH_ID = pl.DeviceIdType.MESH


class Place:
    def __init__(self, levels):
        self.levels = levels
        spot, lane = lax.axis_index(EXPERT), lax.axis_index(SHARD)
        self.z, self.y = spot // 2, spot % 2
        self.x, self.c = lane // 2, lane % 2

    def device(self, z=None, y=None, x=None, c=None):
        z = self.z if z is None else z
        y = self.y if y is None else y
        x = self.x if x is None else x
        c = self.c if c is None else c
        return {EXPERT: z * 2 + y, SHARD: x * 2 + c}

    def flat(self, z, y, x, c):
        return ((z * 2 + y) * 2 + x) * 2 + c


def greet(place, targets, ends):
    barrier = pltpu.get_barrier_semaphore()
    for target in targets:
        pl.semaphore_signal(barrier, inc=1, device_id=target, device_id_type=MESH_ID)
    count = len(targets)
    if ends:
        @pl.when(place.z > 0)
        def _():
            pl.semaphore_signal(
                barrier, inc=1, device_id=place.device(z=place.z - 1), device_id_type=MESH_ID
            )

        @pl.when(place.z < place.levels - 1)
        def _():
            pl.semaphore_signal(
                barrier, inc=1, device_id=place.device(z=place.z + 1), device_id_type=MESH_ID
            )

        inner = (place.z > 0).astype(jnp.int32) + (place.z < place.levels - 1).astype(jnp.int32)
        count = count + inner
    pl.semaphore_wait(barrier, count)


def gather_steps(levels, sources, outs, own_sem, send_sems, recv_sems):
    place = Place(levels)
    z, y, x, c = place.z, place.y, place.x, place.c
    top = levels - 1
    x_dev, y_dev, c_dev = place.device(x=1 - x), place.device(y=1 - y), place.device(c=1 - c)

    class Copies:
        def __init__(self, kind, level, refs_from, refs_to, device):
            self.each = [
                pltpu.make_async_remote_copy(
                    src_ref=ref,
                    dst_ref=dst,
                    send_sem=send_sems.at[kind, level, i],
                    recv_sem=recv_sems.at[kind, level, i],
                    device_id=device,
                    device_id_type=MESH_ID,
                )
                for i, (ref, dst) in enumerate(zip(refs_from, refs_to))
            ]

        def start(self):
            for one in self.each:
                one.start()

        def wait_recv(self):
            for one in self.each:
                one.wait_recv()

        def wait_send(self):
            for one in self.each:
                one.wait_send()

    copy = Copies

    def block(level, yy, xx, cc):
        return [out.at[place.flat(level, yy, xx, cc)] for out in outs]

    def part(level, yy, xx, cc, side):
        flat = place.flat(level, yy, xx, cc)
        return [
            out.at[flat, pl.ds(side * (out.shape[1] // 2), out.shape[1] // 2)] for out in outs
        ]

    UP, DOWN, XN, YN, DX, DY, CO, CX, CY, CDX, CDY = range(11)

    def dst_of(kind, level):
        if kind in (UP, DOWN):
            return block(level, y, x, c)
        if kind == XN:
            return block(level, y, 1 - x, c)
        if kind == YN:
            return block(level, 1 - y, x, c)
        if kind == DX:
            return part(level, 1 - y, 1 - x, c, 0)
        if kind == DY:
            return part(level, 1 - y, 1 - x, c, 1)
        if kind == CO:
            return block(level, y, x, 1 - c)
        if kind == CX:
            return block(level, y, 1 - x, 1 - c)
        if kind == CY:
            return block(level, 1 - y, x, 1 - c)
        if kind == CDX:
            return part(level, 1 - y, 1 - x, 1 - c, 0)
        return part(level, 1 - y, 1 - x, 1 - c, 1)

    def arrived(kind, level):
        ref = dst_of(kind, level)
        copy(kind, level, ref, ref, c_dev).wait_recv()

    def sent(kind, level, ref):
        copy(kind, level, ref, ref, c_dev).wait_send()

    def spread(level, ref):
        copy(XN, level, ref, block(level, y, x, c), x_dev).start()
        copy(YN, level, ref, block(level, y, x, c), y_dev).start()
        copy(CO, level, ref, block(level, y, x, c), c_dev).start()

    def at_distance(t, action):
        if t == 0:
            action(z)
            return

        @pl.when(z - t >= 0)
        def _():
            action(z - t)

        @pl.when(z + t <= top)
        def _():
            action(z + t)

    def from_neighbours(level):
        arrived(XN, level)
        ref = part(level, y, 1 - x, c, 1)
        copy(DY, level, ref, ref, y_dev).start()
        ref = block(level, y, 1 - x, c)
        copy(CX, level, ref, ref, c_dev).start()
        arrived(YN, level)
        ref = part(level, 1 - y, x, c, 0)
        copy(DX, level, ref, ref, x_dev).start()
        ref = block(level, 1 - y, x, c)
        copy(CY, level, ref, ref, c_dev).start()

    def from_diagonal(level):
        arrived(DX, level)
        ref = part(level, 1 - y, 1 - x, c, 0)
        copy(CDX, level, ref, ref, c_dev).start()
        arrived(DY, level)
        ref = part(level, 1 - y, 1 - x, c, 1)
        copy(CDY, level, ref, ref, c_dev).start()

    def start():
        greet(place, [x_dev, y_dev, c_dev], True)
        for i, (ref, dst) in enumerate(zip(sources, block(z, y, x, c))):
            pltpu.make_async_copy(ref, dst, own_sem.at[i]).start()

        @pl.when(z < top)
        def _():
            copy(UP, z, sources, block(z, y, x, c), place.device(z=z + 1)).start()

        @pl.when(z > 0)
        def _():
            copy(DOWN, z, sources, block(z, y, x, c), place.device(z=z - 1)).start()

        spread(z, sources)

    def onward(t):
        if t < levels:
            @pl.when(z - t >= 0)
            def _():
                level = z - t
                arrived(UP, level)
                ref = block(level, y, x, c)

                @pl.when(z < top)
                def _():
                    copy(UP, level, ref, ref, place.device(z=z + 1)).start()

                spread(level, ref)

            @pl.when(z + t <= top)
            def _():
                level = z + t
                arrived(DOWN, level)
                ref = block(level, y, x, c)

                @pl.when(z > 0)
                def _():
                    copy(DOWN, level, ref, ref, place.device(z=z - 1)).start()

                spread(level, ref)

        if t - 1 < levels:
            at_distance(t - 1, from_neighbours)
        if 0 <= t - 2 < levels:
            at_distance(t - 2, from_diagonal)


    def finish():
        for i, (ref, dst) in enumerate(zip(sources, block(z, y, x, c))):
            pltpu.make_async_copy(ref, dst, own_sem.at[i]).wait()
        for level in range(levels):
            for kind in (CO, CX, CY, CDX, CDY):
                arrived(kind, level)
            for kind in (XN, YN, DX, DY, CO, CX, CY, CDX, CDY):
                sent(kind, level, dst_of(kind, level))

            @pl.when((z < top) & (level <= z))
            def _():
                sent(UP, level, dst_of(UP, level))

            @pl.when((z > 0) & (level >= z))
            def _():
                sent(DOWN, level, dst_of(DOWN, level))

    middle = [functools.partial(onward, t) for t in range(1, levels + 2)]
    return [start] + middle + [finish]


def gather_kernel(levels, size, *refs):
    sources, outs = refs[:size], refs[size : 2 * size]
    for step in gather_steps(levels, sources, outs, *refs[2 * size :]):
        step()


def gather_all(arrays, levels, count, ident):
    size = len(arrays)
    outs = pl.pallas_call(
        functools.partial(gather_kernel, levels, size),
        out_shape=[jax.ShapeDtypeStruct((count,) + a.shape, a.dtype) for a in arrays],
        in_specs=[pl.BlockSpec(memory_space=pltpu.VMEM)] * size,
        out_specs=[pl.BlockSpec(memory_space=pl.ANY)] * size,
        scratch_shapes=[
            pltpu.SemaphoreType.DMA((size,)),
            pltpu.SemaphoreType.DMA((11, levels, size)),
            pltpu.SemaphoreType.DMA((11, levels, size)),
        ],
        compiler_params=pltpu.CompilerParams(collective_id=ident, has_side_effects=True),
        name="gather_all",
    )(*arrays)
    return [out.reshape((-1,) + out.shape[2:]) for out in outs]


def scatter_steps(
    levels, part, out, from_c, from_d, from_xy, from_z, load, load_sem, send_sem, recv_sem
):
    place = Place(levels)
    z, y, x, c = place.z, place.y, place.x, place.c
    top = levels - 1
    width = part.shape[-1]
    half = width // 2
    x_dev, y_dev, c_dev = place.device(x=1 - x), place.device(y=1 - y), place.device(c=1 - c)
    OWN, XN, YN, DIAG = 0, 1, 2, 3
    CORE, TOX, TOY, DX, DY, UP, DOWN = 0, 4, 5, 6, 7, 8, 9

    def columns(col):
        return {OWN: (y, x), XN: (y, 1 - x), YN: (1 - y, x), DIAG: (1 - y, 1 - x)}[col]

    def copy(kind, level, ref, dst, device):
        return pltpu.make_async_remote_copy(
            src_ref=ref,
            dst_ref=dst,
            send_sem=send_sem.at[kind, level],
            recv_sem=recv_sem.at[kind, level],
            device_id=device,
            device_id_type=MESH_ID,
        )

    def block(level, col, cc):
        yy, xx = columns(col)
        return part.at[place.flat(level, yy, xx, cc)]

    def core_copy(level, col):
        return copy(CORE + col, level, block(level, col, 1 - c), from_c.at[col, level], c_dev)

    def load_copy(level, col):
        return pltpu.make_async_copy(block(level, col, c), load.at[col, level], load_sem.at[col, level])

    def at_distance(t, action):
        if t == 0:
            action(z)
            return

        @pl.when(z - t >= 0)
        def _():
            action(z - t)

        @pl.when(z + t <= top)
        def _():
            action(z + t)

    def each_level(action):
        for t in range(levels - 1, -1, -1):
            at_distance(t, action)

    def start():
        greet(place, [x_dev, y_dev, c_dev], True)
        for col in (DIAG, XN, YN, OWN):
            def begin(level):
                core_copy(level, col).start()
                load_copy(level, col).start()
            each_level(begin)

    def strips(action):
        def step(i, carry):
            action(pl.ds(pl.multiple_of(i * 16, 16), 16))
            return carry
        lax.fori_loop(0, part.shape[1] // 16, step, 0)

    def f32(ref, *where):
        return ref[where].astype(jnp.float32)

    low, high = slice(0, half), slice(half, width)

    def diagonal(level):
        load_copy(level, DIAG).wait()
        core_copy(level, DIAG).wait_recv()

        def add(rows):
            load[DIAG, level, rows] = (
                f32(load, DIAG, level, rows) + f32(from_c, DIAG, level, rows)
            ).astype(load.dtype)
        strips(add)
        copy(DX, level, load.at[DIAG, level, :, low], from_d.at[0, level], x_dev).start()
        copy(DY, level, load.at[DIAG, level, :, high], from_d.at[1, level], y_dev).start()

    def sides(level):
        for col, kind, side, goes, device in ((XN, DY, 1, TOX, x_dev), (YN, DX, 0, TOY, y_dev)):
            load_copy(level, col).wait()
            core_copy(level, col).wait_recv()
            copy(kind, level, from_d.at[side, level], from_d.at[side, level], device).wait_recv()
            mine, other = (high, low) if side else (low, high)

            def add(rows):
                load[col, level, rows, mine] = (
                    f32(load, col, level, rows, mine)
                    + f32(from_c, col, level, rows, mine)
                    + f32(from_d, side, level, rows)
                ).astype(load.dtype)
                load[col, level, rows, other] = (
                    f32(load, col, level, rows, other) + f32(from_c, col, level, rows, other)
                ).astype(load.dtype)
            strips(add)
            copy(goes, level, load.at[col, level], from_xy.at[goes - TOX, level], device).start()

    def await_column(level):
        load_copy(level, OWN).wait()
        core_copy(level, OWN).wait_recv()
        copy(TOX, level, from_xy.at[0, level], from_xy.at[0, level], x_dev).wait_recv()
        copy(TOY, level, from_xy.at[1, level], from_xy.at[1, level], y_dev).wait_recv()

    def column(level, rows):
        return (
            f32(load, OWN, level, rows)
            + f32(from_c, OWN, level, rows)
            + f32(from_xy, 0, level, rows)
            + f32(from_xy, 1, level, rows)
        )


    def pass_on(level, kind, first, target, slot):
        await_column(level)

        @pl.when(first)
        def _():
            def add(rows):
                load[OWN, level, rows] = column(level, rows).astype(load.dtype)
            strips(add)

        @pl.when(jnp.logical_not(first))
        def _():
            copy(kind, level, from_z.at[level], from_z.at[level], c_dev).wait_recv()

            def add(rows):
                load[OWN, level, rows] = (
                    column(level, rows) + f32(from_z, level, rows)
                ).astype(load.dtype)
            strips(add)
        copy(kind, level, load.at[OWN, level], from_z.at[slot], target).start()

    def along_z(t):
        @pl.when(z + t <= top)
        def _():
            pass_on(z + t, UP, z == 0, place.device(z=z + 1), z + t)

        @pl.when(z - t >= 0)
        def _():
            slot = (z - t) if t > 1 else levels
            pass_on(z - t, DOWN, z == top, place.device(z=z - 1), slot)

    def finish_all():
        await_column(z)

        def add(rows):
            out[rows] = column(z, rows)
        strips(add)

        @pl.when(z > 0)
        def _():
            copy(UP, z, from_z.at[z], from_z.at[z], c_dev).wait_recv()

            def add(rows):
                out[rows] += f32(from_z, z, rows)
            strips(add)

        @pl.when(z < top)
        def _():
            copy(DOWN, z, from_z.at[levels], from_z.at[levels], c_dev).wait_recv()

            def add(rows):
                out[rows] += f32(from_z, levels, rows)
            strips(add)

        def finish(level):
            for col in (OWN, XN, YN, DIAG):
                core_copy(level, col).wait_send()
            copy(DX, level, from_d.at[0, level], from_d.at[0, level], x_dev).wait_send()
            copy(DY, level, from_d.at[1, level], from_d.at[1, level], y_dev).wait_send()
            copy(TOX, level, load.at[XN, level], from_xy.at[0, level], x_dev).wait_send()
            copy(TOY, level, load.at[YN, level], from_xy.at[1, level], y_dev).wait_send()

        for level in range(levels):
            finish(level)

            @pl.when(level > z)
            def _():
                copy(UP, level, load.at[OWN, level], from_z.at[level], c_dev).wait_send()

            @pl.when(level < z)
            def _():
                copy(DOWN, level, load.at[OWN, level], from_z.at[level], c_dev).wait_send()

    far = range(levels - 1, -1, -1)
    return (
        [start, functools.partial(each_level, diagonal)]
        + [functools.partial(at_distance, t, sides) for t in far]
        + [functools.partial(along_z, t) for t in far if t > 0]
        + [finish_all]
    )


def scatter_kernel(levels, *refs):
    for step in scatter_steps(levels, *refs):
        step()


def scatter_scratch(levels, rows, width, low):
    return [
        pltpu.VMEM((4, levels, rows, width), low),
        pltpu.VMEM((2, levels, rows, width // 2), low),
        pltpu.VMEM((2, levels, rows, width), low),
        pltpu.VMEM((levels + 1, rows, width), low),
        pltpu.VMEM((4, levels, rows, width), low),
        pltpu.SemaphoreType.DMA((4, levels)),
        pltpu.SemaphoreType.DMA((10, levels)),
        pltpu.SemaphoreType.DMA((10, levels)),
    ]


def scatter_all(part, levels, ident):
    count, rows, width = part.shape
    return pl.pallas_call(
        functools.partial(scatter_kernel, levels),
        out_shape=jax.ShapeDtypeStruct((rows, width), jnp.float32),
        in_specs=[pl.BlockSpec(memory_space=pl.ANY)],
        out_specs=pl.BlockSpec(memory_space=pltpu.VMEM),
        scratch_shapes=scatter_scratch(levels, rows, width, part.dtype),
        compiler_params=pltpu.CompilerParams(
            collective_id=ident, has_side_effects=True, vmem_limit_bytes=56 * 2**20
        ),
        name="scatter_all",
    )(part)


def lane_block(ref, index, width):
    return ref.at[:, pl.ds(pl.multiple_of(index * width, width), width)]


def gather_first_kernel(
    levels, qkv, wout, rows, qkv_all, wout_all, rows_all, own_sem, send_sem, recv_sem
):
    place = Place(levels)
    z, y, x, c = place.z, place.y, place.x, place.c
    top = levels - 1
    x_dev, y_dev, c_dev = place.device(x=1 - x), place.device(y=1 - y), place.device(c=1 - c)
    UP, DOWN, YN = range(3)
    pieces = 4
    row_kind = pieces * 3
    own_weights = [qkv.at[k] for k in range(3)] + [wout]

    def weight_refs(level, yy):
        spot = level * 2 + yy
        return [qkv_all.at[k, spot] for k in range(3)] + [
            lane_block(wout_all, spot, wout.shape[1])
        ]

    def copy(index, level, ref, dst, device):
        return pltpu.make_async_remote_copy(
            src_ref=ref,
            dst_ref=dst,
            send_sem=send_sem.at[index, level],
            recv_sem=recv_sem.at[index, level],
            device_id=device,
            device_id_type=MESH_ID,
        )

    def send(kind, level, refs, device, only=None):
        for i, (ref, dst) in enumerate(zip(refs, weight_refs(level, y))):
            if only in (None, i):
                copy(kind * pieces + i, level, ref, dst, device).start()

    def arrived(kind, level, only=None):
        for i, ref in enumerate(weight_refs(level, 1 - y if kind == YN else y)):
            if only in (None, i):
                copy(kind * pieces + i, level, ref, ref, c_dev).wait_recv()

    def sent(kind, level):
        for i, ref in enumerate(weight_refs(level, y)):
            copy(kind * pieces + i, level, ref, ref, c_dev).wait_send()

    greet(place, [x_dev, y_dev, c_dev], True)

    @pl.when(z < top)
    def _():
        send(UP, z, own_weights, place.device(z=z + 1))

    @pl.when(z > 0)
    def _():
        send(DOWN, z, own_weights, place.device(z=z - 1))

    send(YN, z, own_weights, y_dev)

    def row_ref(xx, cc):
        return rows_all.at[xx * 2 + cc]

    to_x = copy(row_kind, 0, rows, row_ref(x, c), x_dev)
    to_c = copy(row_kind, 1, rows, row_ref(x, c), c_dev)
    to_x.start()
    to_c.start()
    own = [
        pltpu.make_async_copy(ref, dst, own_sem.at[i])
        for i, (ref, dst) in enumerate(
            zip(own_weights + [rows], weight_refs(z, y) + [row_ref(x, c)])
        )
    ]
    for one in own:
        one.start()
    copy(row_kind, 0, rows, row_ref(1 - x, c), x_dev).wait_recv()
    on = copy(row_kind, 2, row_ref(1 - x, c), row_ref(1 - x, c), c_dev)
    on.start()

    def relay(kind, level, inner, target):
        for i in range(pieces):
            arrived(kind, level, i)

            @pl.when(inner)
            def _():
                send(kind, level, weight_refs(level, y), target, i)

            send(YN, level, weight_refs(level, y), y_dev, i)

    for t in range(1, levels):
        @pl.when(z - t >= 0)
        def _():
            relay(UP, z - t, z < top, place.device(z=z + 1))

        @pl.when(z + t <= top)
        def _():
            relay(DOWN, z + t, z > 0, place.device(z=z - 1))

    for one in own:
        one.wait()
    to_c.wait_recv()
    on.wait_recv()
    for one in (to_x, to_c, on):
        one.wait_send()
    for level in range(levels):
        arrived(YN, level)
        sent(YN, level)

        @pl.when((z < top) & (level <= z))
        def _():
            sent(UP, level)

        @pl.when((z > 0) & (level >= z))
        def _():
            sent(DOWN, level)


def gather_first(w_qkv, w_out, rows, levels, lanes, ident):
    spots = levels * 2
    qkv_all, wout_all, rows_all = pl.pallas_call(
        functools.partial(gather_first_kernel, levels),
        out_shape=[
            jax.ShapeDtypeStruct((3, spots) + w_qkv.shape[1:], w_qkv.dtype),
            jax.ShapeDtypeStruct((w_out.shape[0], spots * w_out.shape[1]), w_out.dtype),
            jax.ShapeDtypeStruct((lanes,) + rows.shape, rows.dtype),
        ],
        in_specs=[pl.BlockSpec(memory_space=pltpu.VMEM)] * 3,
        out_specs=[pl.BlockSpec(memory_space=pl.ANY)] * 3,
        scratch_shapes=[
            pltpu.SemaphoreType.DMA((5,)),
            pltpu.SemaphoreType.DMA((13, levels)),
            pltpu.SemaphoreType.DMA((13, levels)),
        ],
        compiler_params=pltpu.CompilerParams(collective_id=ident, has_side_effects=True),
        name="gather_first",
    )(w_qkv, w_out, rows)
    return (
        qkv_all.reshape(3, -1, w_qkv.shape[2]),
        wout_all,
        rows_all.reshape(-1, rows.shape[1]),
    )


def gather_lanes_kernel(levels, rows, rows_all, own_sem, send_sem, recv_sem):
    place = Place(levels)
    x, c = place.x, place.c
    x_dev, c_dev = place.device(x=1 - x), place.device(c=1 - c)

    def row_ref(xx, cc):
        return rows_all.at[xx * 2 + cc]

    def copy(index, ref, dst, device):
        return pltpu.make_async_remote_copy(
            src_ref=ref,
            dst_ref=dst,
            send_sem=send_sem.at[index],
            recv_sem=recv_sem.at[index],
            device_id=device,
            device_id_type=MESH_ID,
        )

    greet(place, [x_dev, c_dev], False)
    half = rows.shape[0] // 2
    parts = [pl.ds(0, half), pl.ds(half, half)]
    to_x = [copy(i, rows.at[p], row_ref(x, c).at[p], x_dev) for i, p in enumerate(parts)]
    to_c = copy(2, rows, row_ref(x, c), c_dev)
    own = pltpu.make_async_copy(rows, row_ref(x, c), own_sem)
    for one in to_x:
        one.start()
    to_c.start()
    own.start()
    on = []
    for i, p in enumerate(parts):
        to_x[i].wait_recv()
        on.append(copy(3 + i, row_ref(1 - x, c).at[p], row_ref(1 - x, c).at[p], c_dev))
        on[i].start()
    own.wait()
    to_c.wait()
    for one in on:
        one.wait()
    for one in to_x:
        one.wait_send()


def gather_lanes(rows, levels, lanes, ident):
    out = pl.pallas_call(
        functools.partial(gather_lanes_kernel, levels),
        out_shape=jax.ShapeDtypeStruct((lanes,) + rows.shape, rows.dtype),
        in_specs=[pl.BlockSpec(memory_space=pltpu.VMEM)],
        out_specs=pl.BlockSpec(memory_space=pltpu.VMEM),
        scratch_shapes=[
            pltpu.SemaphoreType.DMA,
            pltpu.SemaphoreType.DMA((5,)),
            pltpu.SemaphoreType.DMA((5,)),
        ],
        compiler_params=pltpu.CompilerParams(collective_id=ident, has_side_effects=True),
        name="gather_lanes",
    )(rows)
    return out.reshape(-1, rows.shape[1])


def scatter_lanes_kernel(levels, part, out, from_c, tx, from_x, send_sem, recv_sem):
    place = Place(levels)
    x, c = place.x, place.c
    x_dev, c_dev = place.device(x=1 - x), place.device(c=1 - c)
    rows = part.shape[1]
    pieces = 2
    size = rows // pieces

    def copy(index, ref, dst, device):
        return pltpu.make_async_remote_copy(
            src_ref=ref,
            dst_ref=dst,
            send_sem=send_sem.at[index],
            recv_sem=recv_sem.at[index],
            device_id=device,
            device_id_type=MESH_ID,
        )

    def strips(piece, action):
        def step(i, carry):
            action(pl.ds(pl.multiple_of(piece * size + i * 16, 16), 16))
            return carry
        lax.fori_loop(0, size // 16, step, 0)

    greet(place, [x_dev, c_dev], False)
    spans = [pl.ds(i * size, size) for i in range(pieces)]
    far = [
        copy(i, part.at[(1 - x) * 2 + 1 - c, p], from_c.at[0, p], c_dev)
        for i, p in enumerate(spans)
    ]
    near = copy(pieces, part.at[x * 2 + 1 - c], from_c.at[1], c_dev)
    for one in far:
        one.start()
    near.start()
    to_x = []
    for i, p in enumerate(spans):
        far[i].wait_recv()

        def add(span):
            tx[span] = (
                part[(1 - x) * 2 + c, span].astype(jnp.float32)
                + from_c[0, span].astype(jnp.float32)
            ).astype(tx.dtype)
        strips(i, add)
        to_x.append(copy(pieces + 1 + i, tx.at[p], from_x.at[p], x_dev))
        to_x[i].start()
    near.wait_recv()
    for i in range(pieces):
        to_x[i].wait_recv()

        def add(span):
            out[span] = (
                part[x * 2 + c, span].astype(jnp.float32)
                + from_c[1, span].astype(jnp.float32)
                + from_x[span].astype(jnp.float32)
            )
        strips(i, add)
    for one in far + [near] + to_x:
        one.wait_send()


def scatter_lanes(part, levels, lanes, ident):
    width = part.shape[1]
    rows = part.shape[0] // lanes
    low = part.dtype
    return pl.pallas_call(
        functools.partial(scatter_lanes_kernel, levels),
        out_shape=jax.ShapeDtypeStruct((rows, width), jnp.float32),
        in_specs=[pl.BlockSpec(memory_space=pltpu.VMEM)],
        out_specs=pl.BlockSpec(memory_space=pltpu.VMEM),
        scratch_shapes=[
            pltpu.VMEM((2, rows, width), low),
            pltpu.VMEM((rows, width), low),
            pltpu.VMEM((rows, width), low),
            pltpu.SemaphoreType.DMA((5,)),
            pltpu.SemaphoreType.DMA((5,)),
        ],
        compiler_params=pltpu.CompilerParams(collective_id=ident, has_side_effects=True),
        name="scatter_lanes",
    )(part.reshape(lanes, rows, width))


def scatter_last_kernel(
    levels, qkv, wout, small, parts, qkv_out, wout_out, small_out, gu_out, down_out,
    q_load, w_load, q_y, w_y, q_z, w_z, q_tx, w_tx, s_y, s_tx,
    load_sem, y_send, y_recv, z_send, z_recv, s_send, s_recv,
):
    place = Place(levels)
    z, y, x, c = place.z, place.y, place.x, place.c
    top = levels - 1
    x_dev, y_dev, c_dev = place.device(x=1 - x), place.device(y=1 - y), place.device(c=1 - c)
    out_width = w_y.shape[2]

    def remote(sends, recvs, where, ref, dst, device):
        return pltpu.make_async_remote_copy(
            src_ref=ref,
            dst_ref=dst,
            send_sem=sends.at[where],
            recv_sem=recvs.at[where],
            device_id=device,
            device_id_type=MESH_ID,
        )

    def block(level, yy):
        spot = level * 2 + yy
        return [qkv.at[k, spot] for k in range(3)] + [lane_block(wout, spot, out_width)]

    def pieces(q, w, level):
        return [q.at[level, k] for k in range(3)] + [w.at[level]]

    def load(level, i):
        ref = block(level, y)[i]
        dst = pieces(q_load, w_load, level)[i]
        return pltpu.make_async_copy(ref, dst, load_sem.at[i, level])

    def across(level, i):
        ref = block(level, 1 - y)[i]
        dst = pieces(q_y, w_y, level)[i]
        return remote(y_send, y_recv, (i, level), ref, dst, y_dev)

    def along(kind, level, slot, device, i):
        ref, dst = pieces(q_tx, w_tx, level)[i], pieces(q_z, w_z, slot)[i]
        return remote(z_send, z_recv, (kind, i, level), ref, dst, device)

    greet(place, [x_dev, y_dev, c_dev], True)

    s_first = remote(s_send, s_recv, 0, small.at[1 - c], s_y.at[0], c_dev)
    s_first.start()
    s_first.wait_recv()
    s_tx[0] = small[c] + s_y[0]
    s_yy = remote(s_send, s_recv, 1, s_tx.at[0], s_y.at[1], y_dev)
    s_yy.start()

    def each_level(action):
        for t in range(levels - 1, 0, -1):
            @pl.when(z - t >= 0)
            def _():
                action(z - t)

            @pl.when(z + t <= top)
            def _():
                action(z + t)

        action(z)

    def begin(level):
        for i in range(4):
            across(level, i).start()
            load(level, i).start()

    each_level(begin)

    s_yy.wait_recv()
    s_tx[2 + z] = s_tx[0] + s_y[1]

    def share(kind, level):
        ref = s_tx.at[2 + level]
        target = place.device(z=z + 1) if kind == 0 else place.device(z=z - 1)
        return remote(s_send, s_recv, 4 + kind * levels + level, ref, ref, target)

    @pl.when(z < top)
    def _():
        share(0, z).start()

    @pl.when(z > 0)
    def _():
        share(1, z).start()

    for t in range(1, levels):
        @pl.when(z - t >= 0)
        def _():
            share(0, z - t).wait_recv()

            @pl.when(z < top)
            def _():
                share(0, z - t).start()

        @pl.when(z + t <= top)
        def _():
            share(1, z + t).wait_recv()

            @pl.when(z > 0)
            def _():
                share(1, z + t).start()

    whole = s_tx[2]
    for level in range(1, levels):
        whole = whole + s_tx[2 + level]
    s_tx[1] = whole
    s_x = remote(s_send, s_recv, 2, s_tx.at[1], s_y.at[2], x_dev)
    s_x.start()

    units = parts.shape[3]
    for i in range(parts.shape[0]):
        span = slice(i * units, (i + 1) * units)
        for k in range(2):
            gu_out[k, :, span] = parts[i, k].astype(jnp.float32)
        down_out[span] = parts[i, 2].astype(jnp.float32).T

    def strips(ref, action):
        def step(i, carry):
            rows = pl.ds(pl.multiple_of(i * 16, 16), 16)
            ref[rows] = action(rows).astype(ref.dtype)
            return carry
        lax.fori_loop(0, ref.shape[0] // 16, step, 0)

    def f32(ref, rows):
        return ref[rows].astype(jnp.float32)

    def pass_on(level, kind, first, target, slot):
        mine, theirs = pieces(q_load, w_load, level), pieces(q_y, w_y, level)
        ahead, results = pieces(q_z, w_z, level), pieces(q_tx, w_tx, level)
        for i in range(4):
            load(level, i).wait()
            across(level, i).wait_recv()

            @pl.when(first)
            def _():
                strips(results[i], lambda rows: f32(mine[i], rows) + f32(theirs[i], rows))

            @pl.when(jnp.logical_not(first))
            def _():
                along(kind, level, level, c_dev, i).wait_recv()
                strips(
                    results[i],
                    lambda rows: f32(mine[i], rows) + f32(theirs[i], rows) + f32(ahead[i], rows),
                )
            along(kind, level, slot, target, i).start()

    for t in range(levels - 1, 0, -1):
        @pl.when(z + t <= top)
        def _():
            pass_on(z + t, 0, z == 0, place.device(z=z + 1), z + t)

        @pl.when(z - t >= 0)
        def _():
            slot = (z - t) if t > 1 else levels
            pass_on(z - t, 1, z == top, place.device(z=z - 1), slot)

        if t == levels - 1:
            s_x.wait_recv()
            small_out[c] = s_tx[1] + s_y[2]
            s_last = remote(s_send, s_recv, 3, small_out.at[c], small_out.at[c], c_dev)
            s_last.start()

    results = [qkv_out.at[k] for k in range(3)] + [wout_out]
    mine, theirs = pieces(q_load, w_load, z), pieces(q_y, w_y, z)
    for i in range(4):
        load(z, i).wait()
        across(z, i).wait_recv()
        strips(results[i], lambda rows: f32(mine[i], rows) + f32(theirs[i], rows))
    for kind, here, slot in ((0, z > 0, z), (1, z < top, levels)):
        ahead = pieces(q_z, w_z, slot)

        @pl.when(here)
        def _():
            for i in range(4):
                along(kind, z, slot, c_dev, i).wait_recv()
                strips(results[i], lambda rows: results[i][rows] + f32(ahead[i], rows))

    remote(s_send, s_recv, 3, small_out.at[1 - c], small_out.at[1 - c], c_dev).wait_recv()
    for one in (s_first, s_x, s_yy, s_last):
        one.wait_send()
    for level in range(levels):
        for i in range(4):
            across(level, i).wait_send()

        @pl.when(level > z)
        def _():
            for i in range(4):
                along(0, level, level, c_dev, i).wait_send()

        @pl.when(level < z)
        def _():
            for i in range(4):
                along(1, level, level, c_dev, i).wait_send()

        @pl.when((z < top) & (level <= z))
        def _():
            share(0, level).wait_send()

        @pl.when((z > 0) & (level >= z))
        def _():
            share(1, level).wait_send()


def scatter_last(grad_qkv, grad_wout, small, parts, levels, ident):
    wide = parts.shape[0] * parts.shape[3]
    spots = levels * 2
    depth, width = grad_qkv.shape[1] // spots, grad_qkv.shape[2]
    out_rows, out_width = grad_wout.shape[0], grad_wout.shape[1] // spots
    low = grad_qkv.dtype
    vmem = pl.BlockSpec(memory_space=pltpu.VMEM)
    hbm = pl.BlockSpec(memory_space=pl.ANY)

    def pair(count):
        return [
            pltpu.VMEM((count, 3, depth, width), low),
            pltpu.VMEM((count, out_rows, out_width), low),
        ]

    return pl.pallas_call(
        functools.partial(scatter_last_kernel, levels),
        out_shape=[
            jax.ShapeDtypeStruct((3, depth, width), jnp.float32),
            jax.ShapeDtypeStruct((out_rows, out_width), jnp.float32),
            jax.ShapeDtypeStruct(small.shape, jnp.float32),
            jax.ShapeDtypeStruct((2, parts.shape[2], wide), jnp.float32),
            jax.ShapeDtypeStruct((wide, parts.shape[2]), jnp.float32),
        ],
        in_specs=[hbm, hbm, vmem, vmem],
        out_specs=[vmem] * 5,
        scratch_shapes=pair(levels)
        + pair(levels)
        + pair(levels + 1)
        + pair(levels)
        + [
            pltpu.VMEM((3,) + small.shape[1:], jnp.float32),
            pltpu.VMEM((2 + levels,) + small.shape[1:], jnp.float32),
            pltpu.SemaphoreType.DMA((4, levels)),
            pltpu.SemaphoreType.DMA((4, levels)),
            pltpu.SemaphoreType.DMA((4, levels)),
            pltpu.SemaphoreType.DMA((2, 4, levels)),
            pltpu.SemaphoreType.DMA((2, 4, levels)),
            pltpu.SemaphoreType.DMA((4 + 2 * levels,)),
            pltpu.SemaphoreType.DMA((4 + 2 * levels,)),
        ],
        compiler_params=pltpu.CompilerParams(
            collective_id=ident, has_side_effects=True, vmem_limit_bytes=48 * 2**20
        ),
        name="scatter_last",
    )(grad_qkv.reshape(3, spots, depth, width), grad_wout, small, parts)


PAIR = 256
SIDE = 128


def mul(a, b, ca, cb):
    return lax.dot_general(
        a, b, (((ca,), (cb,)), ((), ())), preferred_element_type=jnp.float32
    )


def swish_parts(gate, up):
    sig = jax.nn.sigmoid(gate)
    silu = gate * sig
    return silu * up, up * sig * (1.0 + gate * (1.0 - sig)), silu


def chosen(slot_row, capacity):
    ids = lax.broadcasted_iota(jnp.int32, (capacity, slot_row.shape[1]), 0)
    return (ids == slot_row).astype(jnp.float32).astype(jnp.bfloat16)


def rows_in_kernel(
    capacity, experts, spare, x, parts, extra, slots,
    hid, to_gate, to_up, stats, taken, weights, down,
):
    units = parts.shape[3]

    @pl.when(pl.program_id(0) == 0)
    def _():
        weights[...] = jnp.zeros_like(weights)
        down[...] = jnp.zeros_like(down)
        weights[:, PAIR + SIDE :] = extra[...]
        depth = parts.shape[2]
        for i in range(parts.shape[0]):
            span = slice(i * depth, (i + 1) * depth)
            weights[span, :units] = parts[i, 0]
            weights[span, PAIR : PAIR + units] = parts[i, 1]
            down[span, :units] = parts[i, 2]

    acc = jnp.dot(x[...], weights[...], preferred_element_type=jnp.float32)
    gate, up = acc[:, :PAIR], acc[:, PAIR:]
    hidden, by_gate, by_up = swish_parts(gate, up)
    hid[...] = hidden.astype(hid.dtype)
    to_gate[...] = by_gate
    to_up[...] = by_up
    side = up[:, SIDE:]
    lane = lax.broadcasted_iota(jnp.int32, side.shape, 1)
    routed = (lane >= spare) & (lane < spare + experts)
    powers = jnp.where(routed, jnp.exp(jnp.where(routed, side, 0.0)), 0.0)
    probs = powers / jnp.sum(powers, axis=1, keepdims=True)
    gated = (lane >= spare + experts) & (lane < spare + experts + 3)
    sig = jax.nn.sigmoid(jnp.sum(jnp.where(gated, side, 0.0), axis=1, keepdims=True))
    stats[...] = jnp.where(routed, probs, jnp.where(gated, sig, 0.0))
    tokens = slots.shape[2]
    for b in range(slots.shape[1]):
        pick = chosen(slots[0, b : b + 1], capacity)
        rows = jnp.dot(
            pick, x[b * tokens : (b + 1) * tokens], preferred_element_type=jnp.float32
        )
        taken[b * capacity : (b + 1) * capacity] = rows.astype(taken.dtype)


def resident(shape):
    zeros = (0,) * len(shape)
    return pl.BlockSpec(shape, lambda i: zeros, pipeline_mode=pl.Buffered(1))


def tiled(rows, width):
    return pl.BlockSpec((rows, width), lambda i: (i, 0))


def stacked(*shape):
    rest = (0,) * len(shape)
    return pl.BlockSpec((1,) + shape, lambda i: (i,) + rest)


def cost(*products):
    return pl.CostEstimate(
        flops=sum(2 * m * k * n for m, k, n in products),
        bytes_accessed=sum(2 * (m * k + k * n + m * n) for m, k, n in products),
        transcendentals=0,
    )


def params():
    return pltpu.CompilerParams(vmem_limit_bytes=60 * 2**20)


def forward_kernel(
    levels, capacity, experts, spare, tiles, x, parts, extra, slots, w_gu, w_down, late,
    hid, to_gate, to_up, stats, taken_out, weights, down, e_hid, e_gate, e_up, e_out, late_all,
    taken, own_sem, send_sems, recv_sems,
):
    step = pl.program_id(0)
    comm = gather_steps(levels, [late], [late_all], own_sem, send_sems, recv_sems)

    @pl.when(step == 0)
    def _():
        comm[0]()

    size = slots.shape[1] * capacity

    @pl.when(step < tiles)
    def _():
        rows_in_kernel(
            capacity, experts, spare, x, parts, extra, slots,
            hid, to_gate, to_up, stats, taken_out, weights, down,
        )
        taken[pl.ds(pl.multiple_of(step * size, size), size)] = taken_out[...]

    @pl.when(step >= tiles)
    def _():
        tile = e_out.shape[0]
        first = pl.multiple_of((step - tiles) * tile, tile)
        rows = taken[pl.ds(first, tile)]
        gate = jnp.dot(rows, w_gu[0], preferred_element_type=jnp.float32)
        up = jnp.dot(rows, w_gu[1], preferred_element_type=jnp.float32)
        hidden, by_gate, by_up = swish_parts(gate, up)
        low = hidden.astype(e_hid.dtype)
        e_hid[...] = low
        e_gate[...] = by_gate
        e_up[...] = by_up
        e_out[...] = jnp.dot(low, w_down[...], preferred_element_type=jnp.float32).astype(
            e_out.dtype
        )

    total = pl.num_programs(0)
    times = (3, 8, 9, 10, 11)
    for i, action in enumerate(comm[1:-1]):
        at = jnp.minimum(times[min(i, len(times) - 1)], total - 1)

        @pl.when(step == at)
        def _():
            action()

    @pl.when(step == total - 1)
    def _():
        comm[-1]()


def forward(x, parts, extra, slots, w_gu, w_down, late, capacity, experts, spare, levels, ident):
    count, tokens = slots.shape
    rows, width = x.shape
    units = w_down.shape[0]
    per = 4
    tile = per * tokens
    tiles = rows // tile
    e_rows, e_tile = count * capacity, 256

    def early(*shape):
        rest = (0,) * (len(shape) - 1)
        return pl.BlockSpec(shape, lambda i: (jnp.minimum(i, tiles - 1),) + rest)

    def after(*shape):
        rest = (0,) * (len(shape) - 1)
        return pl.BlockSpec(shape, lambda i: (jnp.maximum(i - tiles, 0),) + rest)

    hbm = pl.BlockSpec(memory_space=pl.ANY)
    low, wide = jnp.bfloat16, jnp.float32
    sems = (11, levels, 1)
    return pl.pallas_call(
        functools.partial(forward_kernel, levels, capacity, experts, spare, tiles),
        grid=(tiles + e_rows // e_tile,),
        in_specs=[
            early(tile, width),
            resident(parts.shape),
            resident(extra.shape),
            early(1, per, tokens),
            resident(w_gu.shape),
            resident(w_down.shape),
            hbm,
        ],
        out_specs=[
            early(tile, PAIR),
            early(tile, PAIR),
            early(tile, PAIR),
            early(tile, PAIR - SIDE),
            early(per * capacity, width),
            resident((width, 2 * PAIR)),
            resident((width, PAIR)),
            after(e_tile, units),
            after(e_tile, units),
            after(e_tile, units),
            after(e_tile, width),
            hbm,
        ],
        out_shape=[
            jax.ShapeDtypeStruct((rows, PAIR), low),
            jax.ShapeDtypeStruct((rows, PAIR), wide),
            jax.ShapeDtypeStruct((rows, PAIR), wide),
            jax.ShapeDtypeStruct((rows, PAIR - SIDE), wide),
            jax.ShapeDtypeStruct((e_rows, width), low),
            jax.ShapeDtypeStruct((width, 2 * PAIR), low),
            jax.ShapeDtypeStruct((width, PAIR), low),
            jax.ShapeDtypeStruct((e_rows, units), low),
            jax.ShapeDtypeStruct((e_rows, units), wide),
            jax.ShapeDtypeStruct((e_rows, units), wide),
            jax.ShapeDtypeStruct((e_rows, width), low),
            jax.ShapeDtypeStruct((count,) + late.shape, late.dtype),
        ],
        scratch_shapes=[
            pltpu.VMEM((e_rows, width), low),
            pltpu.SemaphoreType.DMA((1,)),
            pltpu.SemaphoreType.DMA(sems),
            pltpu.SemaphoreType.DMA(sems),
        ],
        compiler_params=pltpu.CompilerParams(
            collective_id=ident, has_side_effects=True, vmem_limit_bytes=60 * 2**20
        ),
        cost_estimate=cost(
            (rows, width, 2 * PAIR), (e_rows, width, 2 * units), (e_rows, units, width)
        ),
        name="forward",
    )(x, parts, extra, slots.reshape(count // per, per, tokens), w_gu, w_down, late)


def rows_out_kernel(
    capacity, lane, hid, w_down, stats, slots, share, routed, grad, out, dots
):
    tokens = slots.shape[2]
    whole = mul(hid[...], w_down[...], 1, 1)
    for b in range(slots.shape[1]):
        span = slice(b * tokens, (b + 1) * tokens)
        here = slice(b * capacity, (b + 1) * capacity)
        part = whole[span]
        pick = chosen(slots[0, b : b + 1], capacity)
        weighted = (share[here] * routed[here].astype(jnp.float32)).astype(jnp.bfloat16)
        spread = mul(pick, weighted, 0, 0)
        out[span] = (stats[span, lane : lane + 1] * part + spread).astype(out.dtype)
        inner = jnp.sum(grad[span].astype(jnp.float32) * part, axis=1, keepdims=True)
        dots[span] = jnp.broadcast_to(inner, (tokens, dots.shape[1]))


def rows_out(hid, w_down, stats, slots, share, routed, grad, capacity, lane):
    count, tokens = slots.shape
    rows, width = count * tokens, routed.shape[1]
    per = 4
    tile = per * tokens
    return pl.pallas_call(
        functools.partial(rows_out_kernel, capacity, lane),
        grid=(rows // tile,),
        in_specs=[
            tiled(tile, PAIR),
            resident(w_down.shape),
            tiled(tile, stats.shape[1]),
            stacked(per, tokens),
            tiled(per * capacity, 1),
            tiled(per * capacity, width),
            tiled(tile, width),
        ],
        out_specs=[tiled(tile, width), tiled(tile, 128)],
        out_shape=[
            jax.ShapeDtypeStruct((rows, width), jnp.bfloat16),
            jax.ShapeDtypeStruct((rows, 128), jnp.float32),
        ],
        compiler_params=params(),
        cost_estimate=cost((rows, PAIR, width), (rows, capacity, width)),
        name="rows_out",
    )(hid, w_down, stats, slots.reshape(count // per, per, tokens), share, routed, grad)


def expert_back_kernel(
    capacity, grad, slots, share, out, to_gate, to_up, w_gu, w_down, dout, dgu, din, dots
):
    tokens = slots.shape[2]
    size = slots.shape[1]
    taken = []
    for b in range(size):
        pick = chosen(slots[0, b : b + 1], capacity)
        taken.append(
            jnp.dot(
                pick, grad[b * tokens : (b + 1) * tokens], preferred_element_type=jnp.float32
            )
        )
    rows = jnp.concatenate(taken, axis=0)
    inner = jnp.sum(rows * out[...].astype(jnp.float32), axis=1, keepdims=True)
    dots[...] = jnp.broadcast_to(inner, dots.shape)
    low = (share[...] * rows).astype(jnp.bfloat16)
    dout[...] = low
    dhid = mul(low, w_down[...], 1, 1)
    dgate = (dhid * to_gate[...]).astype(jnp.bfloat16)
    dup = (dhid * to_up[...]).astype(jnp.bfloat16)
    dgu[0] = dgate
    dgu[1] = dup
    din[...] = (mul(dgate, w_gu[0], 1, 1) + mul(dup, w_gu[1], 1, 1)).astype(din.dtype)


def expert_back(grad, slots, share, out, to_gate, to_up, w_gu, w_down, capacity):
    count, tokens = slots.shape
    rows, width = out.shape
    units = w_down.shape[0]
    tile = 256
    per = tile // capacity
    return pl.pallas_call(
        functools.partial(expert_back_kernel, capacity),
        grid=(rows // tile,),
        in_specs=[
            tiled(per * tokens, width),
            stacked(per, tokens),
            tiled(tile, 1),
            tiled(tile, width),
            tiled(tile, units),
            tiled(tile, units),
            resident(w_gu.shape),
            resident(w_down.shape),
        ],
        out_specs=[
            tiled(tile, width),
            pl.BlockSpec((2, tile, units), lambda i: (0, i, 0)),
            tiled(tile, width),
            tiled(tile, 128),
        ],
        out_shape=[
            jax.ShapeDtypeStruct((rows, width), jnp.bfloat16),
            jax.ShapeDtypeStruct((2, rows, units), jnp.bfloat16),
            jax.ShapeDtypeStruct((rows, width), jnp.bfloat16),
            jax.ShapeDtypeStruct((rows, 128), jnp.float32),
        ],
        compiler_params=params(),
        cost_estimate=cost((rows, width, units), (rows, 2 * units, width)),
        name="expert_back",
    )(
        grad,
        slots.reshape(count // per, per, tokens),
        share,
        out,
        to_gate,
        to_up,
        w_gu,
        w_down,
    )


def rows_back_kernel(
    levels, capacity, lane, grad, x, stats, hid, to_gate, to_up, slots, din, weights, w_down, part,
    out, grad_parts, own, sum_weights, sum_down, *scratch
):
    step = pl.program_id(0)
    comm = scatter_steps(levels, part, own, *scratch)

    @pl.when(step == 0)
    def _():
        comm[0]()

    @pl.when(step == 0)
    def _():
        sum_weights[...] = jnp.zeros_like(sum_weights)
        sum_down[...] = jnp.zeros_like(sum_down)

    low = (stats[:, lane : lane + 1] * grad[...].astype(jnp.float32)).astype(jnp.bfloat16)
    dhid = mul(low, w_down[...], 1, 0)
    dgate = (dhid * to_gate[...]).astype(jnp.bfloat16)
    dup = (dhid * to_up[...]).astype(jnp.bfloat16)
    both_grads = jnp.concatenate([dgate, dup], axis=1)
    sum_weights[...] += mul(both_grads, x[...], 0, 0)
    whole = mul(both_grads, weights[...], 1, 1)
    sum_down[...] += mul(hid[...], low, 0, 0)
    tokens = slots.shape[2]
    for b in range(slots.shape[1]):
        span = slice(b * tokens, (b + 1) * tokens)
        pick = chosen(slots[0, b : b + 1], capacity)
        back = whole[span]
        spread = mul(pick, din[b * capacity : (b + 1) * capacity], 0, 0)
        out[span] = (back + spread).astype(out.dtype)

    @pl.when(step == pl.num_programs(0) - 1)
    def _():
        depth, units = grad_parts.shape[2:]
        for i in range(grad_parts.shape[0]):
            span = slice(i * depth, (i + 1) * depth)
            grads = sum_weights[:, span].T.astype(grad_parts.dtype)
            grad_parts[i, 0] = grads[:, :units]
            grad_parts[i, 1] = grads[:, PAIR : PAIR + units]
            grad_parts[i, 2] = sum_down[:, span].T.astype(grad_parts.dtype)[:, :units]

    last = pl.num_programs(0) - 1
    for i, action in enumerate(comm[1:]):
        @pl.when(step == jnp.minimum(i, last))
        def _():
            action()


def rows_back(
    grad, x, stats, hid, to_gate, to_up, slots, din, weights, w_down, part, parts_shape,
    capacity, lane, levels, ident,
):
    count, tokens = slots.shape
    rows, width = x.shape
    per = 4
    tile = per * tokens
    return pl.pallas_call(
        functools.partial(rows_back_kernel, levels, capacity, lane),
        grid=(rows // tile,),
        in_specs=[
            tiled(tile, width),
            tiled(tile, width),
            tiled(tile, stats.shape[1]),
            tiled(tile, PAIR),
            tiled(tile, PAIR),
            tiled(tile, PAIR),
            stacked(per, tokens),
            tiled(per * capacity, width),
            resident(weights.shape),
            resident(w_down.shape),
            pl.BlockSpec(memory_space=pl.ANY),
        ],
        out_specs=[tiled(tile, width), resident(parts_shape), resident(part.shape[1:])],
        out_shape=[
            jax.ShapeDtypeStruct((rows, width), jnp.bfloat16),
            jax.ShapeDtypeStruct(parts_shape, jnp.bfloat16),
            jax.ShapeDtypeStruct(part.shape[1:], jnp.float32),
        ],
        scratch_shapes=[
            pltpu.VMEM(weights.shape[::-1], jnp.float32),
            pltpu.VMEM(w_down.shape[::-1], jnp.float32),
        ]
        + scatter_scratch(levels, part.shape[1], width, part.dtype),
        compiler_params=pltpu.CompilerParams(
            collective_id=ident, has_side_effects=True, vmem_limit_bytes=67043328
        ),
        cost_estimate=cost((rows, width, PAIR), (rows, 2 * PAIR, width), (2 * PAIR, rows, width), (PAIR, rows, width)),
        name="rows_back",
    )(
        grad, x, stats, hid, to_gate, to_up,
        slots.reshape(count // per, per, tokens), din, weights, w_down, part,
    )


def gu_grad_kernel(x, dgu, out):
    rows = x[...].T
    for i in range(2):
        out[i] = jnp.dot(rows, dgu[i], preferred_element_type=jnp.float32)


def down_grad_kernel(hid, dout, out, turned):
    @pl.when(pl.program_id(0) == 0)
    def _():
        turned[...] = hid[...].T

    out[...] = jnp.dot(turned[...], dout[...], preferred_element_type=jnp.float32)


def expert_weight_grads(x, dgu, hid, dout):
    rows, width = x.shape
    units = hid.shape[1]
    tile = 256
    grad_gu = pl.pallas_call(
        gu_grad_kernel,
        grid=(width // tile,),
        in_specs=[pl.BlockSpec((rows, tile), lambda i: (0, i)), resident(dgu.shape)],
        out_specs=pl.BlockSpec((2, tile, units), lambda i: (0, i, 0)),
        out_shape=jax.ShapeDtypeStruct((2, width, units), jnp.float32),
        compiler_params=params(),
        cost_estimate=cost((width, rows, 2 * units)),
        name="expert_gu_grad",
    )(x, dgu)
    grad_down = pl.pallas_call(
        down_grad_kernel,
        grid=(width // tile,),
        in_specs=[resident(hid.shape), pl.BlockSpec((rows, tile), lambda i: (0, i))],
        out_specs=pl.BlockSpec((units, tile), lambda i: (0, i)),
        out_shape=jax.ShapeDtypeStruct((units, width), jnp.float32),
        scratch_shapes=[pltpu.VMEM((units, rows), jnp.bfloat16)],
        compiler_params=params(),
        cost_estimate=cost((units, rows, width)),
        name="expert_down_grad",
    )(hid, dout)
    return grad_gu, grad_down


def rope_tables(length, head_width):
    half_width = head_width // 2
    inverse = rope_base ** (-(jnp.arange(half_width, dtype=jnp.float32) * 2.0 / head_width))
    angles = jnp.arange(length, dtype=jnp.float32)[:, None] * inverse[None, :]
    angles = jnp.concatenate([angles, angles], axis=1)
    return (jnp.cos(angles), jnp.sin(angles))


def rotate(values, cosine, sine_tab):
    half_width = values.shape[-1] // 2
    turned = jnp.concatenate([-values[..., half_width:], values[..., :half_width]], axis=-1)
    return values * cosine[:, None, :] + turned * sine_tab[:, None, :]


def rotate_back(grad_vals, cosine, sine_tab):
    half_width = grad_vals.shape[-1] // 2
    scaled = grad_vals * sine_tab[:, None, :]
    turned = jnp.concatenate([scaled[..., half_width:], -scaled[..., :half_width]], axis=-1)
    return grad_vals * cosine[:, None, :] + turned


def norm_rows(values):
    scale_rows = lax.rsqrt(jnp.mean(values * values, axis=-1, keepdims=True) + eps)
    return (values * scale_rows, scale_rows)


def norm_back(grad_normed, unit_rows, scale_rows, gain_vec):
    inner_term = grad_normed * gain_vec
    return scale_rows * (
        inner_term - unit_rows * jnp.mean(inner_term * unit_rows, axis=-1, keepdims=True)
    )


def heads_dot(a, b, ca, cb, ha, hb):
    return lax.dot_general(
        a, b, (((ca,), (cb,)), ((ha,), (hb,))), preferred_element_type=jnp.float32
    )


def masked_scores(query_blk, keys_low, first_row, factor):
    scores = heads_dot(query_blk, keys_low, 2, 2, 1, 1) * factor
    row_ids = first_row + jnp.arange(query_blk.shape[0], dtype=jnp.int32)
    col_ids = jnp.arange(keys_low.shape[0], dtype=jnp.int32)
    causal = col_ids[None, :] <= row_ids[:, None]
    return jnp.where(causal[None], scores, -jnp.inf)


def silu_pair(gate_up):
    sig_gate = jax.nn.sigmoid(gate_up[0])
    return (gate_up[0] * sig_gate, sig_gate)


def swiglu_back(grad_hid, gate_up):
    silu_gate, sig_gate = silu_pair(gate_up)
    grad_gate = grad_hid * gate_up[1] * sig_gate * (1.0 + gate_up[0] * (1.0 - sig_gate))
    grad_up = grad_hid * silu_gate
    return jnp.stack([grad_gate, grad_up], axis=0).astype(jnp.bfloat16)


def pair_mul(rows, weights):
    return jnp.stack([mul(rows, w, 1, 0) for w in weights])


class Attention:
    def __init__(self, normed_group, full_qkv, b_qkv):
        self.normed, self.weights = normed_group, full_qkv
        self.length, self.width = normed_group.shape[0], full_qkv.shape[2]
        heads = self.width // HEAD_DIM
        self.factor = HEAD_DIM ** (-0.5)
        projected = pair_mul(normed_group, full_qkv) + b_qkv[:, None, :]
        self.cosine, self.sine_tab = rope_tables(self.length, HEAD_DIM)
        split = projected.reshape(3, self.length, heads, HEAD_DIM)
        self.queries = rotate(split[0], self.cosine, self.sine_tab).astype(jnp.bfloat16)
        self.keys = rotate(split[1], self.cosine, self.sine_tab).astype(jnp.bfloat16)
        self.values = split[2].astype(jnp.bfloat16)
        scores = masked_scores(self.queries, self.keys, 0, self.factor)
        row_max = jnp.max(scores, axis=-1, keepdims=True)
        weights = jnp.exp(scores - row_max)
        row_sum = jnp.sum(weights, axis=-1, keepdims=True)
        probs_low = (weights / row_sum).astype(jnp.bfloat16)
        mixed = heads_dot(probs_low, self.values, 2, 0, 0, 1).astype(jnp.bfloat16)
        self.mixed = mixed.swapaxes(0, 1).reshape(self.length, self.width)
        self.logsum = row_max + jnp.log(row_sum)

    def back(self, grad_mixed):
        grad_mixed = grad_mixed.reshape(self.length, -1, HEAD_DIM)
        scores = masked_scores(self.queries, self.keys, 0, self.factor)
        soft_probs = jnp.exp(scores - self.logsum)
        probs_low = soft_probs.astype(jnp.bfloat16)
        grad_values = heads_dot(probs_low, grad_mixed, 1, 0, 0, 1)
        grad_probs = heads_dot(grad_mixed, self.values, 2, 2, 1, 1)
        grad_scores = soft_probs * (
            grad_probs - jnp.sum(soft_probs * grad_probs, axis=-1, keepdims=True)
        )
        low = grad_scores.astype(jnp.bfloat16)
        grad_queries = heads_dot(low, self.keys, 2, 0, 0, 1) * self.factor
        grad_keys = heads_dot(low, self.queries, 1, 0, 0, 1) * self.factor
        grad_proj = jnp.stack(
            [
                rotate_back(grad_queries.swapaxes(0, 1), self.cosine, self.sine_tab),
                rotate_back(grad_keys.swapaxes(0, 1), self.cosine, self.sine_tab),
                grad_values.swapaxes(0, 1),
            ]
        )
        grad_proj = grad_proj.reshape(3, self.length, self.width).astype(jnp.bfloat16)
        bias_sum = jnp.sum(grad_proj, axis=1, dtype=jnp.float32)
        grad_weights = jnp.stack(
            [mul(self.normed, grad, 0, 0).astype(jnp.bfloat16) for grad in grad_proj]
        )
        normed_part = sum(mul(g, w, 1, 1) for g, w in zip(grad_proj, self.weights))
        return bias_sum, grad_weights, normed_part


def local(
    tokens,
    gain_attn,
    w_qkv,
    b_qkv,
    w_out,
    gain_ffn,
    w_router,
    shared_gate,
    w_shared_gu,
    w_shared_down,
    w_expert_gu,
    w_expert_down,
    routes,
    grad_out,
):
    own_rows, model_width = tokens.shape
    spots, lanes = lax.axis_size(EXPERT), lax.axis_size(SHARD)
    levels, devices = spots // 2, spots * lanes
    me = lax.axis_index(both)
    local_width = w_qkv.shape[2]
    experts_all = w_router.shape[1]
    capacity = 2 * own_rows * TOPK // experts_all
    units = w_shared_down.shape[0] // spots

    x_own = tokens.astype(jnp.float32)
    unit_one, scale_one = norm_rows(x_own)
    normed_one = (unit_one * gain_attn).astype(jnp.bfloat16)
    full_qkv, full_out, normed_group = gather_first(w_qkv, w_out, normed_one, levels, lanes, 1)
    w_shared_gu, w_shared_down, normed_group = lax.optimization_barrier(
        (w_shared_gu, w_shared_down, normed_group)
    )
    parts = jnp.concatenate([w_shared_gu, w_shared_down.T[None]])
    parts = parts.reshape(3, -1, spots, units).transpose(2, 0, 1, 3)
    parts = lax.all_to_all(parts, EXPERT, 0, 0)
    gate_terms, rest = [], shared_gate
    for _ in range(3):
        term = lax.reduce_precision(rest, 8, 7)
        gate_terms.append(term.astype(jnp.bfloat16))
        rest = rest - term
    extra = jnp.concatenate([w_router, jnp.stack(gate_terms, axis=1)], axis=1)
    spare = units - SIDE
    extra = jnp.pad(extra, ((0, 0), (spare, PAIR - SIDE - spare - extra.shape[1])))
    gate_lane = spare + experts_all

    attention = Attention(normed_group, full_qkv, b_qkv)
    attn_own = scatter_lanes(mul(attention.mixed, full_out, 1, 0), levels, lanes, 2)
    hidden_own = x_own + attn_own
    unit_two, scale_two = norm_rows(hidden_own)
    normed_own = (unit_two * gain_ffn).astype(jnp.bfloat16)
    route_rows = jnp.zeros((16, own_rows), jnp.int32).at[:TOPK].set(routes.T)
    normed_own, route_rows, parts = lax.optimization_barrier((normed_own, route_rows, parts))
    normed_all, routes_all = gather_all([normed_own, route_rows], levels, devices, 3)

    hits = (routes_all.reshape(devices, 16, own_rows)[:, :TOPK] == me).any(axis=1)
    slots = jnp.where(hits, jnp.cumsum(hits.astype(jnp.int32), axis=1) - 1, -1)
    placed = slots[:, None, :] == jnp.arange(capacity, dtype=jnp.int32)[None, :, None]
    placed = placed.astype(jnp.float32)
    (
        shared_hid, shared_gate_by, shared_up_by, stats, received, slice_gu, slice_down,
        expert_hid, gate_by, up_by, expert_out, grad_all,
    ) = forward(
        normed_all, parts, extra, slots, w_expert_gu[0], w_expert_down[0], grad_out,
        capacity, experts_all, spare, levels, 8,
    )
    grad_all = grad_all.reshape(-1, model_width)
    mine = (jnp.arange(stats.shape[1], dtype=jnp.int32) == spare + me).astype(jnp.float32)
    prob_mine = jnp.sum(stats * mine, axis=1).reshape(devices, 1, own_rows)
    share = jnp.sum(placed * prob_mine, axis=2).reshape(-1, 1)
    ffn_part, gate_dots = rows_out(
        shared_hid, slice_down, stats, slots, share, expert_out, grad_all, capacity, gate_lane
    )

    expert_dout, expert_dgu, expert_din, slot_dots = expert_back(
        grad_all, slots, share, expert_out, gate_by, up_by, w_expert_gu[0], w_expert_down[0], capacity
    )
    row_dots = jnp.sum(placed * slot_dots[:, 0].reshape(devices, capacity, 1), axis=1)
    dots = jnp.stack([row_dots, gate_dots[:, 0].reshape(devices, own_rows)], axis=1)
    dots = lax.all_to_all(dots, both, split_axis=0, concat_axis=0, tiled=True)
    normed_part, grad_parts, ffn_own = rows_back(
        grad_all, normed_all, stats, shared_hid, shared_gate_by, shared_up_by, slots,
        expert_din, slice_gu, slice_down, ffn_part.reshape(devices, own_rows, model_width),
        parts.shape, capacity, gate_lane, levels, 9,
    )
    grad_expert_gu, grad_expert_down = expert_weight_grads(
        received, expert_dgu, expert_hid, expert_dout
    )
    grad_normed_own = scatter_all(
        normed_part.reshape(devices, own_rows, model_width), levels, 4
    )

    grad_normed_own, grad_parts = lax.optimization_barrier((grad_normed_own, grad_parts))
    grad_parts = lax.all_to_all(grad_parts, EXPERT, 0, 0)

    stats_own = lax.dynamic_slice_in_dim(stats, me * own_rows, own_rows, 0)
    probs_own = stats_own[:, spare : spare + experts_all]
    sig_own = stats_own[:, gate_lane]
    grad_own = grad_out.astype(jnp.float32)
    grad_router_probs = dots[:, 0, :].T
    grad_logits = probs_own * (
        grad_router_probs - jnp.sum(probs_own * grad_router_probs, axis=-1, keepdims=True)
    )
    logits_low = grad_logits.astype(jnp.bfloat16)
    grad_router = mul(normed_own, logits_low, 0, 0)
    grad_gate_logit = jnp.sum(dots[:, 1, :], axis=0) * sig_own * (1.0 - sig_own)
    grad_gate_vec = jnp.sum(normed_own.astype(jnp.float32) * grad_gate_logit[:, None], axis=0)
    grad_normed_own = (
        grad_normed_own
        + mul(logits_low, w_router, 1, 1)
        + grad_gate_logit[:, None] * shared_gate[None, :]
    )
    grad_hidden_own = grad_own + norm_back(grad_normed_own, unit_two, scale_two, gain_ffn)
    grad_gain_two = jnp.sum(grad_normed_own * unit_two, axis=0)
    grad_hidden_low = gather_lanes(grad_hidden_own.astype(jnp.bfloat16), levels, lanes, 5)

    grad_mixed = mul(grad_hidden_low, full_out, 1, 1).astype(jnp.bfloat16)
    grad_bias_local, grad_qkv, normed_one_part = attention.back(grad_mixed)
    grad_wout = mul(attention.mixed, grad_hidden_low, 0, 0).astype(jnp.bfloat16)
    grad_normed_one = scatter_lanes(normed_one_part.astype(jnp.bfloat16), levels, lanes, 6)
    grad_tokens = grad_hidden_own + norm_back(grad_normed_one, unit_one, scale_one, gain_attn)
    grad_gain_one = jnp.sum(grad_normed_one * unit_one, axis=0)
    grad_bias_full = lax.dynamic_update_slice_in_dim(
        jnp.zeros((3, model_width), jnp.float32),
        grad_bias_local,
        lax.axis_index(SHARD) * local_width,
        1,
    )
    small = jnp.concatenate(
        [
            grad_router.reshape(-1, model_width),
            grad_gain_one[None],
            grad_gain_two[None],
            grad_gate_vec[None],
            grad_bias_full,
        ]
    )
    small_rows = small.shape[0]
    small = jnp.pad(small, ((0, -small_rows % 16), (0, 0))).reshape(2, -1, model_width)
    qkv_grad_part, wout_grad_part, small, shared_grad_in, shared_grad_down = scatter_last(
        grad_qkv, grad_wout, small, grad_parts, levels, 7
    )
    result = (hidden_own + ffn_own).astype(jnp.bfloat16)
    small = small.reshape(-1, model_width)[:small_rows]
    router_total = small[:-6].reshape(model_width, experts_all)
    gain_one_total, gain_two_total, gate_total = small[-6], small[-5], small[-4]
    bias_total = small[-3:]

    return (
        result,
        grad_tokens,
        gain_one_total,
        qkv_grad_part,
        bias_total,
        wout_grad_part,
        gain_two_total,
        router_total,
        gate_total,
        shared_grad_in,
        shared_grad_down,
        grad_expert_gu[None],
        grad_expert_down[None],
    )


def local_wide(
    tokens,
    gain_attn,
    w_qkv,
    b_qkv,
    w_out,
    gain_ffn,
    w_router,
    shared_gate,
    w_shared_gu,
    w_shared_down,
    w_expert_gu,
    w_expert_down,
    routes,
    grad_out,
):
    own_rows, model_width = tokens.shape
    shard_pos = lax.axis_index(SHARD)
    local_width = w_qkv.shape[2]
    experts_all = w_router.shape[1]
    capacity = 2 * own_rows * TOPK // experts_all
    first_own = shard_pos * own_rows

    def route_rows(block):
        block = block.reshape(experts_all, capacity, model_width)
        block = lax.all_to_all(block, both, split_axis=0, concat_axis=0, tiled=True)
        return block.reshape(-1, model_width)

    def group_rows(rows):
        return lax.all_gather(rows, SHARD, axis=0, tiled=True)

    def own(values):
        return lax.dynamic_slice_in_dim(values, first_own, own_rows, 0)

    full_qkv, full_out, full_sgu, full_sdown = (
        lax.all_gather(w_qkv, EXPERT, axis=1, tiled=True),
        lax.all_gather(w_out, EXPERT, axis=1, tiled=True),
        lax.all_gather(w_shared_gu, EXPERT, axis=1, tiled=True),
        lax.all_gather(w_shared_down, EXPERT, axis=1, tiled=True),
    )
    x_own = tokens.astype(jnp.float32)
    unit_one, scale_one = norm_rows(x_own)
    normed_one = (unit_one * gain_attn).astype(jnp.bfloat16)
    x_group, normed_group = group_rows(tokens), group_rows(normed_one)
    attention = Attention(normed_group, full_qkv, b_qkv)
    attn_group = lax.psum(mul(attention.mixed, full_out, 1, 0), SHARD)
    hidden_group = x_group.astype(jnp.float32) + attn_group
    unit_two, scale_two = norm_rows(hidden_group)
    normed_two = (unit_two * gain_ffn).astype(jnp.bfloat16)
    gate_logit = jnp.dot(normed_two.astype(jnp.float32), shared_gate, precision=highest)
    gate_sig = jax.nn.sigmoid(gate_logit)
    shared_gu = pair_mul(normed_two, full_sgu)
    shared_silu, shared_sig = silu_pair(shared_gu)
    shared_hid = (shared_silu * shared_gu[1]).astype(jnp.bfloat16)
    shared_part = mul(shared_hid, full_sdown, 1, 0)
    shared_own = lax.psum_scatter(
        shared_part.astype(jnp.bfloat16), SHARD, scatter_dimension=0, tiled=True
    ).astype(jnp.float32)
    normed_own, sig_own, hidden_own = own(normed_two), own(gate_sig), own(hidden_group)
    router_exp = jnp.exp(mul(normed_own, w_router, 1, 0))
    router_probs = router_exp / jnp.sum(router_exp, axis=-1, keepdims=True)
    expert_ids = jnp.arange(experts_all, dtype=jnp.int32)
    route_hits = (routes[:, :, None] == expert_ids[None, None, :]).astype(jnp.float32)
    picked = jnp.sum(router_probs[:, None, :] * route_hits, axis=-1)
    flat_routes = routes.reshape(-1)
    matches = (flat_routes[:, None] == expert_ids[None, :]).astype(jnp.int32)
    ranks = jnp.sum((jnp.cumsum(matches, axis=0) - 1) * matches, axis=1)
    targets = flat_routes * capacity + ranks

    def in_slots(rows):
        empty = jnp.zeros((experts_all * capacity, model_width), jnp.bfloat16)
        return empty.at[targets].set(rows)

    def at_slots(rows):
        return rows[targets].reshape(own_rows, TOPK, model_width).astype(jnp.float32)

    received = route_rows(in_slots(jnp.repeat(normed_own, TOPK, axis=0)))
    expert_gu = pair_mul(received, w_expert_gu[0])
    expert_silu, expert_sig = silu_pair(expert_gu)
    expert_hid = (expert_silu * expert_gu[1]).astype(jnp.bfloat16)
    expert_out = mul(expert_hid, w_expert_down[0], 1, 0).astype(jnp.bfloat16)
    route_out = at_slots(route_rows(expert_out))
    routed_own = jnp.sum(route_out * picked[:, :, None], axis=1)
    result = (hidden_own + sig_own[:, None] * shared_own + routed_own).astype(jnp.bfloat16)
    grad_own = grad_out.astype(jnp.float32)
    route_grad = (
        (picked[:, :, None] * grad_own[:, None, :]).reshape(-1, model_width).astype(jnp.bfloat16)
    )
    grad_recv = route_rows(in_slots(route_grad))
    grad_expert_down = mul(expert_hid, grad_recv, 0, 0)
    grad_expert_hid = mul(grad_recv, w_expert_down[0], 1, 1)
    expert_dgu = swiglu_back(grad_expert_hid, expert_gu)
    grad_expert_gu = jnp.stack([mul(received, grad, 0, 0) for grad in expert_dgu])
    expert_din = sum(mul(g, w, 1, 1) for g, w in zip(expert_dgu, w_expert_gu[0]))
    grad_normed_own = jnp.sum(at_slots(route_rows(expert_din.astype(jnp.bfloat16))), axis=1)
    grad_picked = jnp.sum(route_out * grad_own[:, None, :], axis=-1)
    grad_router_probs = jnp.sum(grad_picked[:, :, None] * route_hits, axis=1)
    grad_logits = router_probs * (
        grad_router_probs - jnp.sum(router_probs * grad_router_probs, axis=-1, keepdims=True)
    )
    logits_low = grad_logits.astype(jnp.bfloat16)
    grad_router = mul(normed_own, logits_low, 0, 0)
    grad_normed_own = grad_normed_own + mul(logits_low, w_router, 1, 1)
    grad_gate_logit = jnp.sum(grad_own * shared_own, axis=-1) * sig_own * (1.0 - sig_own)
    grad_gate_vec = jnp.dot(
        grad_gate_logit, normed_own.astype(jnp.float32), precision=highest
    )
    grad_normed_own = grad_normed_own + grad_gate_logit[:, None] * shared_gate[None, :]
    grad_group_f = group_rows(grad_out).astype(jnp.float32)
    grad_shared_out = (gate_sig[:, None] * grad_group_f).astype(jnp.bfloat16)
    grad_sdown = mul(shared_hid, grad_shared_out, 0, 0)
    grad_shared_hid = mul(grad_shared_out, full_sdown, 1, 1)
    shared_dgu = swiglu_back(grad_shared_hid, shared_gu)
    grad_sgu = jnp.stack([mul(normed_two, grad, 0, 0) for grad in shared_dgu])
    normed_part = sum(mul(g, w, 1, 1) for g, w in zip(shared_dgu, full_sgu))
    normed_part = lax.dynamic_update_slice_in_dim(
        normed_part, own(normed_part) + grad_normed_own, first_own, 0
    )
    grad_normed_two = lax.psum(normed_part, SHARD)
    grad_hidden = grad_group_f + norm_back(grad_normed_two, unit_two, scale_two, gain_ffn)
    grad_gain_two = jnp.sum(own(grad_normed_two * unit_two), axis=0)
    grad_hidden_low = grad_hidden.astype(jnp.bfloat16)
    grad_wout = mul(attention.mixed, grad_hidden_low, 0, 0)
    grad_mixed = mul(grad_hidden_low, full_out, 1, 1).astype(jnp.bfloat16)
    grad_bias_local, grad_qkv, normed_one_part = attention.back(grad_mixed)
    grad_normed_one = lax.psum_scatter(
        normed_one_part.astype(jnp.bfloat16), SHARD, scatter_dimension=0, tiled=True
    ).astype(jnp.float32)
    grad_tokens = own(grad_hidden) + norm_back(grad_normed_one, unit_one, scale_one, gain_attn)
    grad_gain_one = jnp.sum(grad_normed_one * unit_one, axis=0)
    grad_bias_full = lax.dynamic_update_slice_in_dim(
        jnp.zeros((3, model_width), jnp.float32), grad_bias_local, shard_pos * local_width, 1
    )

    def weight_sum(grad):
        low = grad.astype(jnp.bfloat16)
        total = lax.psum_scatter(low, EXPERT, scatter_dimension=1, tiled=True)
        return total.astype(jnp.float32)

    router_total, gain_one_total, gain_two_total, gate_total, bias_total = lax.psum(
        (grad_router, grad_gain_one, grad_gain_two, grad_gate_vec, grad_bias_full), both
    )
    return (
        result,
        grad_tokens,
        gain_one_total,
        weight_sum(grad_qkv),
        bias_total,
        weight_sum(grad_wout),
        gain_two_total,
        router_total,
        gate_total,
        weight_sum(grad_sgu),
        weight_sum(grad_sdown),
        grad_expert_gu[None],
        grad_expert_down[None],
    )


def local_by_size(*args):
    spots, lanes = lax.axis_size(EXPERT), lax.axis_size(SHARD)
    w_router, w_shared_down = args[6], args[9]
    units = w_shared_down.shape[0] // spots
    side = units - SIDE + w_router.shape[1] + 3
    fits = lanes == 4 and spots % 2 == 0 and spots * lanes <= 64
    fits = fits and SIDE <= units <= PAIR and side <= PAIR - SIDE
    return local(*args) if fits else local_wide(*args)


def solution(mesh):
    rows, columns = P(both, None), P(None, EXPERT, SHARD)
    weights = P(both, None, None, None), P(both, None, None)
    return jax.shard_map(
        local_by_size,
        mesh=mesh,
        in_specs=(
            rows, P(), columns, P(None, SHARD), P(SHARD, EXPERT), P(), P(), P(),
            columns, P(SHARD, EXPERT), *weights, rows, rows,
        ),
        out_specs=(
            rows, rows, P(), columns, P(), P(SHARD, EXPERT), P(), P(), P(),
            columns, P(SHARD, EXPERT), *weights,
        ),
        check_vma=False,
    )
```

```python
import functools

import jax
import jax.numpy as jnp
from jax import lax
from jax.experimental import pallas as pl
from jax.experimental.pallas import tpu as pltpu
from jax.sharding import PartitionSpec as P

HEAD_DIM = 128
TOPK = 4
EXPERT = "expert"
SHARD = "shard"
both = (EXPERT, SHARD)
eps = 1e-06
rope_base = 1000000.0
highest = lax.Precision.HIGHEST

MESH_ID = pl.DeviceIdType.MESH


class Place:
    def __init__(self, levels):
        self.levels = levels
        spot, lane = lax.axis_index(EXPERT), lax.axis_index(SHARD)
        self.z, self.y = spot // 2, spot % 2
        self.x, self.c = lane // 2, lane % 2

    def device(self, z=None, y=None, x=None, c=None):
        z = self.z if z is None else z
        y = self.y if y is None else y
        x = self.x if x is None else x
        c = self.c if c is None else c
        return {EXPERT: z * 2 + y, SHARD: x * 2 + c}

    def flat(self, z, y, x, c):
        return ((z * 2 + y) * 2 + x) * 2 + c


def greet(place, targets, ends):
    barrier = pltpu.get_barrier_semaphore()
    for target in targets:
        pl.semaphore_signal(barrier, inc=1, device_id=target, device_id_type=MESH_ID)
    count = len(targets)
    if ends:
        @pl.when(place.z > 0)
        def _():
            pl.semaphore_signal(
                barrier, inc=1, device_id=place.device(z=place.z - 1), device_id_type=MESH_ID
            )

        @pl.when(place.z < place.levels - 1)
        def _():
            pl.semaphore_signal(
                barrier, inc=1, device_id=place.device(z=place.z + 1), device_id_type=MESH_ID
            )

        inner = (place.z > 0).astype(jnp.int32) + (place.z < place.levels - 1).astype(jnp.int32)
        count = count + inner
    pl.semaphore_wait(barrier, count)


def gather_steps(levels, sources, outs, own_sem, send_sems, recv_sems):
    place = Place(levels)
    z, y, x, c = place.z, place.y, place.x, place.c
    top = levels - 1
    x_dev, y_dev, c_dev = place.device(x=1 - x), place.device(y=1 - y), place.device(c=1 - c)

    class Copies:
        def __init__(self, kind, level, refs_from, refs_to, device):
            self.each = [
                pltpu.make_async_remote_copy(
                    src_ref=ref,
                    dst_ref=dst,
                    send_sem=send_sems.at[kind, level, i],
                    recv_sem=recv_sems.at[kind, level, i],
                    device_id=device,
                    device_id_type=MESH_ID,
                )
                for i, (ref, dst) in enumerate(zip(refs_from, refs_to))
            ]

        def start(self):
            for one in self.each:
                one.start()

        def wait_recv(self):
            for one in self.each:
                one.wait_recv()

        def wait_send(self):
            for one in self.each:
                one.wait_send()

    copy = Copies

    def block(level, yy, xx, cc):
        return [out.at[place.flat(level, yy, xx, cc)] for out in outs]

    def part(level, yy, xx, cc, side):
        flat = place.flat(level, yy, xx, cc)
        return [
            out.at[flat, pl.ds(side * (out.shape[1] // 2), out.shape[1] // 2)] for out in outs
        ]

    UP, DOWN, XN, YN, DX, DY, CO, CX, CY, CDX, CDY = range(11)

    def dst_of(kind, level):
        if kind in (UP, DOWN):
            return block(level, y, x, c)
        if kind == XN:
            return block(level, y, 1 - x, c)
        if kind == YN:
            return block(level, 1 - y, x, c)
        if kind == DX:
            return part(level, 1 - y, 1 - x, c, 0)
        if kind == DY:
            return part(level, 1 - y, 1 - x, c, 1)
        if kind == CO:
            return block(level, y, x, 1 - c)
        if kind == CX:
            return block(level, y, 1 - x, 1 - c)
        if kind == CY:
            return block(level, 1 - y, x, 1 - c)
        if kind == CDX:
            return part(level, 1 - y, 1 - x, 1 - c, 0)
        return part(level, 1 - y, 1 - x, 1 - c, 1)

    def arrived(kind, level):
        ref = dst_of(kind, level)
        copy(kind, level, ref, ref, c_dev).wait_recv()

    def sent(kind, level, ref):
        copy(kind, level, ref, ref, c_dev).wait_send()

    def spread(level, ref):
        copy(XN, level, ref, block(level, y, x, c), x_dev).start()
        copy(YN, level, ref, block(level, y, x, c), y_dev).start()
        copy(CO, level, ref, block(level, y, x, c), c_dev).start()

    def at_distance(t, action):
        if t == 0:
            action(z)
            return

        @pl.when(z - t >= 0)
        def _():
            action(z - t)

        @pl.when(z + t <= top)
        def _():
            action(z + t)

    def from_neighbours(level):
        arrived(XN, level)
        ref = part(level, y, 1 - x, c, 1)
        copy(DY, level, ref, ref, y_dev).start()
        ref = block(level, y, 1 - x, c)
        copy(CX, level, ref, ref, c_dev).start()
        arrived(YN, level)
        ref = part(level, 1 - y, x, c, 0)
        copy(DX, level, ref, ref, x_dev).start()
        ref = block(level, 1 - y, x, c)
        copy(CY, level, ref, ref, c_dev).start()

    def from_diagonal(level):
        arrived(DX, level)
        ref = part(level, 1 - y, 1 - x, c, 0)
        copy(CDX, level, ref, ref, c_dev).start()
        arrived(DY, level)
        ref = part(level, 1 - y, 1 - x, c, 1)
        copy(CDY, level, ref, ref, c_dev).start()

    def start():
        greet(place, [x_dev, y_dev, c_dev], True)
        for i, (ref, dst) in enumerate(zip(sources, block(z, y, x, c))):
            pltpu.make_async_copy(ref, dst, own_sem.at[i]).start()

        @pl.when(z < top)
        def _():
            copy(UP, z, sources, block(z, y, x, c), place.device(z=z + 1)).start()

        @pl.when(z > 0)
        def _():
            copy(DOWN, z, sources, block(z, y, x, c), place.device(z=z - 1)).start()

        spread(z, sources)

    def onward(t):
        if t < levels:
            @pl.when(z - t >= 0)
            def _():
                level = z - t
                arrived(UP, level)
                ref = block(level, y, x, c)

                @pl.when(z < top)
                def _():
                    copy(UP, level, ref, ref, place.device(z=z + 1)).start()

                spread(level, ref)

            @pl.when(z + t <= top)
            def _():
                level = z + t
                arrived(DOWN, level)
                ref = block(level, y, x, c)

                @pl.when(z > 0)
                def _():
                    copy(DOWN, level, ref, ref, place.device(z=z - 1)).start()

                spread(level, ref)

        if t - 1 < levels:
            at_distance(t - 1, from_neighbours)
        if 0 <= t - 2 < levels:
            at_distance(t - 2, from_diagonal)


    def finish():
        for i, (ref, dst) in enumerate(zip(sources, block(z, y, x, c))):
            pltpu.make_async_copy(ref, dst, own_sem.at[i]).wait()
        for level in range(levels):
            for kind in (CO, CX, CY, CDX, CDY):
                arrived(kind, level)
            for kind in (XN, YN, DX, DY, CO, CX, CY, CDX, CDY):
                sent(kind, level, dst_of(kind, level))

            @pl.when((z < top) & (level <= z))
            def _():
                sent(UP, level, dst_of(UP, level))

            @pl.when((z > 0) & (level >= z))
            def _():
                sent(DOWN, level, dst_of(DOWN, level))

    middle = [functools.partial(onward, t) for t in range(1, levels + 2)]
    return [start] + middle + [finish]


def gather_kernel(levels, size, *refs):
    sources, outs = refs[:size], refs[size : 2 * size]
    for step in gather_steps(levels, sources, outs, *refs[2 * size :]):
        step()


def gather_all(arrays, levels, count, ident):
    size = len(arrays)
    outs = pl.pallas_call(
        functools.partial(gather_kernel, levels, size),
        out_shape=[jax.ShapeDtypeStruct((count,) + a.shape, a.dtype) for a in arrays],
        in_specs=[pl.BlockSpec(memory_space=pltpu.VMEM)] * size,
        out_specs=[pl.BlockSpec(memory_space=pl.ANY)] * size,
        scratch_shapes=[
            pltpu.SemaphoreType.DMA((size,)),
            pltpu.SemaphoreType.DMA((11, levels, size)),
            pltpu.SemaphoreType.DMA((11, levels, size)),
        ],
        compiler_params=pltpu.CompilerParams(collective_id=ident, has_side_effects=True),
        name="gather_all",
    )(*arrays)
    return [out.reshape((-1,) + out.shape[2:]) for out in outs]


def scatter_steps(
    levels, part, out, from_c, from_d, from_xy, from_z, load, load_sem, send_sem, recv_sem
):
    place = Place(levels)
    z, y, x, c = place.z, place.y, place.x, place.c
    top = levels - 1
    width = part.shape[-1]
    half = width // 2
    x_dev, y_dev, c_dev = place.device(x=1 - x), place.device(y=1 - y), place.device(c=1 - c)
    OWN, XN, YN, DIAG = 0, 1, 2, 3
    CORE, TOX, TOY, DX, DY, UP, DOWN = 0, 4, 5, 6, 7, 8, 9

    def columns(col):
        return {OWN: (y, x), XN: (y, 1 - x), YN: (1 - y, x), DIAG: (1 - y, 1 - x)}[col]

    def copy(kind, level, ref, dst, device):
        return pltpu.make_async_remote_copy(
            src_ref=ref,
            dst_ref=dst,
            send_sem=send_sem.at[kind, level],
            recv_sem=recv_sem.at[kind, level],
            device_id=device,
            device_id_type=MESH_ID,
        )

    def block(level, col, cc):
        yy, xx = columns(col)
        return part.at[place.flat(level, yy, xx, cc)]

    def core_copy(level, col):
        return copy(CORE + col, level, block(level, col, 1 - c), from_c.at[col, level], c_dev)

    def load_copy(level, col):
        return pltpu.make_async_copy(block(level, col, c), load.at[col, level], load_sem.at[col, level])

    def at_distance(t, action):
        if t == 0:
            action(z)
            return

        @pl.when(z - t >= 0)
        def _():
            action(z - t)

        @pl.when(z + t <= top)
        def _():
            action(z + t)

    def each_level(action):
        for t in range(levels - 1, -1, -1):
            at_distance(t, action)

    def start():
        greet(place, [x_dev, y_dev, c_dev], True)
        for col in (DIAG, XN, YN, OWN):
            def begin(level):
                core_copy(level, col).start()
                load_copy(level, col).start()
            each_level(begin)

    def strips(action):
        def step(i, carry):
            action(pl.ds(pl.multiple_of(i * 16, 16), 16))
            return carry
        lax.fori_loop(0, part.shape[1] // 16, step, 0)

    def f32(ref, *where):
        return ref[where].astype(jnp.float32)

    low, high = slice(0, half), slice(half, width)

    def diagonal(level):
        load_copy(level, DIAG).wait()
        core_copy(level, DIAG).wait_recv()

        def add(rows):
            load[DIAG, level, rows] = (
                f32(load, DIAG, level, rows) + f32(from_c, DIAG, level, rows)
            ).astype(load.dtype)
        strips(add)
        copy(DX, level, load.at[DIAG, level, :, low], from_d.at[0, level], x_dev).start()
        copy(DY, level, load.at[DIAG, level, :, high], from_d.at[1, level], y_dev).start()

    def sides(level):
        for col, kind, side, goes, device in ((XN, DY, 1, TOX, x_dev), (YN, DX, 0, TOY, y_dev)):
            load_copy(level, col).wait()
            core_copy(level, col).wait_recv()
            copy(kind, level, from_d.at[side, level], from_d.at[side, level], device).wait_recv()
            mine, other = (high, low) if side else (low, high)

            def add(rows):
                load[col, level, rows, mine] = (
                    f32(load, col, level, rows, mine)
                    + f32(from_c, col, level, rows, mine)
                    + f32(from_d, side, level, rows)
                ).astype(load.dtype)
                load[col, level, rows, other] = (
                    f32(load, col, level, rows, other) + f32(from_c, col, level, rows, other)
                ).astype(load.dtype)
            strips(add)
            copy(goes, level, load.at[col, level], from_xy.at[goes - TOX, level], device).start()

    def await_column(level):
        load_copy(level, OWN).wait()
        core_copy(level, OWN).wait_recv()
        copy(TOX, level, from_xy.at[0, level], from_xy.at[0, level], x_dev).wait_recv()
        copy(TOY, level, from_xy.at[1, level], from_xy.at[1, level], y_dev).wait_recv()

    def column(level, rows):
        return (
            f32(load, OWN, level, rows)
            + f32(from_c, OWN, level, rows)
            + f32(from_xy, 0, level, rows)
            + f32(from_xy, 1, level, rows)
        )


    def pass_on(level, kind, first, target, slot):
        await_column(level)

        @pl.when(first)
        def _():
            def add(rows):
                load[OWN, level, rows] = column(level, rows).astype(load.dtype)
            strips(add)

        @pl.when(jnp.logical_not(first))
        def _():
            copy(kind, level, from_z.at[level], from_z.at[level], c_dev).wait_recv()

            def add(rows):
                load[OWN, level, rows] = (
                    column(level, rows) + f32(from_z, level, rows)
                ).astype(load.dtype)
            strips(add)
        copy(kind, level, load.at[OWN, level], from_z.at[slot], target).start()

    def along_z(t):
        @pl.when(z + t <= top)
        def _():
            pass_on(z + t, UP, z == 0, place.device(z=z + 1), z + t)

        @pl.when(z - t >= 0)
        def _():
            slot = (z - t) if t > 1 else levels
            pass_on(z - t, DOWN, z == top, place.device(z=z - 1), slot)

    def finish_all():
        await_column(z)

        def add(rows):
            out[rows] = column(z, rows)
        strips(add)

        @pl.when(z > 0)
        def _():
            copy(UP, z, from_z.at[z], from_z.at[z], c_dev).wait_recv()

            def add(rows):
                out[rows] += f32(from_z, z, rows)
            strips(add)

        @pl.when(z < top)
        def _():
            copy(DOWN, z, from_z.at[levels], from_z.at[levels], c_dev).wait_recv()

            def add(rows):
                out[rows] += f32(from_z, levels, rows)
            strips(add)

        def finish(level):
            for col in (OWN, XN, YN, DIAG):
                core_copy(level, col).wait_send()
            copy(DX, level, from_d.at[0, level], from_d.at[0, level], x_dev).wait_send()
            copy(DY, level, from_d.at[1, level], from_d.at[1, level], y_dev).wait_send()
            copy(TOX, level, load.at[XN, level], from_xy.at[0, level], x_dev).wait_send()
            copy(TOY, level, load.at[YN, level], from_xy.at[1, level], y_dev).wait_send()

        for level in range(levels):
            finish(level)

            @pl.when(level > z)
            def _():
                copy(UP, level, load.at[OWN, level], from_z.at[level], c_dev).wait_send()

            @pl.when(level < z)
            def _():
                copy(DOWN, level, load.at[OWN, level], from_z.at[level], c_dev).wait_send()

    far = range(levels - 1, -1, -1)
    return (
        [start, functools.partial(each_level, diagonal)]
        + [functools.partial(at_distance, t, sides) for t in far]
        + [functools.partial(along_z, t) for t in far if t > 0]
        + [finish_all]
    )


def scatter_kernel(levels, *refs):
    for step in scatter_steps(levels, *refs):
        step()


def scatter_scratch(levels, rows, width, low):
    return [
        pltpu.VMEM((4, levels, rows, width), low),
        pltpu.VMEM((2, levels, rows, width // 2), low),
        pltpu.VMEM((2, levels, rows, width), low),
        pltpu.VMEM((levels + 1, rows, width), low),
        pltpu.VMEM((4, levels, rows, width), low),
        pltpu.SemaphoreType.DMA((4, levels)),
        pltpu.SemaphoreType.DMA((10, levels)),
        pltpu.SemaphoreType.DMA((10, levels)),
    ]


def scatter_all(part, levels, ident):
    count, rows, width = part.shape
    return pl.pallas_call(
        functools.partial(scatter_kernel, levels),
        out_shape=jax.ShapeDtypeStruct((rows, width), jnp.float32),
        in_specs=[pl.BlockSpec(memory_space=pl.ANY)],
        out_specs=pl.BlockSpec(memory_space=pltpu.VMEM),
        scratch_shapes=scatter_scratch(levels, rows, width, part.dtype),
        compiler_params=pltpu.CompilerParams(
            collective_id=ident, has_side_effects=True, vmem_limit_bytes=56 * 2**20
        ),
        name="scatter_all",
    )(part)


def lane_block(ref, index, width):
    return ref.at[:, pl.ds(pl.multiple_of(index * width, width), width)]


def gather_first_kernel(
    levels, qkv, wout, rows, qkv_all, wout_all, rows_all, own_sem, send_sem, recv_sem
):
    place = Place(levels)
    z, y, x, c = place.z, place.y, place.x, place.c
    top = levels - 1
    x_dev, y_dev, c_dev = place.device(x=1 - x), place.device(y=1 - y), place.device(c=1 - c)
    UP, DOWN, YN = range(3)
    pieces = 4
    row_kind = pieces * 3
    own_weights = [qkv.at[k] for k in range(3)] + [wout]

    def weight_refs(level, yy):
        spot = level * 2 + yy
        return [qkv_all.at[k, spot] for k in range(3)] + [
            lane_block(wout_all, spot, wout.shape[1])
        ]

    def copy(index, level, ref, dst, device):
        return pltpu.make_async_remote_copy(
            src_ref=ref,
            dst_ref=dst,
            send_sem=send_sem.at[index, level],
            recv_sem=recv_sem.at[index, level],
            device_id=device,
            device_id_type=MESH_ID,
        )

    def send(kind, level, refs, device, only=None):
        for i, (ref, dst) in enumerate(zip(refs, weight_refs(level, y))):
            if only in (None, i):
                copy(kind * pieces + i, level, ref, dst, device).start()

    def arrived(kind, level, only=None):
        for i, ref in enumerate(weight_refs(level, 1 - y if kind == YN else y)):
            if only in (None, i):
                copy(kind * pieces + i, level, ref, ref, c_dev).wait_recv()

    def sent(kind, level):
        for i, ref in enumerate(weight_refs(level, y)):
            copy(kind * pieces + i, level, ref, ref, c_dev).wait_send()

    greet(place, [x_dev, y_dev, c_dev], True)

    @pl.when(z < top)
    def _():
        send(UP, z, own_weights, place.device(z=z + 1))

    @pl.when(z > 0)
    def _():
        send(DOWN, z, own_weights, place.device(z=z - 1))

    send(YN, z, own_weights, y_dev)

    def row_ref(xx, cc):
        return rows_all.at[xx * 2 + cc]

    to_x = copy(row_kind, 0, rows, row_ref(x, c), x_dev)
    to_c = copy(row_kind, 1, rows, row_ref(x, c), c_dev)
    to_x.start()
    to_c.start()
    own = [
        pltpu.make_async_copy(ref, dst, own_sem.at[i])
        for i, (ref, dst) in enumerate(
            zip(own_weights + [rows], weight_refs(z, y) + [row_ref(x, c)])
        )
    ]
    for one in own:
        one.start()
    copy(row_kind, 0, rows, row_ref(1 - x, c), x_dev).wait_recv()
    on = copy(row_kind, 2, row_ref(1 - x, c), row_ref(1 - x, c), c_dev)
    on.start()

    def relay(kind, level, inner, target):
        for i in range(pieces):
            arrived(kind, level, i)

            @pl.when(inner)
            def _():
                send(kind, level, weight_refs(level, y), target, i)

            send(YN, level, weight_refs(level, y), y_dev, i)

    for t in range(1, levels):
        @pl.when(z - t >= 0)
        def _():
            relay(UP, z - t, z < top, place.device(z=z + 1))

        @pl.when(z + t <= top)
        def _():
            relay(DOWN, z + t, z > 0, place.device(z=z - 1))

    for one in own:
        one.wait()
    to_c.wait_recv()
    on.wait_recv()
    for one in (to_x, to_c, on):
        one.wait_send()
    for level in range(levels):
        arrived(YN, level)
        sent(YN, level)

        @pl.when((z < top) & (level <= z))
        def _():
            sent(UP, level)

        @pl.when((z > 0) & (level >= z))
        def _():
            sent(DOWN, level)


def gather_first(w_qkv, w_out, rows, levels, lanes, ident):
    spots = levels * 2
    qkv_all, wout_all, rows_all = pl.pallas_call(
        functools.partial(gather_first_kernel, levels),
        out_shape=[
            jax.ShapeDtypeStruct((3, spots) + w_qkv.shape[1:], w_qkv.dtype),
            jax.ShapeDtypeStruct((w_out.shape[0], spots * w_out.shape[1]), w_out.dtype),
            jax.ShapeDtypeStruct((lanes,) + rows.shape, rows.dtype),
        ],
        in_specs=[pl.BlockSpec(memory_space=pltpu.VMEM)] * 3,
        out_specs=[pl.BlockSpec(memory_space=pl.ANY)] * 3,
        scratch_shapes=[
            pltpu.SemaphoreType.DMA((5,)),
            pltpu.SemaphoreType.DMA((13, levels)),
            pltpu.SemaphoreType.DMA((13, levels)),
        ],
        compiler_params=pltpu.CompilerParams(collective_id=ident, has_side_effects=True),
        name="gather_first",
    )(w_qkv, w_out, rows)
    return (
        qkv_all.reshape(3, -1, w_qkv.shape[2]),
        wout_all,
        rows_all.reshape(-1, rows.shape[1]),
    )


def gather_lanes_kernel(levels, rows, rows_all, own_sem, send_sem, recv_sem):
    place = Place(levels)
    x, c = place.x, place.c
    x_dev, c_dev = place.device(x=1 - x), place.device(c=1 - c)

    def row_ref(xx, cc):
        return rows_all.at[xx * 2 + cc]

    def copy(index, ref, dst, device):
        return pltpu.make_async_remote_copy(
            src_ref=ref,
            dst_ref=dst,
            send_sem=send_sem.at[index],
            recv_sem=recv_sem.at[index],
            device_id=device,
            device_id_type=MESH_ID,
        )

    greet(place, [x_dev, c_dev], False)
    half = rows.shape[0] // 2
    parts = [pl.ds(0, half), pl.ds(half, half)]
    to_x = [copy(i, rows.at[p], row_ref(x, c).at[p], x_dev) for i, p in enumerate(parts)]
    to_c = copy(2, rows, row_ref(x, c), c_dev)
    own = pltpu.make_async_copy(rows, row_ref(x, c), own_sem)
    for one in to_x:
        one.start()
    to_c.start()
    own.start()
    on = []
    for i, p in enumerate(parts):
        to_x[i].wait_recv()
        on.append(copy(3 + i, row_ref(1 - x, c).at[p], row_ref(1 - x, c).at[p], c_dev))
        on[i].start()
    own.wait()
    to_c.wait()
    for one in on:
        one.wait()
    for one in to_x:
        one.wait_send()


def gather_lanes(rows, levels, lanes, ident):
    out = pl.pallas_call(
        functools.partial(gather_lanes_kernel, levels),
        out_shape=jax.ShapeDtypeStruct((lanes,) + rows.shape, rows.dtype),
        in_specs=[pl.BlockSpec(memory_space=pltpu.VMEM)],
        out_specs=pl.BlockSpec(memory_space=pltpu.VMEM),
        scratch_shapes=[
            pltpu.SemaphoreType.DMA,
            pltpu.SemaphoreType.DMA((5,)),
            pltpu.SemaphoreType.DMA((5,)),
        ],
        compiler_params=pltpu.CompilerParams(collective_id=ident, has_side_effects=True),
        name="gather_lanes",
    )(rows)
    return out.reshape(-1, rows.shape[1])


def scatter_lanes_kernel(levels, part, out, from_c, tx, from_x, send_sem, recv_sem):
    place = Place(levels)
    x, c = place.x, place.c
    x_dev, c_dev = place.device(x=1 - x), place.device(c=1 - c)
    rows = part.shape[1]
    pieces = 2
    size = rows // pieces

    def copy(index, ref, dst, device):
        return pltpu.make_async_remote_copy(
            src_ref=ref,
            dst_ref=dst,
            send_sem=send_sem.at[index],
            recv_sem=recv_sem.at[index],
            device_id=device,
            device_id_type=MESH_ID,
        )

    def strips(piece, action):
        def step(i, carry):
            action(pl.ds(pl.multiple_of(piece * size + i * 16, 16), 16))
            return carry
        lax.fori_loop(0, size // 16, step, 0)

    greet(place, [x_dev, c_dev], False)
    spans = [pl.ds(i * size, size) for i in range(pieces)]
    far = [
        copy(i, part.at[(1 - x) * 2 + 1 - c, p], from_c.at[0, p], c_dev)
        for i, p in enumerate(spans)
    ]
    near = copy(pieces, part.at[x * 2 + 1 - c], from_c.at[1], c_dev)
    for one in far:
        one.start()
    near.start()
    to_x = []
    for i, p in enumerate(spans):
        far[i].wait_recv()

        def add(span):
            tx[span] = (
                part[(1 - x) * 2 + c, span].astype(jnp.float32)
                + from_c[0, span].astype(jnp.float32)
            ).astype(tx.dtype)
        strips(i, add)
        to_x.append(copy(pieces + 1 + i, tx.at[p], from_x.at[p], x_dev))
        to_x[i].start()
    near.wait_recv()
    for i in range(pieces):
        to_x[i].wait_recv()

        def add(span):
            out[span] = (
                part[x * 2 + c, span].astype(jnp.float32)
                + from_c[1, span].astype(jnp.float32)
                + from_x[span].astype(jnp.float32)
            )
        strips(i, add)
    for one in far + [near] + to_x:
        one.wait_send()


def scatter_lanes(part, levels, lanes, ident):
    width = part.shape[1]
    rows = part.shape[0] // lanes
    low = part.dtype
    return pl.pallas_call(
        functools.partial(scatter_lanes_kernel, levels),
        out_shape=jax.ShapeDtypeStruct((rows, width), jnp.float32),
        in_specs=[pl.BlockSpec(memory_space=pltpu.VMEM)],
        out_specs=pl.BlockSpec(memory_space=pltpu.VMEM),
        scratch_shapes=[
            pltpu.VMEM((2, rows, width), low),
            pltpu.VMEM((rows, width), low),
            pltpu.VMEM((rows, width), low),
            pltpu.SemaphoreType.DMA((5,)),
            pltpu.SemaphoreType.DMA((5,)),
        ],
        compiler_params=pltpu.CompilerParams(collective_id=ident, has_side_effects=True),
        name="scatter_lanes",
    )(part.reshape(lanes, rows, width))


def scatter_last_kernel(
    levels, qkv, wout, small, parts, qkv_out, wout_out, small_out, gu_out, down_out,
    q_load, w_load, q_y, w_y, q_z, w_z, q_tx, w_tx, s_y, s_tx,
    load_sem, y_send, y_recv, z_send, z_recv, s_send, s_recv,
):
    place = Place(levels)
    z, y, x, c = place.z, place.y, place.x, place.c
    top = levels - 1
    x_dev, y_dev, c_dev = place.device(x=1 - x), place.device(y=1 - y), place.device(c=1 - c)
    out_width = w_y.shape[2]

    def remote(sends, recvs, where, ref, dst, device):
        return pltpu.make_async_remote_copy(
            src_ref=ref,
            dst_ref=dst,
            send_sem=sends.at[where],
            recv_sem=recvs.at[where],
            device_id=device,
            device_id_type=MESH_ID,
        )

    def block(level, yy):
        spot = level * 2 + yy
        return [qkv.at[k, spot] for k in range(3)] + [lane_block(wout, spot, out_width)]

    def pieces(q, w, level):
        return [q.at[level, k] for k in range(3)] + [w.at[level]]

    def load(level, i):
        ref = block(level, y)[i]
        dst = pieces(q_load, w_load, level)[i]
        return pltpu.make_async_copy(ref, dst, load_sem.at[i, level])

    def across(level, i):
        ref = block(level, 1 - y)[i]
        dst = pieces(q_y, w_y, level)[i]
        return remote(y_send, y_recv, (i, level), ref, dst, y_dev)

    def along(kind, level, slot, device, i):
        ref, dst = pieces(q_tx, w_tx, level)[i], pieces(q_z, w_z, slot)[i]
        return remote(z_send, z_recv, (kind, i, level), ref, dst, device)

    greet(place, [x_dev, y_dev, c_dev], True)

    s_first = remote(s_send, s_recv, 0, small.at[1 - c], s_y.at[0], c_dev)
    s_first.start()
    s_first.wait_recv()
    s_tx[0] = small[c] + s_y[0]
    s_yy = remote(s_send, s_recv, 1, s_tx.at[0], s_y.at[1], y_dev)
    s_yy.start()

    def each_level(action):
        for t in range(levels - 1, 0, -1):
            @pl.when(z - t >= 0)
            def _():
                action(z - t)

            @pl.when(z + t <= top)
            def _():
                action(z + t)

        action(z)

    def begin(level):
        for i in range(4):
            across(level, i).start()
            load(level, i).start()

    each_level(begin)

    s_yy.wait_recv()
    s_tx[2 + z] = s_tx[0] + s_y[1]

    def share(kind, level):
        ref = s_tx.at[2 + level]
        target = place.device(z=z + 1) if kind == 0 else place.device(z=z - 1)
        return remote(s_send, s_recv, 4 + kind * levels + level, ref, ref, target)

    @pl.when(z < top)
    def _():
        share(0, z).start()

    @pl.when(z > 0)
    def _():
        share(1, z).start()

    for t in range(1, levels):
        @pl.when(z - t >= 0)
        def _():
            share(0, z - t).wait_recv()

            @pl.when(z < top)
            def _():
                share(0, z - t).start()

        @pl.when(z + t <= top)
        def _():
            share(1, z + t).wait_recv()

            @pl.when(z > 0)
            def _():
                share(1, z + t).start()

    whole = s_tx[2]
    for level in range(1, levels):
        whole = whole + s_tx[2 + level]
    s_tx[1] = whole
    s_x = remote(s_send, s_recv, 2, s_tx.at[1], s_y.at[2], x_dev)
    s_x.start()

    units = parts.shape[3]
    for i in range(parts.shape[0]):
        span = slice(i * units, (i + 1) * units)
        for k in range(2):
            gu_out[k, :, span] = parts[i, k].astype(jnp.float32)
        down_out[span] = parts[i, 2].astype(jnp.float32).T

    def strips(ref, action):
        def step(i, carry):
            rows = pl.ds(pl.multiple_of(i * 16, 16), 16)
            ref[rows] = action(rows).astype(ref.dtype)
            return carry
        lax.fori_loop(0, ref.shape[0] // 16, step, 0)

    def f32(ref, rows):
        return ref[rows].astype(jnp.float32)

    def pass_on(level, kind, first, target, slot):
        mine, theirs = pieces(q_load, w_load, level), pieces(q_y, w_y, level)
        ahead, results = pieces(q_z, w_z, level), pieces(q_tx, w_tx, level)
        for i in range(4):
            load(level, i).wait()
            across(level, i).wait_recv()

            @pl.when(first)
            def _():
                strips(results[i], lambda rows: f32(mine[i], rows) + f32(theirs[i], rows))

            @pl.when(jnp.logical_not(first))
            def _():
                along(kind, level, level, c_dev, i).wait_recv()
                strips(
                    results[i],
                    lambda rows: f32(mine[i], rows) + f32(theirs[i], rows) + f32(ahead[i], rows),
                )
            along(kind, level, slot, target, i).start()

    for t in range(levels - 1, 0, -1):
        @pl.when(z + t <= top)
        def _():
            pass_on(z + t, 0, z == 0, place.device(z=z + 1), z + t)

        @pl.when(z - t >= 0)
        def _():
            slot = (z - t) if t > 1 else levels
            pass_on(z - t, 1, z == top, place.device(z=z - 1), slot)

        if t == levels - 1:
            s_x.wait_recv()
            small_out[c] = s_tx[1] + s_y[2]
            s_last = remote(s_send, s_recv, 3, small_out.at[c], small_out.at[c], c_dev)
            s_last.start()

    results = [qkv_out.at[k] for k in range(3)] + [wout_out]
    mine, theirs = pieces(q_load, w_load, z), pieces(q_y, w_y, z)
    for i in range(4):
        load(z, i).wait()
        across(z, i).wait_recv()
        strips(results[i], lambda rows: f32(mine[i], rows) + f32(theirs[i], rows))
    for kind, here, slot in ((0, z > 0, z), (1, z < top, levels)):
        ahead = pieces(q_z, w_z, slot)

        @pl.when(here)
        def _():
            for i in range(4):
                along(kind, z, slot, c_dev, i).wait_recv()
                strips(results[i], lambda rows: results[i][rows] + f32(ahead[i], rows))

    remote(s_send, s_recv, 3, small_out.at[1 - c], small_out.at[1 - c], c_dev).wait_recv()
    for one in (s_first, s_x, s_yy, s_last):
        one.wait_send()
    for level in range(levels):
        for i in range(4):
            across(level, i).wait_send()

        @pl.when(level > z)
        def _():
            for i in range(4):
                along(0, level, level, c_dev, i).wait_send()

        @pl.when(level < z)
        def _():
            for i in range(4):
                along(1, level, level, c_dev, i).wait_send()

        @pl.when((z < top) & (level <= z))
        def _():
            share(0, level).wait_send()

        @pl.when((z > 0) & (level >= z))
        def _():
            share(1, level).wait_send()


def scatter_last(grad_qkv, grad_wout, small, parts, levels, ident):
    wide = parts.shape[0] * parts.shape[3]
    spots = levels * 2
    depth, width = grad_qkv.shape[1] // spots, grad_qkv.shape[2]
    out_rows, out_width = grad_wout.shape[0], grad_wout.shape[1] // spots
    low = grad_qkv.dtype
    vmem = pl.BlockSpec(memory_space=pltpu.VMEM)
    hbm = pl.BlockSpec(memory_space=pl.ANY)

    def pair(count):
        return [
            pltpu.VMEM((count, 3, depth, width), low),
            pltpu.VMEM((count, out_rows, out_width), low),
        ]

    return pl.pallas_call(
        functools.partial(scatter_last_kernel, levels),
        out_shape=[
            jax.ShapeDtypeStruct((3, depth, width), jnp.float32),
            jax.ShapeDtypeStruct((out_rows, out_width), jnp.float32),
            jax.ShapeDtypeStruct(small.shape, jnp.float32),
            jax.ShapeDtypeStruct((2, parts.shape[2], wide), jnp.float32),
            jax.ShapeDtypeStruct((wide, parts.shape[2]), jnp.float32),
        ],
        in_specs=[hbm, hbm, vmem, vmem],
        out_specs=[vmem] * 5,
        scratch_shapes=pair(levels)
        + pair(levels)
        + pair(levels + 1)
        + pair(levels)
        + [
            pltpu.VMEM((3,) + small.shape[1:], jnp.float32),
            pltpu.VMEM((2 + levels,) + small.shape[1:], jnp.float32),
            pltpu.SemaphoreType.DMA((4, levels)),
            pltpu.SemaphoreType.DMA((4, levels)),
            pltpu.SemaphoreType.DMA((4, levels)),
            pltpu.SemaphoreType.DMA((2, 4, levels)),
            pltpu.SemaphoreType.DMA((2, 4, levels)),
            pltpu.SemaphoreType.DMA((4 + 2 * levels,)),
            pltpu.SemaphoreType.DMA((4 + 2 * levels,)),
        ],
        compiler_params=pltpu.CompilerParams(
            collective_id=ident, has_side_effects=True, vmem_limit_bytes=48 * 2**20
        ),
        name="scatter_last",
    )(grad_qkv.reshape(3, spots, depth, width), grad_wout, small, parts)


PAIR = 256
SIDE = 128


def mul(a, b, ca, cb):
    return lax.dot_general(
        a, b, (((ca,), (cb,)), ((), ())), preferred_element_type=jnp.float32
    )


def swish_parts(gate, up):
    sig = jax.nn.sigmoid(gate)
    silu = gate * sig
    return silu * up, up * sig * (1.0 + gate * (1.0 - sig)), silu


def chosen(slot_row, capacity):
    ids = lax.broadcasted_iota(jnp.int32, (capacity, slot_row.shape[1]), 0)
    return (ids == slot_row).astype(jnp.float32).astype(jnp.bfloat16)


def rows_in_kernel(
    capacity, experts, spare, x, parts, extra, slots,
    hid, to_gate, to_up, stats, taken, weights, down, share,
):
    units = parts.shape[3]

    @pl.when(pl.program_id(0) == 0)
    def _():
        weights[...] = jnp.zeros_like(weights)
        down[...] = jnp.zeros_like(down)
        weights[:, PAIR + SIDE :] = extra[...]
        depth = parts.shape[2]
        for i in range(parts.shape[0]):
            span = slice(i * depth, (i + 1) * depth)
            weights[span, :units] = parts[i, 0]
            weights[span, PAIR : PAIR + units] = parts[i, 1]
            down[span, :units] = parts[i, 2]

    acc = jnp.dot(x[...], weights[...], preferred_element_type=jnp.float32)
    gate, up = acc[:, :PAIR], acc[:, PAIR:]
    hidden, by_gate, by_up = swish_parts(gate, up)
    hid[...] = hidden.astype(hid.dtype)
    to_gate[...] = by_gate
    to_up[...] = by_up
    side = up[:, SIDE:]
    lane = lax.broadcasted_iota(jnp.int32, side.shape, 1)
    routed = (lane >= spare) & (lane < spare + experts)
    powers = jnp.where(routed, jnp.exp(jnp.where(routed, side, 0.0)), 0.0)
    probs = powers / jnp.sum(powers, axis=1, keepdims=True)
    gated = (lane >= spare + experts) & (lane < spare + experts + 3)
    sig = jax.nn.sigmoid(jnp.sum(jnp.where(gated, side, 0.0), axis=1, keepdims=True))
    stats[...] = jnp.where(routed, probs, jnp.where(gated, sig, 0.0))
    mine = jnp.sum(jnp.where(lane == spare + lax.axis_index(both), probs, 0.0), axis=1, keepdims=True)
    tokens = slots.shape[2]
    for b in range(slots.shape[1]):
        pick = chosen(slots[0, b : b + 1], capacity)
        rows = jnp.dot(
            pick, x[b * tokens : (b + 1) * tokens], preferred_element_type=jnp.float32
        )
        taken[b * capacity : (b + 1) * capacity] = rows.astype(taken.dtype)
        share[b * capacity : (b + 1) * capacity] = jnp.dot(
            pick.astype(jnp.float32), mine[b * tokens : (b + 1) * tokens],
            precision=highest, preferred_element_type=jnp.float32,
        )


def resident(shape):
    zeros = (0,) * len(shape)
    return pl.BlockSpec(shape, lambda i: zeros, pipeline_mode=pl.Buffered(1))


def tiled(rows, width):
    return pl.BlockSpec((rows, width), lambda i: (i, 0))


def stacked(*shape):
    rest = (0,) * len(shape)
    return pl.BlockSpec((1,) + shape, lambda i: (i,) + rest)


def cost(*products):
    return pl.CostEstimate(
        flops=sum(2 * m * k * n for m, k, n in products),
        bytes_accessed=sum(2 * (m * k + k * n + m * n) for m, k, n in products),
        transcendentals=0,
    )


def params():
    return pltpu.CompilerParams(vmem_limit_bytes=60 * 2**20)


def forward_kernel(
    levels, capacity, experts, spare, tiles, x, parts, extra, slots, w_gu, w_down, late,
    hid, to_gate, to_up, stats, taken_out, weights, down, e_hid, e_gate, e_up, e_out, share, part,
    late_all, taken, hid_all, stats_all, share_all, own_sem, send_sems, recv_sems,
):
    step = pl.program_id(0)
    comm = gather_steps(levels, [late], [late_all], own_sem, send_sems, recv_sems)

    @pl.when(step == 0)
    def _():
        comm[0]()

    size = slots.shape[1] * capacity

    @pl.when(step < tiles)
    def _():
        rows_in_kernel(
            capacity, experts, spare, x, parts, extra, slots,
            hid, to_gate, to_up, stats, taken_out, weights, down, share,
        )
        here = pl.ds(pl.multiple_of(step * size, size), size)
        taken[here] = taken_out[...]
        share_all[here] = share[...]
        here = pl.ds(pl.multiple_of(step * x.shape[0], x.shape[0]), x.shape[0])
        hid_all[here] = hid[...]
        stats_all[here] = stats[...]

    e_tiles = taken.shape[0] // e_out.shape[0]

    @pl.when((step >= tiles) & (step < tiles + e_tiles))
    def _():
        tile = e_out.shape[0]
        here = pl.ds(pl.multiple_of((step - tiles) * tile, tile), tile)
        rows = taken[here]
        gate = jnp.dot(rows, w_gu[0], preferred_element_type=jnp.float32)
        up = jnp.dot(rows, w_gu[1], preferred_element_type=jnp.float32)
        hidden, by_gate, by_up = swish_parts(gate, up)
        low = hidden.astype(e_hid.dtype)
        e_hid[...] = low
        e_gate[...] = by_gate
        e_up[...] = by_up
        result = jnp.dot(low, w_down[...], preferred_element_type=jnp.float32).astype(e_out.dtype)
        e_out[...] = result
        taken[here] = result

    @pl.when(step >= tiles + e_tiles)
    def _():
        tile, tokens = x.shape[0], slots.shape[2]
        at = step - tiles - e_tiles
        here = pl.ds(pl.multiple_of(at * tile, tile), tile)
        whole = mul(hid_all[here], down[...], 1, 1)
        sig = stats_all[here][:, spare + experts : spare + experts + 1]
        for b in range(slots.shape[1]):
            span = slice(b * tokens, (b + 1) * tokens)
            own = pl.ds(pl.multiple_of(at * size + b * capacity, capacity), capacity)
            pick = chosen(slots[0, b : b + 1], capacity)
            weighted = (share_all[own] * taken[own].astype(jnp.float32)).astype(jnp.bfloat16)
            part[span] = (sig[span] * whole[span] + mul(pick, weighted, 0, 0)).astype(part.dtype)

    total = pl.num_programs(0)
    times = (3, 8, 10, 12, 15)
    for i, action in enumerate(comm[1:-1]):
        at = jnp.minimum(times[min(i, len(times) - 1)], total - 1)

        @pl.when(step == at)
        def _():
            action()

    @pl.when(step == total - 1)
    def _():
        comm[-1]()


def forward(x, parts, extra, slots, w_gu, w_down, late, capacity, experts, spare, levels, ident):
    count, tokens = slots.shape
    rows, width = x.shape
    units = w_down.shape[0]
    per = 4
    tile = per * tokens
    tiles = rows // tile
    e_rows, e_tile = count * capacity, 256

    def early(*shape):
        rest = (0,) * (len(shape) - 1)
        return pl.BlockSpec(shape, lambda i: (jnp.minimum(i, tiles - 1),) + rest)

    def after(*shape):
        rest = (0,) * (len(shape) - 1)
        return pl.BlockSpec(
            shape, lambda i: (jnp.clip(i - tiles, 0, e_rows // e_tile - 1),) + rest
        )

    e_tiles = e_rows // e_tile

    def twice(*shape):
        rest = (0,) * (len(shape) - 1)

        def index(i):
            return (jnp.where(i < tiles, i, jnp.maximum(i - tiles - e_tiles, 0)),) + rest
        return pl.BlockSpec(shape, index)

    def final(*shape):
        rest = (0,) * (len(shape) - 1)
        return pl.BlockSpec(shape, lambda i: (jnp.maximum(i - tiles - e_tiles, 0),) + rest)

    hbm = pl.BlockSpec(memory_space=pl.ANY)
    low, wide = jnp.bfloat16, jnp.float32
    sems = (11, levels, 1)
    return pl.pallas_call(
        functools.partial(forward_kernel, levels, capacity, experts, spare, tiles),
        grid=(2 * tiles + e_tiles,),
        in_specs=[
            early(tile, width),
            resident(parts.shape),
            resident(extra.shape),
            twice(1, per, tokens),
            resident(w_gu.shape),
            resident(w_down.shape),
            hbm,
        ],
        out_specs=[
            early(tile, PAIR),
            early(tile, PAIR),
            early(tile, PAIR),
            early(tile, PAIR - SIDE),
            early(per * capacity, width),
            resident((width, 2 * PAIR)),
            resident((width, PAIR)),
            after(e_tile, units),
            after(e_tile, units),
            after(e_tile, units),
            after(e_tile, width),
            early(per * capacity, 1),
            final(tile, width),
            hbm,
        ],
        out_shape=[
            jax.ShapeDtypeStruct((rows, PAIR), low),
            jax.ShapeDtypeStruct((rows, PAIR), wide),
            jax.ShapeDtypeStruct((rows, PAIR), wide),
            jax.ShapeDtypeStruct((rows, PAIR - SIDE), wide),
            jax.ShapeDtypeStruct((e_rows, width), low),
            jax.ShapeDtypeStruct((width, 2 * PAIR), low),
            jax.ShapeDtypeStruct((width, PAIR), low),
            jax.ShapeDtypeStruct((e_rows, units), low),
            jax.ShapeDtypeStruct((e_rows, units), wide),
            jax.ShapeDtypeStruct((e_rows, units), wide),
            jax.ShapeDtypeStruct((e_rows, width), low),
            jax.ShapeDtypeStruct((e_rows, 1), wide),
            jax.ShapeDtypeStruct((rows, width), low),
            jax.ShapeDtypeStruct((count,) + late.shape, late.dtype),
        ],
        scratch_shapes=[
            pltpu.VMEM((e_rows, width), low),
            pltpu.VMEM((rows, PAIR), low),
            pltpu.VMEM((rows, PAIR - SIDE), wide),
            pltpu.VMEM((e_rows, 1), wide),
            pltpu.SemaphoreType.DMA((1,)),
            pltpu.SemaphoreType.DMA(sems),
            pltpu.SemaphoreType.DMA(sems),
        ],
        compiler_params=pltpu.CompilerParams(
            collective_id=ident, has_side_effects=True, vmem_limit_bytes=67043328
        ),
        cost_estimate=cost(
            (rows, width, 2 * PAIR), (e_rows, width, 2 * units), (e_rows, units, width)
        ),
        name="forward",
    )(x, parts, extra, slots.reshape(count // per, per, tokens), w_gu, w_down, late)


def expert_back_kernel(
    capacity, grad, slots, share, out, to_gate, to_up, w_gu, w_down, dout, dgu, din, dots
):
    tokens = slots.shape[2]
    size = slots.shape[1]
    taken = []
    for b in range(size):
        pick = chosen(slots[0, b : b + 1], capacity)
        taken.append(
            jnp.dot(
                pick, grad[b * tokens : (b + 1) * tokens], preferred_element_type=jnp.float32
            )
        )
    rows = jnp.concatenate(taken, axis=0)
    inner = jnp.sum(rows * out[...].astype(jnp.float32), axis=1, keepdims=True)
    dots[...] = jnp.broadcast_to(inner, dots.shape)
    low = (share[...] * rows).astype(jnp.bfloat16)
    dout[...] = low
    dhid = mul(low, w_down[...], 1, 1)
    dgate = (dhid * to_gate[...]).astype(jnp.bfloat16)
    dup = (dhid * to_up[...]).astype(jnp.bfloat16)
    dgu[0] = dgate
    dgu[1] = dup
    din[...] = (mul(dgate, w_gu[0], 1, 1) + mul(dup, w_gu[1], 1, 1)).astype(din.dtype)


def expert_back(grad, slots, share, out, to_gate, to_up, w_gu, w_down, capacity):
    count, tokens = slots.shape
    rows, width = out.shape
    units = w_down.shape[0]
    tile = 256
    per = tile // capacity
    return pl.pallas_call(
        functools.partial(expert_back_kernel, capacity),
        grid=(rows // tile,),
        in_specs=[
            tiled(per * tokens, width),
            stacked(per, tokens),
            tiled(tile, 1),
            tiled(tile, width),
            tiled(tile, units),
            tiled(tile, units),
            resident(w_gu.shape),
            resident(w_down.shape),
        ],
        out_specs=[
            tiled(tile, width),
            pl.BlockSpec((2, tile, units), lambda i: (0, i, 0)),
            tiled(tile, width),
            tiled(tile, 128),
        ],
        out_shape=[
            jax.ShapeDtypeStruct((rows, width), jnp.bfloat16),
            jax.ShapeDtypeStruct((2, rows, units), jnp.bfloat16),
            jax.ShapeDtypeStruct((rows, width), jnp.bfloat16),
            jax.ShapeDtypeStruct((rows, 128), jnp.float32),
        ],
        compiler_params=params(),
        cost_estimate=cost((rows, width, units), (rows, 2 * units, width)),
        name="expert_back",
    )(
        grad,
        slots.reshape(count // per, per, tokens),
        share,
        out,
        to_gate,
        to_up,
        w_gu,
        w_down,
    )


def rows_back_kernel(
    levels, capacity, lane, grad, x, stats, hid, to_gate, to_up, slots, din, weights, w_down, part,
    out, grad_parts, own, dots, sum_weights, sum_down, *scratch
):
    step = pl.program_id(0)
    comm = scatter_steps(levels, part, own, *scratch)

    @pl.when(step == 0)
    def _():
        comm[0]()

    @pl.when(step == 0)
    def _():
        sum_weights[...] = jnp.zeros_like(sum_weights)
        sum_down[...] = jnp.zeros_like(sum_down)

    low = (stats[:, lane : lane + 1] * grad[...].astype(jnp.float32)).astype(jnp.bfloat16)
    inner = jnp.sum(
        mul(grad[...], w_down[...], 1, 0) * hid[...].astype(jnp.float32), axis=1, keepdims=True
    )
    dots[...] = jnp.broadcast_to(inner, dots.shape)
    dhid = mul(low, w_down[...], 1, 0)
    dgate = (dhid * to_gate[...]).astype(jnp.bfloat16)
    dup = (dhid * to_up[...]).astype(jnp.bfloat16)
    both_grads = jnp.concatenate([dgate, dup], axis=1)
    sum_weights[...] += mul(both_grads, x[...], 0, 0)
    whole = mul(both_grads, weights[...], 1, 1)
    sum_down[...] += mul(hid[...], low, 0, 0)
    tokens = slots.shape[2]
    for b in range(slots.shape[1]):
        span = slice(b * tokens, (b + 1) * tokens)
        pick = chosen(slots[0, b : b + 1], capacity)
        back = whole[span]
        spread = mul(pick, din[b * capacity : (b + 1) * capacity], 0, 0)
        out[span] = (back + spread).astype(out.dtype)

    @pl.when(step == pl.num_programs(0) - 1)
    def _():
        depth, units = grad_parts.shape[2:]
        for i in range(grad_parts.shape[0]):
            span = slice(i * depth, (i + 1) * depth)
            grads = sum_weights[:, span].T.astype(grad_parts.dtype)
            grad_parts[i, 0] = grads[:, :units]
            grad_parts[i, 1] = grads[:, PAIR : PAIR + units]
            grad_parts[i, 2] = sum_down[:, span].T.astype(grad_parts.dtype)[:, :units]

    last = pl.num_programs(0) - 1
    for i, action in enumerate(comm[1:]):
        @pl.when(step == jnp.minimum(i, last))
        def _():
            action()


def rows_back(
    grad, x, stats, hid, to_gate, to_up, slots, din, weights, w_down, part, parts_shape,
    capacity, lane, levels, ident,
):
    count, tokens = slots.shape
    rows, width = x.shape
    per = 4
    tile = per * tokens
    return pl.pallas_call(
        functools.partial(rows_back_kernel, levels, capacity, lane),
        grid=(rows // tile,),
        in_specs=[
            tiled(tile, width),
            tiled(tile, width),
            tiled(tile, stats.shape[1]),
            tiled(tile, PAIR),
            tiled(tile, PAIR),
            tiled(tile, PAIR),
            stacked(per, tokens),
            tiled(per * capacity, width),
            resident(weights.shape),
            resident(w_down.shape),
            pl.BlockSpec(memory_space=pl.ANY),
        ],
        out_specs=[
            tiled(tile, width),
            resident(parts_shape),
            resident(part.shape[1:]),
            tiled(tile, 128),
        ],
        out_shape=[
            jax.ShapeDtypeStruct((rows, width), jnp.bfloat16),
            jax.ShapeDtypeStruct(parts_shape, jnp.bfloat16),
            jax.ShapeDtypeStruct(part.shape[1:], jnp.float32),
            jax.ShapeDtypeStruct((rows, 128), jnp.float32),
        ],
        scratch_shapes=[
            pltpu.VMEM(weights.shape[::-1], jnp.float32),
            pltpu.VMEM(w_down.shape[::-1], jnp.float32),
        ]
        + scatter_scratch(levels, part.shape[1], width, part.dtype),
        compiler_params=pltpu.CompilerParams(
            collective_id=ident, has_side_effects=True, vmem_limit_bytes=67043328
        ),
        cost_estimate=cost((rows, width, PAIR), (rows, 2 * PAIR, width), (2 * PAIR, rows, width), (PAIR, rows, width)),
        name="rows_back",
    )(
        grad, x, stats, hid, to_gate, to_up,
        slots.reshape(count // per, per, tokens), din, weights, w_down, part,
    )


def gu_grad_kernel(x, dgu, out):
    rows = x[...].T
    for i in range(2):
        out[i] = jnp.dot(rows, dgu[i], preferred_element_type=jnp.float32)


def down_grad_kernel(hid, dout, out, turned):
    @pl.when(pl.program_id(0) == 0)
    def _():
        turned[...] = hid[...].T

    out[...] = jnp.dot(turned[...], dout[...], preferred_element_type=jnp.float32)


def expert_weight_grads(x, dgu, hid, dout):
    rows, width = x.shape
    units = hid.shape[1]
    tile = 256
    grad_gu = pl.pallas_call(
        gu_grad_kernel,
        grid=(width // tile,),
        in_specs=[pl.BlockSpec((rows, tile), lambda i: (0, i)), resident(dgu.shape)],
        out_specs=pl.BlockSpec((2, tile, units), lambda i: (0, i, 0)),
        out_shape=jax.ShapeDtypeStruct((2, width, units), jnp.float32),
        compiler_params=params(),
        cost_estimate=cost((width, rows, 2 * units)),
        name="expert_gu_grad",
    )(x, dgu)
    grad_down = pl.pallas_call(
        down_grad_kernel,
        grid=(width // tile,),
        in_specs=[resident(hid.shape), pl.BlockSpec((rows, tile), lambda i: (0, i))],
        out_specs=pl.BlockSpec((units, tile), lambda i: (0, i)),
        out_shape=jax.ShapeDtypeStruct((units, width), jnp.float32),
        scratch_shapes=[pltpu.VMEM((units, rows), jnp.bfloat16)],
        compiler_params=params(),
        cost_estimate=cost((units, rows, width)),
        name="expert_down_grad",
    )(hid, dout)
    return grad_gu, grad_down


def rope_tables(length, head_width):
    half_width = head_width // 2
    inverse = rope_base ** (-(jnp.arange(half_width, dtype=jnp.float32) * 2.0 / head_width))
    angles = jnp.arange(length, dtype=jnp.float32)[:, None] * inverse[None, :]
    angles = jnp.concatenate([angles, angles], axis=1)
    return (jnp.cos(angles), jnp.sin(angles))


def rotate(values, cosine, sine_tab):
    half_width = values.shape[-1] // 2
    turned = jnp.concatenate([-values[..., half_width:], values[..., :half_width]], axis=-1)
    return values * cosine[:, None, :] + turned * sine_tab[:, None, :]


def rotate_back(grad_vals, cosine, sine_tab):
    half_width = grad_vals.shape[-1] // 2
    scaled = grad_vals * sine_tab[:, None, :]
    turned = jnp.concatenate([scaled[..., half_width:], -scaled[..., :half_width]], axis=-1)
    return grad_vals * cosine[:, None, :] + turned


def norm_rows(values):
    scale_rows = lax.rsqrt(jnp.mean(values * values, axis=-1, keepdims=True) + eps)
    return (values * scale_rows, scale_rows)


def norm_back(grad_normed, unit_rows, scale_rows, gain_vec):
    inner_term = grad_normed * gain_vec
    return scale_rows * (
        inner_term - unit_rows * jnp.mean(inner_term * unit_rows, axis=-1, keepdims=True)
    )


def heads_dot(a, b, ca, cb, ha, hb):
    return lax.dot_general(
        a, b, (((ca,), (cb,)), ((ha,), (hb,))), preferred_element_type=jnp.float32
    )


def masked_scores(query_blk, keys_low, first_row, factor):
    scores = heads_dot(query_blk, keys_low, 2, 2, 1, 1) * factor
    row_ids = first_row + jnp.arange(query_blk.shape[0], dtype=jnp.int32)
    col_ids = jnp.arange(keys_low.shape[0], dtype=jnp.int32)
    causal = col_ids[None, :] <= row_ids[:, None]
    return jnp.where(causal[None], scores, -jnp.inf)


def silu_pair(gate_up):
    sig_gate = jax.nn.sigmoid(gate_up[0])
    return (gate_up[0] * sig_gate, sig_gate)


def swiglu_back(grad_hid, gate_up):
    silu_gate, sig_gate = silu_pair(gate_up)
    grad_gate = grad_hid * gate_up[1] * sig_gate * (1.0 + gate_up[0] * (1.0 - sig_gate))
    grad_up = grad_hid * silu_gate
    return jnp.stack([grad_gate, grad_up], axis=0).astype(jnp.bfloat16)


def pair_mul(rows, weights):
    return jnp.stack([mul(rows, w, 1, 0) for w in weights])


class Attention:
    def __init__(self, normed_group, full_qkv, b_qkv):
        self.normed, self.weights = normed_group, full_qkv
        self.length, self.width = normed_group.shape[0], full_qkv.shape[2]
        heads = self.width // HEAD_DIM
        self.factor = HEAD_DIM ** (-0.5)
        projected = pair_mul(normed_group, full_qkv) + b_qkv[:, None, :]
        self.cosine, self.sine_tab = rope_tables(self.length, HEAD_DIM)
        split = projected.reshape(3, self.length, heads, HEAD_DIM)
        self.queries = rotate(split[0], self.cosine, self.sine_tab).astype(jnp.bfloat16)
        self.keys = rotate(split[1], self.cosine, self.sine_tab).astype(jnp.bfloat16)
        self.values = split[2].astype(jnp.bfloat16)
        scores = masked_scores(self.queries, self.keys, 0, self.factor)
        row_max = jnp.max(scores, axis=-1, keepdims=True)
        weights = jnp.exp(scores - row_max)
        row_sum = jnp.sum(weights, axis=-1, keepdims=True)
        probs_low = (weights / row_sum).astype(jnp.bfloat16)
        mixed = heads_dot(probs_low, self.values, 2, 0, 0, 1).astype(jnp.bfloat16)
        self.mixed = mixed.swapaxes(0, 1).reshape(self.length, self.width)
        self.logsum = row_max + jnp.log(row_sum)

    def back(self, grad_mixed):
        grad_mixed = grad_mixed.reshape(self.length, -1, HEAD_DIM)
        scores = masked_scores(self.queries, self.keys, 0, self.factor)
        soft_probs = jnp.exp(scores - self.logsum)
        probs_low = soft_probs.astype(jnp.bfloat16)
        grad_values = heads_dot(probs_low, grad_mixed, 1, 0, 0, 1)
        grad_probs = heads_dot(grad_mixed, self.values, 2, 2, 1, 1)
        grad_scores = soft_probs * (
            grad_probs - jnp.sum(soft_probs * grad_probs, axis=-1, keepdims=True)
        )
        low = grad_scores.astype(jnp.bfloat16)
        grad_queries = heads_dot(low, self.keys, 2, 0, 0, 1) * self.factor
        grad_keys = heads_dot(low, self.queries, 1, 0, 0, 1) * self.factor
        grad_proj = jnp.stack(
            [
                rotate_back(grad_queries.swapaxes(0, 1), self.cosine, self.sine_tab),
                rotate_back(grad_keys.swapaxes(0, 1), self.cosine, self.sine_tab),
                grad_values.swapaxes(0, 1),
            ]
        )
        grad_proj = grad_proj.reshape(3, self.length, self.width).astype(jnp.bfloat16)
        bias_sum = jnp.sum(grad_proj, axis=1, dtype=jnp.float32)
        grad_weights = jnp.stack(
            [mul(self.normed, grad, 0, 0).astype(jnp.bfloat16) for grad in grad_proj]
        )
        normed_part = sum(mul(g, w, 1, 1) for g, w in zip(grad_proj, self.weights))
        return bias_sum, grad_weights, normed_part


def local(
    tokens,
    gain_attn,
    w_qkv,
    b_qkv,
    w_out,
    gain_ffn,
    w_router,
    shared_gate,
    w_shared_gu,
    w_shared_down,
    w_expert_gu,
    w_expert_down,
    routes,
    grad_out,
):
    own_rows, model_width = tokens.shape
    spots, lanes = lax.axis_size(EXPERT), lax.axis_size(SHARD)
    levels, devices = spots // 2, spots * lanes
    me = lax.axis_index(both)
    local_width = w_qkv.shape[2]
    experts_all = w_router.shape[1]
    capacity = 2 * own_rows * TOPK // experts_all
    units = w_shared_down.shape[0] // spots

    x_own = tokens.astype(jnp.float32)
    unit_one, scale_one = norm_rows(x_own)
    normed_one = (unit_one * gain_attn).astype(jnp.bfloat16)
    full_qkv, full_out, normed_group = gather_first(w_qkv, w_out, normed_one, levels, lanes, 1)
    w_shared_gu, w_shared_down, normed_group = lax.optimization_barrier(
        (w_shared_gu, w_shared_down, normed_group)
    )
    parts = jnp.concatenate([w_shared_gu, w_shared_down.T[None]])
    parts = parts.reshape(3, -1, spots, units).transpose(2, 0, 1, 3)
    parts = lax.all_to_all(parts, EXPERT, 0, 0)
    gate_terms, rest = [], shared_gate
    for _ in range(3):
        term = lax.reduce_precision(rest, 8, 7)
        gate_terms.append(term.astype(jnp.bfloat16))
        rest = rest - term
    extra = jnp.concatenate([w_router, jnp.stack(gate_terms, axis=1)], axis=1)
    spare = units - SIDE
    extra = jnp.pad(extra, ((0, 0), (spare, PAIR - SIDE - spare - extra.shape[1])))
    gate_lane = spare + experts_all

    attention = Attention(normed_group, full_qkv, b_qkv)
    attn_own = scatter_lanes(mul(attention.mixed, full_out, 1, 0), levels, lanes, 2)
    hidden_own = x_own + attn_own
    unit_two, scale_two = norm_rows(hidden_own)
    normed_own = (unit_two * gain_ffn).astype(jnp.bfloat16)
    route_rows = jnp.zeros((16, own_rows), jnp.int32).at[:TOPK].set(routes.T)
    normed_own, route_rows, parts = lax.optimization_barrier((normed_own, route_rows, parts))
    normed_all, routes_all = gather_all([normed_own, route_rows], levels, devices, 3)

    hits = (routes_all.reshape(devices, 16, own_rows)[:, :TOPK] == me).any(axis=1)
    slots = jnp.where(hits, jnp.cumsum(hits.astype(jnp.int32), axis=1) - 1, -1)
    placed = slots[:, None, :] == jnp.arange(capacity, dtype=jnp.int32)[None, :, None]
    placed = placed.astype(jnp.float32)
    (
        shared_hid, shared_gate_by, shared_up_by, stats, received, slice_gu, slice_down,
        expert_hid, gate_by, up_by, expert_out, share, ffn_part, grad_all,
    ) = forward(
        normed_all, parts, extra, slots, w_expert_gu[0], w_expert_down[0], grad_out,
        capacity, experts_all, spare, levels, 8,
    )
    grad_all = grad_all.reshape(-1, model_width)
    expert_dout, expert_dgu, expert_din, slot_dots = expert_back(
        grad_all, slots, share, expert_out, gate_by, up_by, w_expert_gu[0], w_expert_down[0], capacity
    )
    normed_part, grad_parts, ffn_own, gate_dots = rows_back(
        grad_all, normed_all, stats, shared_hid, shared_gate_by, shared_up_by, slots,
        expert_din, slice_gu, slice_down, ffn_part.reshape(devices, own_rows, model_width),
        parts.shape, capacity, gate_lane, levels, 9,
    )
    row_dots = jnp.sum(placed * slot_dots[:, 0].reshape(devices, capacity, 1), axis=1)
    dots = jnp.stack([row_dots, gate_dots[:, 0].reshape(devices, own_rows)], axis=1)
    dots = lax.all_to_all(dots, both, split_axis=0, concat_axis=0, tiled=True)
    grad_expert_gu, grad_expert_down = expert_weight_grads(
        received, expert_dgu, expert_hid, expert_dout
    )
    grad_normed_own = scatter_all(
        normed_part.reshape(devices, own_rows, model_width), levels, 4
    )

    grad_normed_own, grad_parts = lax.optimization_barrier((grad_normed_own, grad_parts))
    grad_parts = lax.all_to_all(grad_parts, EXPERT, 0, 0)

    stats_own = lax.dynamic_slice_in_dim(stats, me * own_rows, own_rows, 0)
    probs_own = stats_own[:, spare : spare + experts_all]
    sig_own = stats_own[:, gate_lane]
    grad_own = grad_out.astype(jnp.float32)
    grad_router_probs = dots[:, 0, :].T
    grad_logits = probs_own * (
        grad_router_probs - jnp.sum(probs_own * grad_router_probs, axis=-1, keepdims=True)
    )
    logits_low = grad_logits.astype(jnp.bfloat16)
    grad_router = mul(normed_own, logits_low, 0, 0)
    grad_gate_logit = jnp.sum(dots[:, 1, :], axis=0) * sig_own * (1.0 - sig_own)
    grad_gate_vec = jnp.sum(normed_own.astype(jnp.float32) * grad_gate_logit[:, None], axis=0)
    grad_normed_own = (
        grad_normed_own
        + mul(logits_low, w_router, 1, 1)
        + grad_gate_logit[:, None] * shared_gate[None, :]
    )
    grad_hidden_own = grad_own + norm_back(grad_normed_own, unit_two, scale_two, gain_ffn)
    grad_gain_two = jnp.sum(grad_normed_own * unit_two, axis=0)
    grad_hidden_low = gather_lanes(grad_hidden_own.astype(jnp.bfloat16), levels, lanes, 5)

    grad_mixed = mul(grad_hidden_low, full_out, 1, 1).astype(jnp.bfloat16)
    grad_bias_local, grad_qkv, normed_one_part = attention.back(grad_mixed)
    grad_wout = mul(attention.mixed, grad_hidden_low, 0, 0).astype(jnp.bfloat16)
    grad_normed_one = scatter_lanes(normed_one_part.astype(jnp.bfloat16), levels, lanes, 6)
    grad_tokens = grad_hidden_own + norm_back(grad_normed_one, unit_one, scale_one, gain_attn)
    grad_gain_one = jnp.sum(grad_normed_one * unit_one, axis=0)
    grad_bias_full = lax.dynamic_update_slice_in_dim(
        jnp.zeros((3, model_width), jnp.float32),
        grad_bias_local,
        lax.axis_index(SHARD) * local_width,
        1,
    )
    small = jnp.concatenate(
        [
            grad_router.reshape(-1, model_width),
            grad_gain_one[None],
            grad_gain_two[None],
            grad_gate_vec[None],
            grad_bias_full,
        ]
    )
    small_rows = small.shape[0]
    small = jnp.pad(small, ((0, -small_rows % 16), (0, 0))).reshape(2, -1, model_width)
    qkv_grad_part, wout_grad_part, small, shared_grad_in, shared_grad_down = scatter_last(
        grad_qkv, grad_wout, small, grad_parts, levels, 7
    )
    result = (hidden_own + ffn_own).astype(jnp.bfloat16)
    small = small.reshape(-1, model_width)[:small_rows]
    router_total = small[:-6].reshape(model_width, experts_all)
    gain_one_total, gain_two_total, gate_total = small[-6], small[-5], small[-4]
    bias_total = small[-3:]

    return (
        result,
        grad_tokens,
        gain_one_total,
        qkv_grad_part,
        bias_total,
        wout_grad_part,
        gain_two_total,
        router_total,
        gate_total,
        shared_grad_in,
        shared_grad_down,
        grad_expert_gu[None],
        grad_expert_down[None],
    )


def local_wide(
    tokens,
    gain_attn,
    w_qkv,
    b_qkv,
    w_out,
    gain_ffn,
    w_router,
    shared_gate,
    w_shared_gu,
    w_shared_down,
    w_expert_gu,
    w_expert_down,
    routes,
    grad_out,
):
    own_rows, model_width = tokens.shape
    shard_pos = lax.axis_index(SHARD)
    local_width = w_qkv.shape[2]
    experts_all = w_router.shape[1]
    capacity = 2 * own_rows * TOPK // experts_all
    first_own = shard_pos * own_rows

    def route_rows(block):
        block = block.reshape(experts_all, capacity, model_width)
        block = lax.all_to_all(block, both, split_axis=0, concat_axis=0, tiled=True)
        return block.reshape(-1, model_width)

    def group_rows(rows):
        return lax.all_gather(rows, SHARD, axis=0, tiled=True)

    def own(values):
        return lax.dynamic_slice_in_dim(values, first_own, own_rows, 0)

    full_qkv, full_out, full_sgu, full_sdown = (
        lax.all_gather(w_qkv, EXPERT, axis=1, tiled=True),
        lax.all_gather(w_out, EXPERT, axis=1, tiled=True),
        lax.all_gather(w_shared_gu, EXPERT, axis=1, tiled=True),
        lax.all_gather(w_shared_down, EXPERT, axis=1, tiled=True),
    )
    x_own = tokens.astype(jnp.float32)
    unit_one, scale_one = norm_rows(x_own)
    normed_one = (unit_one * gain_attn).astype(jnp.bfloat16)
    x_group, normed_group = group_rows(tokens), group_rows(normed_one)
    attention = Attention(normed_group, full_qkv, b_qkv)
    attn_group = lax.psum(mul(attention.mixed, full_out, 1, 0), SHARD)
    hidden_group = x_group.astype(jnp.float32) + attn_group
    unit_two, scale_two = norm_rows(hidden_group)
    normed_two = (unit_two * gain_ffn).astype(jnp.bfloat16)
    gate_logit = jnp.dot(normed_two.astype(jnp.float32), shared_gate, precision=highest)
    gate_sig = jax.nn.sigmoid(gate_logit)
    shared_gu = pair_mul(normed_two, full_sgu)
    shared_silu, shared_sig = silu_pair(shared_gu)
    shared_hid = (shared_silu * shared_gu[1]).astype(jnp.bfloat16)
    shared_part = mul(shared_hid, full_sdown, 1, 0)
    shared_own = lax.psum_scatter(
        shared_part.astype(jnp.bfloat16), SHARD, scatter_dimension=0, tiled=True
    ).astype(jnp.float32)
    normed_own, sig_own, hidden_own = own(normed_two), own(gate_sig), own(hidden_group)
    router_exp = jnp.exp(mul(normed_own, w_router, 1, 0))
    router_probs = router_exp / jnp.sum(router_exp, axis=-1, keepdims=True)
    expert_ids = jnp.arange(experts_all, dtype=jnp.int32)
    route_hits = (routes[:, :, None] == expert_ids[None, None, :]).astype(jnp.float32)
    picked = jnp.sum(router_probs[:, None, :] * route_hits, axis=-1)
    flat_routes = routes.reshape(-1)
    matches = (flat_routes[:, None] == expert_ids[None, :]).astype(jnp.int32)
    ranks = jnp.sum((jnp.cumsum(matches, axis=0) - 1) * matches, axis=1)
    targets = flat_routes * capacity + ranks

    def in_slots(rows):
        empty = jnp.zeros((experts_all * capacity, model_width), jnp.bfloat16)
        return empty.at[targets].set(rows)

    def at_slots(rows):
        return rows[targets].reshape(own_rows, TOPK, model_width).astype(jnp.float32)

    received = route_rows(in_slots(jnp.repeat(normed_own, TOPK, axis=0)))
    expert_gu = pair_mul(received, w_expert_gu[0])
    expert_silu, expert_sig = silu_pair(expert_gu)
    expert_hid = (expert_silu * expert_gu[1]).astype(jnp.bfloat16)
    expert_out = mul(expert_hid, w_expert_down[0], 1, 0).astype(jnp.bfloat16)
    route_out = at_slots(route_rows(expert_out))
    routed_own = jnp.sum(route_out * picked[:, :, None], axis=1)
    result = (hidden_own + sig_own[:, None] * shared_own + routed_own).astype(jnp.bfloat16)
    grad_own = grad_out.astype(jnp.float32)
    route_grad = (
        (picked[:, :, None] * grad_own[:, None, :]).reshape(-1, model_width).astype(jnp.bfloat16)
    )
    grad_recv = route_rows(in_slots(route_grad))
    grad_expert_down = mul(expert_hid, grad_recv, 0, 0)
    grad_expert_hid = mul(grad_recv, w_expert_down[0], 1, 1)
    expert_dgu = swiglu_back(grad_expert_hid, expert_gu)
    grad_expert_gu = jnp.stack([mul(received, grad, 0, 0) for grad in expert_dgu])
    expert_din = sum(mul(g, w, 1, 1) for g, w in zip(expert_dgu, w_expert_gu[0]))
    grad_normed_own = jnp.sum(at_slots(route_rows(expert_din.astype(jnp.bfloat16))), axis=1)
    grad_picked = jnp.sum(route_out * grad_own[:, None, :], axis=-1)
    grad_router_probs = jnp.sum(grad_picked[:, :, None] * route_hits, axis=1)
    grad_logits = router_probs * (
        grad_router_probs - jnp.sum(router_probs * grad_router_probs, axis=-1, keepdims=True)
    )
    logits_low = grad_logits.astype(jnp.bfloat16)
    grad_router = mul(normed_own, logits_low, 0, 0)
    grad_normed_own = grad_normed_own + mul(logits_low, w_router, 1, 1)
    grad_gate_logit = jnp.sum(grad_own * shared_own, axis=-1) * sig_own * (1.0 - sig_own)
    grad_gate_vec = jnp.dot(
        grad_gate_logit, normed_own.astype(jnp.float32), precision=highest
    )
    grad_normed_own = grad_normed_own + grad_gate_logit[:, None] * shared_gate[None, :]
    grad_group_f = group_rows(grad_out).astype(jnp.float32)
    grad_shared_out = (gate_sig[:, None] * grad_group_f).astype(jnp.bfloat16)
    grad_sdown = mul(shared_hid, grad_shared_out, 0, 0)
    grad_shared_hid = mul(grad_shared_out, full_sdown, 1, 1)
    shared_dgu = swiglu_back(grad_shared_hid, shared_gu)
    grad_sgu = jnp.stack([mul(normed_two, grad, 0, 0) for grad in shared_dgu])
    normed_part = sum(mul(g, w, 1, 1) for g, w in zip(shared_dgu, full_sgu))
    normed_part = lax.dynamic_update_slice_in_dim(
        normed_part, own(normed_part) + grad_normed_own, first_own, 0
    )
    grad_normed_two = lax.psum(normed_part, SHARD)
    grad_hidden = grad_group_f + norm_back(grad_normed_two, unit_two, scale_two, gain_ffn)
    grad_gain_two = jnp.sum(own(grad_normed_two * unit_two), axis=0)
    grad_hidden_low = grad_hidden.astype(jnp.bfloat16)
    grad_wout = mul(attention.mixed, grad_hidden_low, 0, 0)
    grad_mixed = mul(grad_hidden_low, full_out, 1, 1).astype(jnp.bfloat16)
    grad_bias_local, grad_qkv, normed_one_part = attention.back(grad_mixed)
    grad_normed_one = lax.psum_scatter(
        normed_one_part.astype(jnp.bfloat16), SHARD, scatter_dimension=0, tiled=True
    ).astype(jnp.float32)
    grad_tokens = own(grad_hidden) + norm_back(grad_normed_one, unit_one, scale_one, gain_attn)
    grad_gain_one = jnp.sum(grad_normed_one * unit_one, axis=0)
    grad_bias_full = lax.dynamic_update_slice_in_dim(
        jnp.zeros((3, model_width), jnp.float32), grad_bias_local, shard_pos * local_width, 1
    )

    def weight_sum(grad):
        low = grad.astype(jnp.bfloat16)
        total = lax.psum_scatter(low, EXPERT, scatter_dimension=1, tiled=True)
        return total.astype(jnp.float32)

    router_total, gain_one_total, gain_two_total, gate_total, bias_total = lax.psum(
        (grad_router, grad_gain_one, grad_gain_two, grad_gate_vec, grad_bias_full), both
    )
    return (
        result,
        grad_tokens,
        gain_one_total,
        weight_sum(grad_qkv),
        bias_total,
        weight_sum(grad_wout),
        gain_two_total,
        router_total,
        gate_total,
        weight_sum(grad_sgu),
        weight_sum(grad_sdown),
        grad_expert_gu[None],
        grad_expert_down[None],
    )


def local_by_size(*args):
    spots, lanes = lax.axis_size(EXPERT), lax.axis_size(SHARD)
    w_router, w_shared_down = args[6], args[9]
    units = w_shared_down.shape[0] // spots
    side = units - SIDE + w_router.shape[1] + 3
    fits = lanes == 4 and spots % 2 == 0 and spots * lanes <= 64
    fits = fits and SIDE <= units <= PAIR and side <= PAIR - SIDE
    return local(*args) if fits else local_wide(*args)


def solution(mesh):
    rows, columns = P(both, None), P(None, EXPERT, SHARD)
    weights = P(both, None, None, None), P(both, None, None)
    return jax.shard_map(
        local_by_size,
        mesh=mesh,
        in_specs=(
            rows, P(), columns, P(None, SHARD), P(SHARD, EXPERT), P(), P(), P(),
            columns, P(SHARD, EXPERT), *weights, rows, rows,
        ),
        out_specs=(
            rows, rows, P(), columns, P(), P(SHARD, EXPERT), P(), P(), P(),
            columns, P(SHARD, EXPERT), *weights,
        ),
        check_vma=False,
    )
```

```python
import functools

import jax
import jax.numpy as jnp
from jax import lax
from jax.experimental import pallas as pl
from jax.experimental.pallas import tpu as pltpu
from jax.sharding import PartitionSpec as P

HEAD_DIM = 128
TOPK = 4
EXPERT = "expert"
SHARD = "shard"
both = (EXPERT, SHARD)
eps = 1e-06
rope_base = 1000000.0
highest = lax.Precision.HIGHEST

MESH_ID = pl.DeviceIdType.MESH


class Place:
    def __init__(self, levels):
        self.levels = levels
        spot, lane = lax.axis_index(EXPERT), lax.axis_index(SHARD)
        self.z, self.y = spot // 2, spot % 2
        self.x, self.c = lane // 2, lane % 2

    def device(self, z=None, y=None, x=None, c=None):
        z = self.z if z is None else z
        y = self.y if y is None else y
        x = self.x if x is None else x
        c = self.c if c is None else c
        return {EXPERT: z * 2 + y, SHARD: x * 2 + c}

    def flat(self, z, y, x, c):
        return ((z * 2 + y) * 2 + x) * 2 + c


def greet(place, targets, ends):
    barrier = pltpu.get_barrier_semaphore()
    for target in targets:
        pl.semaphore_signal(barrier, inc=1, device_id=target, device_id_type=MESH_ID)
    count = len(targets)
    if ends:
        @pl.when(place.z > 0)
        def _():
            pl.semaphore_signal(
                barrier, inc=1, device_id=place.device(z=place.z - 1), device_id_type=MESH_ID
            )

        @pl.when(place.z < place.levels - 1)
        def _():
            pl.semaphore_signal(
                barrier, inc=1, device_id=place.device(z=place.z + 1), device_id_type=MESH_ID
            )

        inner = (place.z > 0).astype(jnp.int32) + (place.z < place.levels - 1).astype(jnp.int32)
        count = count + inner
    pl.semaphore_wait(barrier, count)


def gather_steps(levels, sources, outs, own_sem, send_sems, recv_sems):
    place = Place(levels)
    z, y, x, c = place.z, place.y, place.x, place.c
    top = levels - 1
    x_dev, y_dev, c_dev = place.device(x=1 - x), place.device(y=1 - y), place.device(c=1 - c)

    class Copies:
        def __init__(self, kind, level, refs_from, refs_to, device):
            self.each = [
                pltpu.make_async_remote_copy(
                    src_ref=ref,
                    dst_ref=dst,
                    send_sem=send_sems.at[kind, level, i],
                    recv_sem=recv_sems.at[kind, level, i],
                    device_id=device,
                    device_id_type=MESH_ID,
                )
                for i, (ref, dst) in enumerate(zip(refs_from, refs_to))
            ]

        def start(self):
            for one in self.each:
                one.start()

        def wait_recv(self):
            for one in self.each:
                one.wait_recv()

        def wait_send(self):
            for one in self.each:
                one.wait_send()

    copy = Copies

    def block(level, yy, xx, cc):
        return [out.at[place.flat(level, yy, xx, cc)] for out in outs]

    def part(level, yy, xx, cc, side):
        flat = place.flat(level, yy, xx, cc)
        return [
            out.at[flat, pl.ds(side * (out.shape[1] // 2), out.shape[1] // 2)] for out in outs
        ]

    UP, DOWN, XN, YN, DX, DY, CO, CX, CY, CDX, CDY = range(11)

    def dst_of(kind, level):
        if kind in (UP, DOWN):
            return block(level, y, x, c)
        if kind == XN:
            return block(level, y, 1 - x, c)
        if kind == YN:
            return block(level, 1 - y, x, c)
        if kind == DX:
            return part(level, 1 - y, 1 - x, c, 0)
        if kind == DY:
            return part(level, 1 - y, 1 - x, c, 1)
        if kind == CO:
            return block(level, y, x, 1 - c)
        if kind == CX:
            return block(level, y, 1 - x, 1 - c)
        if kind == CY:
            return block(level, 1 - y, x, 1 - c)
        if kind == CDX:
            return part(level, 1 - y, 1 - x, 1 - c, 0)
        return part(level, 1 - y, 1 - x, 1 - c, 1)

    def arrived(kind, level):
        ref = dst_of(kind, level)
        copy(kind, level, ref, ref, c_dev).wait_recv()

    def sent(kind, level, ref):
        copy(kind, level, ref, ref, c_dev).wait_send()

    def spread(level, ref):
        copy(XN, level, ref, block(level, y, x, c), x_dev).start()
        copy(YN, level, ref, block(level, y, x, c), y_dev).start()
        copy(CO, level, ref, block(level, y, x, c), c_dev).start()

    def at_distance(t, action):
        if t == 0:
            action(z)
            return

        @pl.when(z - t >= 0)
        def _():
            action(z - t)

        @pl.when(z + t <= top)
        def _():
            action(z + t)

    def from_neighbours(level):
        arrived(XN, level)
        ref = part(level, y, 1 - x, c, 1)
        copy(DY, level, ref, ref, y_dev).start()
        ref = block(level, y, 1 - x, c)
        copy(CX, level, ref, ref, c_dev).start()
        arrived(YN, level)
        ref = part(level, 1 - y, x, c, 0)
        copy(DX, level, ref, ref, x_dev).start()
        ref = block(level, 1 - y, x, c)
        copy(CY, level, ref, ref, c_dev).start()

    def from_diagonal(level):
        arrived(DX, level)
        ref = part(level, 1 - y, 1 - x, c, 0)
        copy(CDX, level, ref, ref, c_dev).start()
        arrived(DY, level)
        ref = part(level, 1 - y, 1 - x, c, 1)
        copy(CDY, level, ref, ref, c_dev).start()

    def start():
        greet(place, [x_dev, y_dev, c_dev], True)
        for i, (ref, dst) in enumerate(zip(sources, block(z, y, x, c))):
            pltpu.make_async_copy(ref, dst, own_sem.at[i]).start()

        @pl.when(z < top)
        def _():
            copy(UP, z, sources, block(z, y, x, c), place.device(z=z + 1)).start()

        @pl.when(z > 0)
        def _():
            copy(DOWN, z, sources, block(z, y, x, c), place.device(z=z - 1)).start()

        spread(z, sources)

    def onward(t):
        if t < levels:
            @pl.when(z - t >= 0)
            def _():
                level = z - t
                arrived(UP, level)
                ref = block(level, y, x, c)

                @pl.when(z < top)
                def _():
                    copy(UP, level, ref, ref, place.device(z=z + 1)).start()

                spread(level, ref)

            @pl.when(z + t <= top)
            def _():
                level = z + t
                arrived(DOWN, level)
                ref = block(level, y, x, c)

                @pl.when(z > 0)
                def _():
                    copy(DOWN, level, ref, ref, place.device(z=z - 1)).start()

                spread(level, ref)

        if t - 1 < levels:
            at_distance(t - 1, from_neighbours)
        if 0 <= t - 2 < levels:
            at_distance(t - 2, from_diagonal)


    def finish():
        for i, (ref, dst) in enumerate(zip(sources, block(z, y, x, c))):
            pltpu.make_async_copy(ref, dst, own_sem.at[i]).wait()
        for level in range(levels):
            for kind in (CO, CX, CY, CDX, CDY):
                arrived(kind, level)
            for kind in (XN, YN, DX, DY, CO, CX, CY, CDX, CDY):
                sent(kind, level, dst_of(kind, level))

            @pl.when((z < top) & (level <= z))
            def _():
                sent(UP, level, dst_of(UP, level))

            @pl.when((z > 0) & (level >= z))
            def _():
                sent(DOWN, level, dst_of(DOWN, level))

    middle = [functools.partial(onward, t) for t in range(1, levels + 2)]
    return [start] + middle + [finish]


def gather_kernel(levels, size, *refs):
    sources, outs = refs[:size], refs[size : 2 * size]
    for step in gather_steps(levels, sources, outs, *refs[2 * size :]):
        step()


def gather_all(arrays, levels, count, ident):
    size = len(arrays)
    outs = pl.pallas_call(
        functools.partial(gather_kernel, levels, size),
        out_shape=[jax.ShapeDtypeStruct((count,) + a.shape, a.dtype) for a in arrays],
        in_specs=[pl.BlockSpec(memory_space=pltpu.VMEM)] * size,
        out_specs=[pl.BlockSpec(memory_space=pl.ANY)] * size,
        scratch_shapes=[
            pltpu.SemaphoreType.DMA((size,)),
            pltpu.SemaphoreType.DMA((11, levels, size)),
            pltpu.SemaphoreType.DMA((11, levels, size)),
        ],
        compiler_params=pltpu.CompilerParams(collective_id=ident, has_side_effects=True),
        name="gather_all",
    )(*arrays)
    return [out.reshape((-1,) + out.shape[2:]) for out in outs]


def scatter_steps(
    levels, part, out, from_c, from_d, from_xy, from_z, load, load_sem, send_sem, recv_sem
):
    place = Place(levels)
    z, y, x, c = place.z, place.y, place.x, place.c
    top = levels - 1
    width = part.shape[-1]
    half = width // 2
    x_dev, y_dev, c_dev = place.device(x=1 - x), place.device(y=1 - y), place.device(c=1 - c)
    OWN, XN, YN, DIAG = 0, 1, 2, 3
    CORE, TOX, TOY, DX, DY, UP, DOWN = 0, 4, 5, 6, 7, 8, 9

    def columns(col):
        return {OWN: (y, x), XN: (y, 1 - x), YN: (1 - y, x), DIAG: (1 - y, 1 - x)}[col]

    def copy(kind, level, ref, dst, device):
        return pltpu.make_async_remote_copy(
            src_ref=ref,
            dst_ref=dst,
            send_sem=send_sem.at[kind, level],
            recv_sem=recv_sem.at[kind, level],
            device_id=device,
            device_id_type=MESH_ID,
        )

    def block(level, col, cc):
        yy, xx = columns(col)
        return part.at[place.flat(level, yy, xx, cc)]

    def core_copy(level, col):
        return copy(CORE + col, level, block(level, col, 1 - c), from_c.at[col, level], c_dev)

    def load_copy(level, col):
        return pltpu.make_async_copy(block(level, col, c), load.at[col, level], load_sem.at[col, level])

    def at_distance(t, action):
        if t == 0:
            action(z)
            return

        @pl.when(z - t >= 0)
        def _():
            action(z - t)

        @pl.when(z + t <= top)
        def _():
            action(z + t)

    def each_level(action):
        for t in range(levels - 1, -1, -1):
            at_distance(t, action)

    def start():
        greet(place, [x_dev, y_dev, c_dev], True)
        for col in (DIAG, XN, YN, OWN):
            def begin(level):
                core_copy(level, col).start()
                load_copy(level, col).start()
            each_level(begin)

    def strips(action):
        def step(i, carry):
            action(pl.ds(pl.multiple_of(i * 16, 16), 16))
            return carry
        lax.fori_loop(0, part.shape[1] // 16, step, 0)

    def f32(ref, *where):
        return ref[where].astype(jnp.float32)

    low, high = slice(0, half), slice(half, width)

    def diagonal(level):
        load_copy(level, DIAG).wait()
        core_copy(level, DIAG).wait_recv()

        def add(rows):
            load[DIAG, level, rows] = (
                f32(load, DIAG, level, rows) + f32(from_c, DIAG, level, rows)
            ).astype(load.dtype)
        strips(add)
        copy(DX, level, load.at[DIAG, level, :, low], from_d.at[0, level], x_dev).start()
        copy(DY, level, load.at[DIAG, level, :, high], from_d.at[1, level], y_dev).start()

    def sides(level):
        for col, kind, side, goes, device in ((XN, DY, 1, TOX, x_dev), (YN, DX, 0, TOY, y_dev)):
            load_copy(level, col).wait()
            core_copy(level, col).wait_recv()
            copy(kind, level, from_d.at[side, level], from_d.at[side, level], device).wait_recv()
            mine, other = (high, low) if side else (low, high)

            def add(rows):
                load[col, level, rows, mine] = (
                    f32(load, col, level, rows, mine)
                    + f32(from_c, col, level, rows, mine)
                    + f32(from_d, side, level, rows)
                ).astype(load.dtype)
                load[col, level, rows, other] = (
                    f32(load, col, level, rows, other) + f32(from_c, col, level, rows, other)
                ).astype(load.dtype)
            strips(add)
            copy(goes, level, load.at[col, level], from_xy.at[goes - TOX, level], device).start()

    def await_column(level):
        load_copy(level, OWN).wait()
        core_copy(level, OWN).wait_recv()
        copy(TOX, level, from_xy.at[0, level], from_xy.at[0, level], x_dev).wait_recv()
        copy(TOY, level, from_xy.at[1, level], from_xy.at[1, level], y_dev).wait_recv()

    def column(level, rows):
        return (
            f32(load, OWN, level, rows)
            + f32(from_c, OWN, level, rows)
            + f32(from_xy, 0, level, rows)
            + f32(from_xy, 1, level, rows)
        )


    def pass_on(level, kind, first, target, slot):
        await_column(level)

        @pl.when(first)
        def _():
            def add(rows):
                load[OWN, level, rows] = column(level, rows).astype(load.dtype)
            strips(add)

        @pl.when(jnp.logical_not(first))
        def _():
            copy(kind, level, from_z.at[level], from_z.at[level], c_dev).wait_recv()

            def add(rows):
                load[OWN, level, rows] = (
                    column(level, rows) + f32(from_z, level, rows)
                ).astype(load.dtype)
            strips(add)
        copy(kind, level, load.at[OWN, level], from_z.at[slot], target).start()

    def along_z(t):
        @pl.when(z + t <= top)
        def _():
            pass_on(z + t, UP, z == 0, place.device(z=z + 1), z + t)

        @pl.when(z - t >= 0)
        def _():
            slot = (z - t) if t > 1 else levels
            pass_on(z - t, DOWN, z == top, place.device(z=z - 1), slot)

    def finish_all():
        await_column(z)

        def add(rows):
            out[rows] = column(z, rows)
        strips(add)

        @pl.when(z > 0)
        def _():
            copy(UP, z, from_z.at[z], from_z.at[z], c_dev).wait_recv()

            def add(rows):
                out[rows] += f32(from_z, z, rows)
            strips(add)

        @pl.when(z < top)
        def _():
            copy(DOWN, z, from_z.at[levels], from_z.at[levels], c_dev).wait_recv()

            def add(rows):
                out[rows] += f32(from_z, levels, rows)
            strips(add)

        def finish(level):
            for col in (OWN, XN, YN, DIAG):
                core_copy(level, col).wait_send()
            copy(DX, level, from_d.at[0, level], from_d.at[0, level], x_dev).wait_send()
            copy(DY, level, from_d.at[1, level], from_d.at[1, level], y_dev).wait_send()
            copy(TOX, level, load.at[XN, level], from_xy.at[0, level], x_dev).wait_send()
            copy(TOY, level, load.at[YN, level], from_xy.at[1, level], y_dev).wait_send()

        for level in range(levels):
            finish(level)

            @pl.when(level > z)
            def _():
                copy(UP, level, load.at[OWN, level], from_z.at[level], c_dev).wait_send()

            @pl.when(level < z)
            def _():
                copy(DOWN, level, load.at[OWN, level], from_z.at[level], c_dev).wait_send()

    far = range(levels - 1, -1, -1)
    return (
        [start, functools.partial(each_level, diagonal)]
        + [functools.partial(at_distance, t, sides) for t in far]
        + [functools.partial(along_z, t) for t in far if t > 0]
        + [finish_all]
    )


def scatter_kernel(levels, *refs):
    for step in scatter_steps(levels, *refs):
        step()


def scatter_scratch(levels, rows, width, low):
    return [
        pltpu.VMEM((4, levels, rows, width), low),
        pltpu.VMEM((2, levels, rows, width // 2), low),
        pltpu.VMEM((2, levels, rows, width), low),
        pltpu.VMEM((levels + 1, rows, width), low),
        pltpu.VMEM((4, levels, rows, width), low),
        pltpu.SemaphoreType.DMA((4, levels)),
        pltpu.SemaphoreType.DMA((10, levels)),
        pltpu.SemaphoreType.DMA((10, levels)),
    ]


def scatter_all(part, levels, ident):
    count, rows, width = part.shape
    return pl.pallas_call(
        functools.partial(scatter_kernel, levels),
        out_shape=jax.ShapeDtypeStruct((rows, width), jnp.float32),
        in_specs=[pl.BlockSpec(memory_space=pl.ANY)],
        out_specs=pl.BlockSpec(memory_space=pltpu.VMEM),
        scratch_shapes=scatter_scratch(levels, rows, width, part.dtype),
        compiler_params=pltpu.CompilerParams(
            collective_id=ident, has_side_effects=True, vmem_limit_bytes=56 * 2**20
        ),
        name="scatter_all",
    )(part)


def lane_block(ref, index, width, rows):
    return ref.at[rows, pl.ds(pl.multiple_of(index * width, width), width)]


def halves(count):
    return [pl.ds(0, count // 2), pl.ds(count // 2, count // 2)]


def gather_first_kernel(
    levels, qkv, wout, rows, qkv_all, wout_all, rows_all, own_sem, send_sem, recv_sem
):
    place = Place(levels)
    z, y, x, c = place.z, place.y, place.x, place.c
    top = levels - 1
    x_dev, y_dev, c_dev = place.device(x=1 - x), place.device(y=1 - y), place.device(c=1 - c)
    UP, DOWN, YN = range(3)
    pieces, last = 5, 4
    row_kind = pieces * 3
    OVER_UP, OVER_DOWN = row_kind + 1, row_kind + 2
    own_weights = [qkv.at[k] for k in range(3)] + [wout.at[r] for r in halves(wout.shape[0])]

    def weight_refs(level, yy):
        spot = level * 2 + yy
        return [qkv_all.at[k, spot] for k in range(3)] + [
            lane_block(wout_all, spot, wout.shape[1], r) for r in halves(wout.shape[0])
        ]

    def copy(index, level, ref, dst, device):
        return pltpu.make_async_remote_copy(
            src_ref=ref,
            dst_ref=dst,
            send_sem=send_sem.at[index, level],
            recv_sem=recv_sem.at[index, level],
            device_id=device,
            device_id_type=MESH_ID,
        )

    def send(kind, level, refs, device, only=None):
        for i, (ref, dst) in enumerate(zip(refs, weight_refs(level, y))):
            if only in (None, i):
                copy(kind * pieces + i, level, ref, dst, device).start()

    def arrived(kind, level, only=None):
        for i, ref in enumerate(weight_refs(level, 1 - y if kind == YN else y)):
            if only in (None, i):
                copy(kind * pieces + i, level, ref, ref, c_dev).wait_recv()

    def sent(kind, level):
        for i, ref in enumerate(weight_refs(level, y)):
            copy(kind * pieces + i, level, ref, ref, c_dev).wait_send()

    greet(place, [x_dev, y_dev, c_dev], True)

    @pl.when(z < top)
    def _():
        send(UP, z, own_weights, place.device(z=z + 1))

    @pl.when(z > 0)
    def _():
        send(DOWN, z, own_weights, place.device(z=z - 1))

    send(YN, z, own_weights, y_dev, last)
    for i in range(last):
        send(YN, z, own_weights, y_dev, i)

    def row_ref(xx, cc):
        return rows_all.at[xx * 2 + cc]

    to_x = copy(row_kind, 0, rows, row_ref(x, c), x_dev)
    to_c = copy(row_kind, 1, rows, row_ref(x, c), c_dev)
    to_x.start()
    to_c.start()
    own = [
        pltpu.make_async_copy(ref, dst, own_sem.at[i])
        for i, (ref, dst) in enumerate(
            zip(own_weights + [rows], weight_refs(z, y) + [row_ref(x, c)])
        )
    ]
    for one in own:
        one.start()
    copy(row_kind, 0, rows, row_ref(1 - x, c), x_dev).wait_recv()
    on = copy(row_kind, 2, row_ref(1 - x, c), row_ref(1 - x, c), c_dev)
    on.start()

    def over(kind, level, target):
        ref = weight_refs(level, 1 - y)[last]
        return copy(kind, level, ref, ref, target)

    arrived(YN, z, last)

    @pl.when(z < top)
    def _():
        over(OVER_UP, z, place.device(z=z + 1)).start()

    @pl.when(z > 0)
    def _():
        over(OVER_DOWN, z, place.device(z=z - 1)).start()

    def relay(kind, over_kind, level, inner, target):
        for i in range(pieces):
            arrived(kind, level, i)

            @pl.when(inner)
            def _():
                send(kind, level, weight_refs(level, y), target, i)

            if i != last:
                send(YN, level, weight_refs(level, y), y_dev, i)
        over(over_kind, level, c_dev).wait_recv()

        @pl.when(inner)
        def _():
            over(over_kind, level, target).start()

    for t in range(1, levels):
        @pl.when(z - t >= 0)
        def _():
            relay(UP, OVER_UP, z - t, z < top, place.device(z=z + 1))

        @pl.when(z + t <= top)
        def _():
            relay(DOWN, OVER_DOWN, z + t, z > 0, place.device(z=z - 1))

    for one in own:
        one.wait()
    to_c.wait_recv()
    on.wait_recv()
    for one in (to_x, to_c, on):
        one.wait_send()
    for level in range(levels):
        for i in range(last):
            arrived(YN, level, i)
            copy(YN * pieces + i, level, own_weights[i], own_weights[i], c_dev).wait_send()

        @pl.when((z < top) & (level <= z))
        def _():
            sent(UP, level)
            over(OVER_UP, level, c_dev).wait_send()

        @pl.when((z > 0) & (level >= z))
        def _():
            sent(DOWN, level)
            over(OVER_DOWN, level, c_dev).wait_send()
    copy(YN * pieces + last, z, own_weights[last], own_weights[last], c_dev).wait_send()


def gather_first(w_qkv, w_out, rows, levels, lanes, ident):
    spots = levels * 2
    qkv_all, wout_all, rows_all = pl.pallas_call(
        functools.partial(gather_first_kernel, levels),
        out_shape=[
            jax.ShapeDtypeStruct((3, spots) + w_qkv.shape[1:], w_qkv.dtype),
            jax.ShapeDtypeStruct((w_out.shape[0], spots * w_out.shape[1]), w_out.dtype),
            jax.ShapeDtypeStruct((lanes,) + rows.shape, rows.dtype),
        ],
        in_specs=[pl.BlockSpec(memory_space=pltpu.VMEM)] * 3,
        out_specs=[pl.BlockSpec(memory_space=pl.ANY)] * 3,
        scratch_shapes=[
            pltpu.SemaphoreType.DMA((6,)),
            pltpu.SemaphoreType.DMA((18, levels)),
            pltpu.SemaphoreType.DMA((18, levels)),
        ],
        compiler_params=pltpu.CompilerParams(collective_id=ident, has_side_effects=True),
        name="gather_first",
    )(w_qkv, w_out, rows)
    return (
        qkv_all.reshape(3, -1, w_qkv.shape[2]),
        wout_all,
        rows_all.reshape(-1, rows.shape[1]),
    )


def gather_lanes_kernel(levels, rows, rows_all, own_sem, send_sem, recv_sem):
    place = Place(levels)
    x, c = place.x, place.c
    x_dev, c_dev = place.device(x=1 - x), place.device(c=1 - c)

    def row_ref(xx, cc):
        return rows_all.at[xx * 2 + cc]

    def copy(index, ref, dst, device):
        return pltpu.make_async_remote_copy(
            src_ref=ref,
            dst_ref=dst,
            send_sem=send_sem.at[index],
            recv_sem=recv_sem.at[index],
            device_id=device,
            device_id_type=MESH_ID,
        )

    greet(place, [x_dev, c_dev], False)
    half = rows.shape[0] // 2
    parts = [pl.ds(0, half), pl.ds(half, half)]
    to_x = [copy(i, rows.at[p], row_ref(x, c).at[p], x_dev) for i, p in enumerate(parts)]
    to_c = copy(2, rows, row_ref(x, c), c_dev)
    own = pltpu.make_async_copy(rows, row_ref(x, c), own_sem)
    for one in to_x:
        one.start()
    to_c.start()
    own.start()
    on = []
    for i, p in enumerate(parts):
        to_x[i].wait_recv()
        on.append(copy(3 + i, row_ref(1 - x, c).at[p], row_ref(1 - x, c).at[p], c_dev))
        on[i].start()
    own.wait()
    to_c.wait()
    for one in on:
        one.wait()
    for one in to_x:
        one.wait_send()


def gather_lanes(rows, levels, lanes, ident):
    out = pl.pallas_call(
        functools.partial(gather_lanes_kernel, levels),
        out_shape=jax.ShapeDtypeStruct((lanes,) + rows.shape, rows.dtype),
        in_specs=[pl.BlockSpec(memory_space=pltpu.VMEM)],
        out_specs=pl.BlockSpec(memory_space=pltpu.VMEM),
        scratch_shapes=[
            pltpu.SemaphoreType.DMA,
            pltpu.SemaphoreType.DMA((5,)),
            pltpu.SemaphoreType.DMA((5,)),
        ],
        compiler_params=pltpu.CompilerParams(collective_id=ident, has_side_effects=True),
        name="gather_lanes",
    )(rows)
    return out.reshape(-1, rows.shape[1])


def scatter_lanes_kernel(levels, part, out, from_c, tx, from_x, send_sem, recv_sem):
    place = Place(levels)
    x, c = place.x, place.c
    x_dev, c_dev = place.device(x=1 - x), place.device(c=1 - c)
    rows = part.shape[1]
    pieces = 2
    size = rows // pieces

    def copy(index, ref, dst, device):
        return pltpu.make_async_remote_copy(
            src_ref=ref,
            dst_ref=dst,
            send_sem=send_sem.at[index],
            recv_sem=recv_sem.at[index],
            device_id=device,
            device_id_type=MESH_ID,
        )

    def strips(piece, action):
        def step(i, carry):
            action(pl.ds(pl.multiple_of(piece * size + i * 16, 16), 16))
            return carry
        lax.fori_loop(0, size // 16, step, 0)

    greet(place, [x_dev, c_dev], False)
    spans = [pl.ds(i * size, size) for i in range(pieces)]
    far = [
        copy(i, part.at[(1 - x) * 2 + 1 - c, p], from_c.at[0, p], c_dev)
        for i, p in enumerate(spans)
    ]
    near = copy(pieces, part.at[x * 2 + 1 - c], from_c.at[1], c_dev)
    for one in far:
        one.start()
    near.start()
    to_x = []
    for i, p in enumerate(spans):
        far[i].wait_recv()

        def add(span):
            tx[span] = (
                part[(1 - x) * 2 + c, span].astype(jnp.float32)
                + from_c[0, span].astype(jnp.float32)
            ).astype(tx.dtype)
        strips(i, add)
        to_x.append(copy(pieces + 1 + i, tx.at[p], from_x.at[p], x_dev))
        to_x[i].start()
    near.wait_recv()
    for i in range(pieces):
        to_x[i].wait_recv()

        def add(span):
            out[span] = (
                part[x * 2 + c, span].astype(jnp.float32)
                + from_c[1, span].astype(jnp.float32)
                + from_x[span].astype(jnp.float32)
            )
        strips(i, add)
    for one in far + [near] + to_x:
        one.wait_send()


def scatter_lanes(part, levels, lanes, ident):
    width = part.shape[1]
    rows = part.shape[0] // lanes
    low = part.dtype
    return pl.pallas_call(
        functools.partial(scatter_lanes_kernel, levels),
        out_shape=jax.ShapeDtypeStruct((rows, width), jnp.float32),
        in_specs=[pl.BlockSpec(memory_space=pltpu.VMEM)],
        out_specs=pl.BlockSpec(memory_space=pltpu.VMEM),
        scratch_shapes=[
            pltpu.VMEM((2, rows, width), low),
            pltpu.VMEM((rows, width), low),
            pltpu.VMEM((rows, width), low),
            pltpu.SemaphoreType.DMA((5,)),
            pltpu.SemaphoreType.DMA((5,)),
        ],
        compiler_params=pltpu.CompilerParams(collective_id=ident, has_side_effects=True),
        name="scatter_lanes",
    )(part.reshape(lanes, rows, width))


def scatter_last_kernel(
    levels, qkv, wout, small, parts, qkv_out, wout_out, small_out, gu_out, down_out,
    q_load, w_load, q_y, w_y, q_z, w_z, q_tx, w_tx, s_y, s_tx, over_sum,
    load_sem, y_send, y_recv, z_send, z_recv, s_send, s_recv,
):
    place = Place(levels)
    z, y, x, c = place.z, place.y, place.x, place.c
    top = levels - 1
    x_dev, y_dev, c_dev = place.device(x=1 - x), place.device(y=1 - y), place.device(c=1 - c)
    out_width = w_y.shape[3]
    upper, lower = halves(wout.shape[0])

    def remote(sends, recvs, where, ref, dst, device):
        return pltpu.make_async_remote_copy(
            src_ref=ref,
            dst_ref=dst,
            send_sem=sends.at[where],
            recv_sem=recvs.at[where],
            device_id=device,
            device_id_type=MESH_ID,
        )

    LOWER, OVER = 4, 5
    order = (OVER, LOWER, 0, 1, 2, 3)

    def block(level, yy):
        spot = level * 2 + yy
        return [qkv.at[k, spot] for k in range(3)] + [
            lane_block(wout, spot, out_width, r) for r in (upper, lower)
        ]

    def pieces(q, w, level):
        return [q.at[level, k] for k in range(3)] + [w.at[level, k] for k in range(3)]

    def load(level, i):
        ref = block(level, 1 - y)[LOWER] if i == OVER else block(level, y)[i]
        dst = pieces(q_load, w_load, level)[i]
        return pltpu.make_async_copy(ref, dst, load_sem.at[i, level])

    def across(level, i):
        ref = block(level, 1 - y)[i]
        dst = pieces(q_y, w_y, level)[i]
        return remote(y_send, y_recv, (i, level), ref, dst, y_dev)

    def along(kind, level, slot, device, i):
        ref, dst = pieces(q_tx, w_tx, level)[i], pieces(q_z, w_z, slot)[i]
        return remote(z_send, z_recv, (kind, i, level), ref, dst, device)

    greet(place, [x_dev, y_dev, c_dev], True)

    s_first = remote(s_send, s_recv, 0, small.at[1 - c], s_y.at[0], c_dev)
    s_first.start()
    s_first.wait_recv()
    s_tx[0] = small[c] + s_y[0]
    s_yy = remote(s_send, s_recv, 1, s_tx.at[0], s_y.at[1], y_dev)
    s_yy.start()

    def each_level(action):
        for t in range(levels - 1, 0, -1):
            @pl.when(z - t >= 0)
            def _():
                action(z - t)

            @pl.when(z + t <= top)
            def _():
                action(z + t)

        action(z)

    def begin(level):
        for i in order:
            if i < LOWER:
                across(level, i).start()
            load(level, i).start()

    each_level(begin)

    s_yy.wait_recv()
    s_tx[2 + z] = s_tx[0] + s_y[1]

    def share(kind, level):
        ref = s_tx.at[2 + level]
        target = place.device(z=z + 1) if kind == 0 else place.device(z=z - 1)
        return remote(s_send, s_recv, 4 + kind * levels + level, ref, ref, target)

    @pl.when(z < top)
    def _():
        share(0, z).start()

    @pl.when(z > 0)
    def _():
        share(1, z).start()

    for t in range(1, levels):
        @pl.when(z - t >= 0)
        def _():
            share(0, z - t).wait_recv()

            @pl.when(z < top)
            def _():
                share(0, z - t).start()

        @pl.when(z + t <= top)
        def _():
            share(1, z + t).wait_recv()

            @pl.when(z > 0)
            def _():
                share(1, z + t).start()

    whole = s_tx[2]
    for level in range(1, levels):
        whole = whole + s_tx[2 + level]
    s_tx[1] = whole
    s_x = remote(s_send, s_recv, 2, s_tx.at[1], s_y.at[2], x_dev)
    s_x.start()

    units = parts.shape[3]
    for i in range(parts.shape[0]):
        span = slice(i * units, (i + 1) * units)
        for k in range(2):
            gu_out[k, :, span] = parts[i, k].astype(jnp.float32)
        down_out[span] = parts[i, 2].astype(jnp.float32).T

    def strips(ref, action):
        def step(i, carry):
            rows = pl.ds(pl.multiple_of(i * 16, 16), 16)
            ref[rows] = action(rows).astype(ref.dtype)
            return carry
        lax.fori_loop(0, ref.shape[0] // 16, step, 0)

    def f32(ref, rows):
        return ref[rows].astype(jnp.float32)

    def own_sum(level, i, rows):
        value = f32(pieces(q_load, w_load, level)[i], rows)
        return value + f32(pieces(q_y, w_y, level)[i], rows) if i < LOWER else value

    def ready(level, i):
        load(level, i).wait()
        if i < LOWER:
            across(level, i).wait_recv()

    def pass_on(level, kind, first, target, slot):
        ahead, results = pieces(q_z, w_z, level), pieces(q_tx, w_tx, level)
        for i in order:
            ready(level, i)

            @pl.when(first)
            def _():
                strips(results[i], lambda rows: own_sum(level, i, rows))

            @pl.when(jnp.logical_not(first))
            def _():
                along(kind, level, level, c_dev, i).wait_recv()
                strips(results[i], lambda rows: own_sum(level, i, rows) + f32(ahead[i], rows))
            along(kind, level, slot, target, i).start()

    for t in range(levels - 1, 0, -1):
        @pl.when(z + t <= top)
        def _():
            pass_on(z + t, 0, z == 0, place.device(z=z + 1), z + t)

        @pl.when(z - t >= 0)
        def _():
            slot = (z - t) if t > 1 else levels
            pass_on(z - t, 1, z == top, place.device(z=z - 1), slot)

        if t == levels - 1:
            s_x.wait_recv()
            small_out[c] = s_tx[1] + s_y[2]
            s_last = remote(s_send, s_recv, 3, small_out.at[c], small_out.at[c], c_dev)
            s_last.start()

    results = [qkv_out.at[k] for k in range(3)] + [wout_out.at[upper], wout_out.at[lower], over_sum]
    passed = remote(y_send, y_recv, (LOWER, 0), w_tx.at[z, 2], w_y.at[z, 1], y_dev)
    for i in order:
        ready(z, i)
        strips(results[i], lambda rows: own_sum(z, i, rows))
        for kind, here, slot in ((0, z > 0, z), (1, z < top, levels)):
            @pl.when(here)
            def _():
                along(kind, z, slot, c_dev, i).wait_recv()
                ahead = pieces(q_z, w_z, slot)[i]
                strips(results[i], lambda rows: results[i][rows] + f32(ahead, rows))
        if i == OVER:
            strips(w_tx.at[z, 2], lambda rows: over_sum[rows])
            passed.start()
    passed.wait_recv()
    strips(results[LOWER], lambda rows: results[LOWER][rows] + f32(w_y.at[z, 1], rows))
    passed.wait_send()

    remote(s_send, s_recv, 3, small_out.at[1 - c], small_out.at[1 - c], c_dev).wait_recv()
    for one in (s_first, s_x, s_yy, s_last):
        one.wait_send()
    for level in range(levels):
        for i in range(4):
            across(level, i).wait_send()

        @pl.when(level > z)
        def _():
            for i in order:
                along(0, level, level, c_dev, i).wait_send()

        @pl.when(level < z)
        def _():
            for i in order:
                along(1, level, level, c_dev, i).wait_send()

        @pl.when((z < top) & (level <= z))
        def _():
            share(0, level).wait_send()

        @pl.when((z > 0) & (level >= z))
        def _():
            share(1, level).wait_send()


def scatter_last(grad_qkv, grad_wout, small, parts, levels, ident):
    wide = parts.shape[0] * parts.shape[3]
    spots = levels * 2
    depth, width = grad_qkv.shape[1] // spots, grad_qkv.shape[2]
    out_rows, out_width = grad_wout.shape[0], grad_wout.shape[1] // spots
    low = grad_qkv.dtype
    vmem = pl.BlockSpec(memory_space=pltpu.VMEM)
    hbm = pl.BlockSpec(memory_space=pl.ANY)

    def pair(count):
        return [
            pltpu.VMEM((count, 3, depth, width), low),
            pltpu.VMEM((count, 3, out_rows // 2, out_width), low),
        ]

    return pl.pallas_call(
        functools.partial(scatter_last_kernel, levels),
        out_shape=[
            jax.ShapeDtypeStruct((3, depth, width), jnp.float32),
            jax.ShapeDtypeStruct((out_rows, out_width), jnp.float32),
            jax.ShapeDtypeStruct(small.shape, jnp.float32),
            jax.ShapeDtypeStruct((2, parts.shape[2], wide), jnp.float32),
            jax.ShapeDtypeStruct((wide, parts.shape[2]), jnp.float32),
        ],
        in_specs=[hbm, hbm, vmem, vmem],
        out_specs=[vmem] * 5,
        scratch_shapes=pair(levels)
        + pair(levels)
        + pair(levels + 1)
        + pair(levels)
        + [
            pltpu.VMEM((3,) + small.shape[1:], jnp.float32),
            pltpu.VMEM((2 + levels,) + small.shape[1:], jnp.float32),
            pltpu.VMEM((out_rows // 2, out_width), jnp.float32),
            pltpu.SemaphoreType.DMA((6, levels)),
            pltpu.SemaphoreType.DMA((5, levels)),
            pltpu.SemaphoreType.DMA((5, levels)),
            pltpu.SemaphoreType.DMA((2, 6, levels)),
            pltpu.SemaphoreType.DMA((2, 6, levels)),
            pltpu.SemaphoreType.DMA((4 + 2 * levels,)),
            pltpu.SemaphoreType.DMA((4 + 2 * levels,)),
        ],
        compiler_params=pltpu.CompilerParams(
            collective_id=ident, has_side_effects=True, vmem_limit_bytes=48 * 2**20
        ),
        name="scatter_last",
    )(grad_qkv.reshape(3, spots, depth, width), grad_wout, small, parts)


PAIR = 256
SIDE = 128


def mul(a, b, ca, cb):
    return lax.dot_general(
        a, b, (((ca,), (cb,)), ((), ())), preferred_element_type=jnp.float32
    )


def swish_parts(gate, up):
    sig = jax.nn.sigmoid(gate)
    silu = gate * sig
    return silu * up, up * sig * (1.0 + gate * (1.0 - sig)), silu


def chosen(slot_row, capacity):
    ids = lax.broadcasted_iota(jnp.int32, (capacity, slot_row.shape[1]), 0)
    return (ids == slot_row).astype(jnp.float32).astype(jnp.bfloat16)


def rows_in_kernel(
    capacity, experts, spare, x, parts, extra, slots,
    hid, to_gate, to_up, stats, taken, weights, down, share,
):
    units = parts.shape[3]

    @pl.when(pl.program_id(0) == 0)
    def _():
        weights[...] = jnp.zeros_like(weights)
        down[...] = jnp.zeros_like(down)
        weights[:, PAIR + SIDE :] = extra[...]
        depth = parts.shape[2]
        for i in range(parts.shape[0]):
            span = slice(i * depth, (i + 1) * depth)
            weights[span, :units] = parts[i, 0]
            weights[span, PAIR : PAIR + units] = parts[i, 1]
            down[span, :units] = parts[i, 2]

    acc = jnp.dot(x[...], weights[...], preferred_element_type=jnp.float32)
    gate, up = acc[:, :PAIR], acc[:, PAIR:]
    hidden, by_gate, by_up = swish_parts(gate, up)
    hid[...] = hidden.astype(hid.dtype)
    to_gate[...] = by_gate
    to_up[...] = by_up
    side = up[:, SIDE:]
    lane = lax.broadcasted_iota(jnp.int32, side.shape, 1)
    routed = (lane >= spare) & (lane < spare + experts)
    powers = jnp.where(routed, jnp.exp(jnp.where(routed, side, 0.0)), 0.0)
    probs = powers / jnp.sum(powers, axis=1, keepdims=True)
    gated = (lane >= spare + experts) & (lane < spare + experts + 3)
    sig = jax.nn.sigmoid(jnp.sum(jnp.where(gated, side, 0.0), axis=1, keepdims=True))
    stats[...] = jnp.where(routed, probs, jnp.where(gated, sig, 0.0))
    mine = jnp.sum(jnp.where(lane == spare + lax.axis_index(both), probs, 0.0), axis=1, keepdims=True)
    tokens = slots.shape[2]
    for b in range(slots.shape[1]):
        pick = chosen(slots[0, b : b + 1], capacity)
        rows = jnp.dot(
            pick, x[b * tokens : (b + 1) * tokens], preferred_element_type=jnp.float32
        )
        taken[b * capacity : (b + 1) * capacity] = rows.astype(taken.dtype)
        share[b * capacity : (b + 1) * capacity] = jnp.dot(
            pick.astype(jnp.float32), mine[b * tokens : (b + 1) * tokens],
            precision=highest, preferred_element_type=jnp.float32,
        )


def resident(shape):
    zeros = (0,) * len(shape)
    return pl.BlockSpec(shape, lambda i: zeros, pipeline_mode=pl.Buffered(1))


def tiled(rows, width):
    return pl.BlockSpec((rows, width), lambda i: (i, 0))


def stacked(*shape):
    rest = (0,) * len(shape)
    return pl.BlockSpec((1,) + shape, lambda i: (i,) + rest)


def cost(*products):
    return pl.CostEstimate(
        flops=sum(2 * m * k * n for m, k, n in products),
        bytes_accessed=sum(2 * (m * k + k * n + m * n) for m, k, n in products),
        transcendentals=0,
    )


def params():
    return pltpu.CompilerParams(vmem_limit_bytes=60 * 2**20)


def weight_loads(w_gu, w_down, gu_here, down_here, sem):
    return [
        pltpu.make_async_copy(w_gu, gu_here, sem.at[0]),
        pltpu.make_async_copy(w_down, down_here, sem.at[1]),
    ]


def forward_kernel(
    levels, capacity, experts, spare, tiles, x, parts, extra, slots, w_gu, w_down, late,
    hid, to_gate, to_up, stats, taken_out, weights, down, e_hid, e_gate, e_up, e_out, share, part,
    late_all, taken, hid_all, stats_all, share_all, gu_here, down_here, load_sem,
    own_sem, send_sems, recv_sems,
):
    step = pl.program_id(0)
    comm = gather_steps(levels, [late], [late_all], own_sem, send_sems, recv_sems)

    loads = weight_loads(w_gu, w_down, gu_here, down_here, load_sem)

    @pl.when(step == 0)
    def _():
        comm[0]()
        for load in loads:
            load.start()

    @pl.when(step == tiles)
    def _():
        for load in loads:
            load.wait()

    size = slots.shape[1] * capacity

    @pl.when(step < tiles)
    def _():
        rows_in_kernel(
            capacity, experts, spare, x, parts, extra, slots,
            hid, to_gate, to_up, stats, taken_out, weights, down, share,
        )
        here = pl.ds(pl.multiple_of(step * size, size), size)
        taken[here] = taken_out[...]
        share_all[here] = share[...]
        here = pl.ds(pl.multiple_of(step * x.shape[0], x.shape[0]), x.shape[0])
        hid_all[here] = hid[...]
        stats_all[here] = stats[...]

    e_tiles = taken.shape[0] // e_out.shape[0]

    @pl.when((step >= tiles) & (step < tiles + e_tiles))
    def _():
        tile = e_out.shape[0]
        here = pl.ds(pl.multiple_of((step - tiles) * tile, tile), tile)
        rows = taken[here]
        gate = jnp.dot(rows, gu_here[0], preferred_element_type=jnp.float32)
        up = jnp.dot(rows, gu_here[1], preferred_element_type=jnp.float32)
        hidden, by_gate, by_up = swish_parts(gate, up)
        low = hidden.astype(e_hid.dtype)
        e_hid[...] = low
        e_gate[...] = by_gate
        e_up[...] = by_up
        result = jnp.dot(low, down_here[...], preferred_element_type=jnp.float32).astype(e_out.dtype)
        e_out[...] = result
        taken[here] = result

    @pl.when(step >= tiles + e_tiles)
    def _():
        tile, tokens = x.shape[0], slots.shape[2]
        at = step - tiles - e_tiles
        here = pl.ds(pl.multiple_of(at * tile, tile), tile)
        whole = mul(hid_all[here], down[...], 1, 1)
        sig = stats_all[here][:, spare + experts : spare + experts + 1]
        for b in range(slots.shape[1]):
            span = slice(b * tokens, (b + 1) * tokens)
            own = pl.ds(pl.multiple_of(at * size + b * capacity, capacity), capacity)
            pick = chosen(slots[0, b : b + 1], capacity)
            weighted = (share_all[own] * taken[own].astype(jnp.float32)).astype(jnp.bfloat16)
            part[span] = (sig[span] * whole[span] + mul(pick, weighted, 0, 0)).astype(part.dtype)

    total = pl.num_programs(0)
    times = (3, 8, 10, 12, 15)
    for i, action in enumerate(comm[1:-1]):
        at = jnp.minimum(times[min(i, len(times) - 1)], total - 1)

        @pl.when(step == at)
        def _():
            action()

    @pl.when(step == total - 1)
    def _():
        comm[-1]()


def forward(x, parts, extra, slots, w_gu, w_down, late, capacity, experts, spare, levels, ident):
    count, tokens = slots.shape
    rows, width = x.shape
    units = w_down.shape[0]
    per = 4
    tile = per * tokens
    tiles = rows // tile
    e_rows, e_tile = count * capacity, 256

    def early(*shape):
        rest = (0,) * (len(shape) - 1)
        return pl.BlockSpec(shape, lambda i: (jnp.minimum(i, tiles - 1),) + rest)

    def after(*shape):
        rest = (0,) * (len(shape) - 1)
        return pl.BlockSpec(
            shape, lambda i: (jnp.clip(i - tiles, 0, e_rows // e_tile - 1),) + rest
        )

    e_tiles = e_rows // e_tile

    def twice(*shape):
        rest = (0,) * (len(shape) - 1)

        def index(i):
            return (jnp.where(i < tiles, i, jnp.maximum(i - tiles - e_tiles, 0)),) + rest
        return pl.BlockSpec(shape, index)

    def final(*shape):
        rest = (0,) * (len(shape) - 1)
        return pl.BlockSpec(shape, lambda i: (jnp.maximum(i - tiles - e_tiles, 0),) + rest)

    hbm = pl.BlockSpec(memory_space=pl.ANY)
    low, wide = jnp.bfloat16, jnp.float32
    sems = (11, levels, 1)
    return pl.pallas_call(
        functools.partial(forward_kernel, levels, capacity, experts, spare, tiles),
        grid=(2 * tiles + e_tiles,),
        in_specs=[
            early(tile, width),
            resident(parts.shape),
            resident(extra.shape),
            twice(1, per, tokens),
            hbm,
            hbm,
            hbm,
        ],
        out_specs=[
            early(tile, PAIR),
            early(tile, PAIR),
            early(tile, PAIR),
            early(tile, PAIR - SIDE),
            early(per * capacity, width),
            resident((width, 2 * PAIR)),
            resident((width, PAIR)),
            after(e_tile, units),
            after(e_tile, units),
            after(e_tile, units),
            after(e_tile, width),
            early(per * capacity, 1),
            final(tile, width),
            hbm,
        ],
        out_shape=[
            jax.ShapeDtypeStruct((rows, PAIR), low),
            jax.ShapeDtypeStruct((rows, PAIR), wide),
            jax.ShapeDtypeStruct((rows, PAIR), wide),
            jax.ShapeDtypeStruct((rows, PAIR - SIDE), wide),
            jax.ShapeDtypeStruct((e_rows, width), low),
            jax.ShapeDtypeStruct((width, 2 * PAIR), low),
            jax.ShapeDtypeStruct((width, PAIR), low),
            jax.ShapeDtypeStruct((e_rows, units), low),
            jax.ShapeDtypeStruct((e_rows, units), wide),
            jax.ShapeDtypeStruct((e_rows, units), wide),
            jax.ShapeDtypeStruct((e_rows, width), low),
            jax.ShapeDtypeStruct((e_rows, 1), wide),
            jax.ShapeDtypeStruct((rows, width), low),
            jax.ShapeDtypeStruct((count,) + late.shape, late.dtype),
        ],
        scratch_shapes=[
            pltpu.VMEM((e_rows, width), low),
            pltpu.VMEM((rows, PAIR), low),
            pltpu.VMEM((rows, PAIR - SIDE), wide),
            pltpu.VMEM((e_rows, 1), wide),
            pltpu.VMEM(w_gu.shape, w_gu.dtype),
            pltpu.VMEM(w_down.shape, w_down.dtype),
            pltpu.SemaphoreType.DMA((2,)),
            pltpu.SemaphoreType.DMA((1,)),
            pltpu.SemaphoreType.DMA(sems),
            pltpu.SemaphoreType.DMA(sems),
        ],
        compiler_params=pltpu.CompilerParams(
            collective_id=ident, has_side_effects=True, vmem_limit_bytes=67043328
        ),
        cost_estimate=cost(
            (rows, width, 2 * PAIR), (e_rows, width, 2 * units), (e_rows, units, width)
        ),
        name="forward",
    )(x, parts, extra, slots.reshape(count // per, per, tokens), w_gu, w_down, late)


def expert_back_kernel(
    capacity, grad, slots, share, out, to_gate, to_up, w_gu, w_down,
    dout, dgu, din, dots, gu_here, down_here, load_sem,
):
    loads = weight_loads(w_gu, w_down, gu_here, down_here, load_sem)
    first = pl.program_id(0) == 0

    @pl.when(first)
    def _():
        for load in loads[::-1]:
            load.start()

    tokens = slots.shape[2]
    size = slots.shape[1]
    taken = []
    for b in range(size):
        pick = chosen(slots[0, b : b + 1], capacity)
        taken.append(
            jnp.dot(
                pick, grad[b * tokens : (b + 1) * tokens], preferred_element_type=jnp.float32
            )
        )
    rows = jnp.concatenate(taken, axis=0)
    inner = jnp.sum(rows * out[...].astype(jnp.float32), axis=1, keepdims=True)
    dots[...] = jnp.broadcast_to(inner, dots.shape)
    low = (share[...] * rows).astype(jnp.bfloat16)
    dout[...] = low

    @pl.when(first)
    def _():
        loads[1].wait()

    dhid = mul(low, down_here[...], 1, 1)
    dgate = (dhid * to_gate[...]).astype(jnp.bfloat16)
    dup = (dhid * to_up[...]).astype(jnp.bfloat16)
    dgu[0] = dgate
    dgu[1] = dup

    @pl.when(first)
    def _():
        loads[0].wait()

    din[...] = (mul(dgate, gu_here[0], 1, 1) + mul(dup, gu_here[1], 1, 1)).astype(din.dtype)


def expert_back(grad, slots, share, out, to_gate, to_up, w_gu, w_down, capacity):
    count, tokens = slots.shape
    rows, width = out.shape
    units = w_down.shape[0]
    tile = 256
    per = tile // capacity
    return pl.pallas_call(
        functools.partial(expert_back_kernel, capacity),
        grid=(rows // tile,),
        in_specs=[
            tiled(per * tokens, width),
            stacked(per, tokens),
            tiled(tile, 1),
            tiled(tile, width),
            tiled(tile, units),
            tiled(tile, units),
            pl.BlockSpec(memory_space=pl.ANY),
            pl.BlockSpec(memory_space=pl.ANY),
        ],
        out_specs=[
            tiled(tile, width),
            pl.BlockSpec((2, tile, units), lambda i: (0, i, 0)),
            tiled(tile, width),
            tiled(tile, 128),
        ],
        out_shape=[
            jax.ShapeDtypeStruct((rows, width), jnp.bfloat16),
            jax.ShapeDtypeStruct((2, rows, units), jnp.bfloat16),
            jax.ShapeDtypeStruct((rows, width), jnp.bfloat16),
            jax.ShapeDtypeStruct((rows, 128), jnp.float32),
        ],
        scratch_shapes=[
            pltpu.VMEM(w_gu.shape, w_gu.dtype),
            pltpu.VMEM(w_down.shape, w_down.dtype),
            pltpu.SemaphoreType.DMA((2,)),
        ],
        compiler_params=params(),
        cost_estimate=cost((rows, width, units), (rows, 2 * units, width)),
        name="expert_back",
    )(
        grad,
        slots.reshape(count // per, per, tokens),
        share,
        out,
        to_gate,
        to_up,
        w_gu,
        w_down,
    )


def rows_back_kernel(
    levels, capacity, lane, grad, x, stats, hid, to_gate, to_up, slots, din, weights, w_down, part,
    out, grad_parts, own, dots, sum_weights, sum_down, *scratch
):
    step = pl.program_id(0)
    comm = scatter_steps(levels, part, own, *scratch)

    @pl.when(step == 0)
    def _():
        comm[0]()

    @pl.when(step == 0)
    def _():
        sum_weights[...] = jnp.zeros_like(sum_weights)
        sum_down[...] = jnp.zeros_like(sum_down)

    low = (stats[:, lane : lane + 1] * grad[...].astype(jnp.float32)).astype(jnp.bfloat16)
    inner = jnp.sum(
        mul(grad[...], w_down[...], 1, 0) * hid[...].astype(jnp.float32), axis=1, keepdims=True
    )
    dots[...] = jnp.broadcast_to(inner, dots.shape)
    dhid = mul(low, w_down[...], 1, 0)
    dgate = (dhid * to_gate[...]).astype(jnp.bfloat16)
    dup = (dhid * to_up[...]).astype(jnp.bfloat16)
    both_grads = jnp.concatenate([dgate, dup], axis=1)
    sum_weights[...] += mul(both_grads, x[...], 0, 0)
    whole = mul(both_grads, weights[...], 1, 1)
    sum_down[...] += mul(hid[...], low, 0, 0)
    tokens = slots.shape[2]
    for b in range(slots.shape[1]):
        span = slice(b * tokens, (b + 1) * tokens)
        pick = chosen(slots[0, b : b + 1], capacity)
        back = whole[span]
        spread = mul(pick, din[b * capacity : (b + 1) * capacity], 0, 0)
        out[span] = (back + spread).astype(out.dtype)

    @pl.when(step == pl.num_programs(0) - 1)
    def _():
        depth, units = grad_parts.shape[2:]
        for i in range(grad_parts.shape[0]):
            span = slice(i * depth, (i + 1) * depth)
            grads = sum_weights[:, span].T.astype(grad_parts.dtype)
            grad_parts[i, 0] = grads[:, :units]
            grad_parts[i, 1] = grads[:, PAIR : PAIR + units]
            grad_parts[i, 2] = sum_down[:, span].T.astype(grad_parts.dtype)[:, :units]

    last = pl.num_programs(0) - 1
    for i, action in enumerate(comm[1:]):
        @pl.when(step == jnp.minimum(i, last))
        def _():
            action()


def rows_back(
    grad, x, stats, hid, to_gate, to_up, slots, din, weights, w_down, part, parts_shape,
    capacity, lane, levels, ident,
):
    count, tokens = slots.shape
    rows, width = x.shape
    per = 4
    tile = per * tokens
    return pl.pallas_call(
        functools.partial(rows_back_kernel, levels, capacity, lane),
        grid=(rows // tile,),
        in_specs=[
            tiled(tile, width),
            tiled(tile, width),
            tiled(tile, stats.shape[1]),
            tiled(tile, PAIR),
            tiled(tile, PAIR),
            tiled(tile, PAIR),
            stacked(per, tokens),
            tiled(per * capacity, width),
            resident(weights.shape),
            resident(w_down.shape),
            pl.BlockSpec(memory_space=pl.ANY),
        ],
        out_specs=[
            tiled(tile, width),
            resident(parts_shape),
            resident(part.shape[1:]),
            tiled(tile, 128),
        ],
        out_shape=[
            jax.ShapeDtypeStruct((rows, width), jnp.bfloat16),
            jax.ShapeDtypeStruct(parts_shape, jnp.bfloat16),
            jax.ShapeDtypeStruct(part.shape[1:], jnp.float32),
            jax.ShapeDtypeStruct((rows, 128), jnp.float32),
        ],
        scratch_shapes=[
            pltpu.VMEM(weights.shape[::-1], jnp.float32),
            pltpu.VMEM(w_down.shape[::-1], jnp.float32),
        ]
        + scatter_scratch(levels, part.shape[1], width, part.dtype),
        compiler_params=pltpu.CompilerParams(
            collective_id=ident, has_side_effects=True, vmem_limit_bytes=67043328
        ),
        cost_estimate=cost((rows, width, PAIR), (rows, 2 * PAIR, width), (2 * PAIR, rows, width), (PAIR, rows, width)),
        name="rows_back",
    )(
        grad, x, stats, hid, to_gate, to_up,
        slots.reshape(count // per, per, tokens), din, weights, w_down, part,
    )


def gu_grad_kernel(x, dgu, out):
    rows = x[...].T
    for i in range(2):
        out[i] = jnp.dot(rows, dgu[i], preferred_element_type=jnp.float32)


def down_grad_kernel(hid, dout, out, turned):
    @pl.when(pl.program_id(0) == 0)
    def _():
        turned[...] = hid[...].T

    out[...] = jnp.dot(turned[...], dout[...], preferred_element_type=jnp.float32)


def expert_weight_grads(x, dgu, hid, dout):
    rows, width = x.shape
    units = hid.shape[1]
    tile = 256
    grad_gu = pl.pallas_call(
        gu_grad_kernel,
        grid=(width // tile,),
        in_specs=[pl.BlockSpec((rows, tile), lambda i: (0, i)), resident(dgu.shape)],
        out_specs=pl.BlockSpec((2, tile, units), lambda i: (0, i, 0)),
        out_shape=jax.ShapeDtypeStruct((2, width, units), jnp.float32),
        compiler_params=params(),
        cost_estimate=cost((width, rows, 2 * units)),
        name="expert_gu_grad",
    )(x, dgu)
    grad_down = pl.pallas_call(
        down_grad_kernel,
        grid=(width // tile,),
        in_specs=[resident(hid.shape), pl.BlockSpec((rows, tile), lambda i: (0, i))],
        out_specs=pl.BlockSpec((units, tile), lambda i: (0, i)),
        out_shape=jax.ShapeDtypeStruct((units, width), jnp.float32),
        scratch_shapes=[pltpu.VMEM((units, rows), jnp.bfloat16)],
        compiler_params=params(),
        cost_estimate=cost((units, rows, width)),
        name="expert_down_grad",
    )(hid, dout)
    return grad_gu, grad_down


def rope_tables(length, head_width):
    half_width = head_width // 2
    inverse = rope_base ** (-(jnp.arange(half_width, dtype=jnp.float32) * 2.0 / head_width))
    angles = jnp.arange(length, dtype=jnp.float32)[:, None] * inverse[None, :]
    angles = jnp.concatenate([angles, angles], axis=1)
    return (jnp.cos(angles), jnp.sin(angles))


def rotate(values, cosine, sine_tab):
    half_width = values.shape[-1] // 2
    turned = jnp.concatenate([-values[..., half_width:], values[..., :half_width]], axis=-1)
    return values * cosine[:, None, :] + turned * sine_tab[:, None, :]


def rotate_back(grad_vals, cosine, sine_tab):
    half_width = grad_vals.shape[-1] // 2
    scaled = grad_vals * sine_tab[:, None, :]
    turned = jnp.concatenate([scaled[..., half_width:], -scaled[..., :half_width]], axis=-1)
    return grad_vals * cosine[:, None, :] + turned


def norm_rows(values):
    scale_rows = lax.rsqrt(jnp.mean(values * values, axis=-1, keepdims=True) + eps)
    return (values * scale_rows, scale_rows)


def norm_back(grad_normed, unit_rows, scale_rows, gain_vec):
    inner_term = grad_normed * gain_vec
    return scale_rows * (
        inner_term - unit_rows * jnp.mean(inner_term * unit_rows, axis=-1, keepdims=True)
    )


def heads_dot(a, b, ca, cb, ha, hb):
    return lax.dot_general(
        a, b, (((ca,), (cb,)), ((ha,), (hb,))), preferred_element_type=jnp.float32
    )


def masked_scores(query_blk, keys_low, first_row, factor):
    scores = heads_dot(query_blk, keys_low, 2, 2, 1, 1) * factor
    row_ids = first_row + jnp.arange(query_blk.shape[0], dtype=jnp.int32)
    col_ids = jnp.arange(keys_low.shape[0], dtype=jnp.int32)
    causal = col_ids[None, :] <= row_ids[:, None]
    return jnp.where(causal[None], scores, -jnp.inf)


def silu_pair(gate_up):
    sig_gate = jax.nn.sigmoid(gate_up[0])
    return (gate_up[0] * sig_gate, sig_gate)


def swiglu_back(grad_hid, gate_up):
    silu_gate, sig_gate = silu_pair(gate_up)
    grad_gate = grad_hid * gate_up[1] * sig_gate * (1.0 + gate_up[0] * (1.0 - sig_gate))
    grad_up = grad_hid * silu_gate
    return jnp.stack([grad_gate, grad_up], axis=0).astype(jnp.bfloat16)


def pair_mul(rows, weights):
    return jnp.stack([mul(rows, w, 1, 0) for w in weights])


class Attention:
    def __init__(self, normed_group, full_qkv, b_qkv):
        self.normed, self.weights = normed_group, full_qkv
        self.length, self.width = normed_group.shape[0], full_qkv.shape[2]
        heads = self.width // HEAD_DIM
        self.factor = HEAD_DIM ** (-0.5)
        projected = pair_mul(normed_group, full_qkv) + b_qkv[:, None, :]
        self.cosine, self.sine_tab = rope_tables(self.length, HEAD_DIM)
        split = projected.reshape(3, self.length, heads, HEAD_DIM)
        self.queries = rotate(split[0], self.cosine, self.sine_tab).astype(jnp.bfloat16)
        self.keys = rotate(split[1], self.cosine, self.sine_tab).astype(jnp.bfloat16)
        self.values = split[2].astype(jnp.bfloat16)
        scores = masked_scores(self.queries, self.keys, 0, self.factor)
        row_max = jnp.max(scores, axis=-1, keepdims=True)
        weights = jnp.exp(scores - row_max)
        row_sum = jnp.sum(weights, axis=-1, keepdims=True)
        probs_low = (weights / row_sum).astype(jnp.bfloat16)
        mixed = heads_dot(probs_low, self.values, 2, 0, 0, 1).astype(jnp.bfloat16)
        self.mixed = mixed.swapaxes(0, 1).reshape(self.length, self.width)
        self.logsum = row_max + jnp.log(row_sum)

    def back(self, grad_mixed):
        grad_mixed = grad_mixed.reshape(self.length, -1, HEAD_DIM)
        scores = masked_scores(self.queries, self.keys, 0, self.factor)
        soft_probs = jnp.exp(scores - self.logsum)
        probs_low = soft_probs.astype(jnp.bfloat16)
        grad_values = heads_dot(probs_low, grad_mixed, 1, 0, 0, 1)
        grad_probs = heads_dot(grad_mixed, self.values, 2, 2, 1, 1)
        grad_scores = soft_probs * (
            grad_probs - jnp.sum(soft_probs * grad_probs, axis=-1, keepdims=True)
        )
        low = grad_scores.astype(jnp.bfloat16)
        grad_queries = heads_dot(low, self.keys, 2, 0, 0, 1) * self.factor
        grad_keys = heads_dot(low, self.queries, 1, 0, 0, 1) * self.factor
        grad_proj = jnp.stack(
            [
                rotate_back(grad_queries.swapaxes(0, 1), self.cosine, self.sine_tab),
                rotate_back(grad_keys.swapaxes(0, 1), self.cosine, self.sine_tab),
                grad_values.swapaxes(0, 1),
            ]
        )
        grad_proj = grad_proj.reshape(3, self.length, self.width).astype(jnp.bfloat16)
        bias_sum = jnp.sum(grad_proj, axis=1, dtype=jnp.float32)
        grad_weights = jnp.stack(
            [mul(self.normed, grad, 0, 0).astype(jnp.bfloat16) for grad in grad_proj]
        )
        normed_part = sum(mul(g, w, 1, 1) for g, w in zip(grad_proj, self.weights))
        return bias_sum, grad_weights, normed_part


def local(
    tokens,
    gain_attn,
    w_qkv,
    b_qkv,
    w_out,
    gain_ffn,
    w_router,
    shared_gate,
    w_shared_gu,
    w_shared_down,
    w_expert_gu,
    w_expert_down,
    routes,
    grad_out,
):
    own_rows, model_width = tokens.shape
    spots, lanes = lax.axis_size(EXPERT), lax.axis_size(SHARD)
    levels, devices = spots // 2, spots * lanes
    me = lax.axis_index(both)
    local_width = w_qkv.shape[2]
    experts_all = w_router.shape[1]
    capacity = 2 * own_rows * TOPK // experts_all
    units = w_shared_down.shape[0] // spots

    x_own = tokens.astype(jnp.float32)
    unit_one, scale_one = norm_rows(x_own)
    normed_one = (unit_one * gain_attn).astype(jnp.bfloat16)
    full_qkv, full_out, normed_group = gather_first(w_qkv, w_out, normed_one, levels, lanes, 1)
    w_shared_gu, w_shared_down, normed_group = lax.optimization_barrier(
        (w_shared_gu, w_shared_down, normed_group)
    )
    parts = jnp.concatenate([w_shared_gu, w_shared_down.T[None]])
    parts = parts.reshape(3, -1, spots, units).transpose(2, 0, 1, 3)
    parts = lax.all_to_all(parts, EXPERT, 0, 0)
    gate_terms, rest = [], shared_gate
    for _ in range(3):
        term = lax.reduce_precision(rest, 8, 7)
        gate_terms.append(term.astype(jnp.bfloat16))
        rest = rest - term
    extra = jnp.concatenate([w_router, jnp.stack(gate_terms, axis=1)], axis=1)
    spare = units - SIDE
    extra = jnp.pad(extra, ((0, 0), (spare, PAIR - SIDE - spare - extra.shape[1])))
    gate_lane = spare + experts_all

    attention = Attention(normed_group, full_qkv, b_qkv)
    attn_own = scatter_lanes(mul(attention.mixed, full_out, 1, 0), levels, lanes, 2)
    hidden_own = x_own + attn_own
    unit_two, scale_two = norm_rows(hidden_own)
    normed_own = (unit_two * gain_ffn).astype(jnp.bfloat16)
    route_rows = jnp.zeros((16, own_rows), jnp.int32).at[:TOPK].set(routes.T)
    normed_own, route_rows, parts = lax.optimization_barrier((normed_own, route_rows, parts))
    normed_all, routes_all = gather_all([normed_own, route_rows], levels, devices, 3)

    hits = (routes_all.reshape(devices, 16, own_rows)[:, :TOPK] == me).any(axis=1)
    slots = jnp.where(hits, jnp.cumsum(hits.astype(jnp.int32), axis=1) - 1, -1)
    placed = slots[:, None, :] == jnp.arange(capacity, dtype=jnp.int32)[None, :, None]
    placed = placed.astype(jnp.float32)
    (
        shared_hid, shared_gate_by, shared_up_by, stats, received, slice_gu, slice_down,
        expert_hid, gate_by, up_by, expert_out, share, ffn_part, grad_all,
    ) = forward(
        normed_all, parts, extra, slots, w_expert_gu[0], w_expert_down[0], grad_out,
        capacity, experts_all, spare, levels, 8,
    )
    grad_all = grad_all.reshape(-1, model_width)
    expert_dout, expert_dgu, expert_din, slot_dots = expert_back(
        grad_all, slots, share, expert_out, gate_by, up_by, w_expert_gu[0], w_expert_down[0], capacity
    )
    normed_part, grad_parts, ffn_own, gate_dots = rows_back(
        grad_all, normed_all, stats, shared_hid, shared_gate_by, shared_up_by, slots,
        expert_din, slice_gu, slice_down, ffn_part.reshape(devices, own_rows, model_width),
        parts.shape, capacity, gate_lane, levels, 9,
    )
    row_dots = jnp.sum(placed * slot_dots[:, 0].reshape(devices, capacity, 1), axis=1)
    dots = jnp.stack([row_dots, gate_dots[:, 0].reshape(devices, own_rows)], axis=1)
    dots = lax.all_to_all(dots, both, split_axis=0, concat_axis=0, tiled=True)
    grad_expert_gu, grad_expert_down = expert_weight_grads(
        received, expert_dgu, expert_hid, expert_dout
    )
    grad_normed_own = scatter_all(
        normed_part.reshape(devices, own_rows, model_width), levels, 4
    )

    grad_normed_own, grad_parts = lax.optimization_barrier((grad_normed_own, grad_parts))
    grad_parts = lax.all_to_all(grad_parts, EXPERT, 0, 0)

    stats_own = lax.dynamic_slice_in_dim(stats, me * own_rows, own_rows, 0)
    probs_own = stats_own[:, spare : spare + experts_all]
    sig_own = stats_own[:, gate_lane]
    grad_own = grad_out.astype(jnp.float32)
    grad_router_probs = dots[:, 0, :].T
    grad_logits = probs_own * (
        grad_router_probs - jnp.sum(probs_own * grad_router_probs, axis=-1, keepdims=True)
    )
    logits_low = grad_logits.astype(jnp.bfloat16)
    grad_router = mul(normed_own, logits_low, 0, 0)
    grad_gate_logit = jnp.sum(dots[:, 1, :], axis=0) * sig_own * (1.0 - sig_own)
    grad_gate_vec = jnp.sum(normed_own.astype(jnp.float32) * grad_gate_logit[:, None], axis=0)
    grad_normed_own = (
        grad_normed_own
        + mul(logits_low, w_router, 1, 1)
        + grad_gate_logit[:, None] * shared_gate[None, :]
    )
    grad_hidden_own = grad_own + norm_back(grad_normed_own, unit_two, scale_two, gain_ffn)
    grad_gain_two = jnp.sum(grad_normed_own * unit_two, axis=0)
    grad_hidden_low = gather_lanes(grad_hidden_own.astype(jnp.bfloat16), levels, lanes, 5)

    grad_mixed = mul(grad_hidden_low, full_out, 1, 1).astype(jnp.bfloat16)
    grad_bias_local, grad_qkv, normed_one_part = attention.back(grad_mixed)
    grad_wout = mul(attention.mixed, grad_hidden_low, 0, 0).astype(jnp.bfloat16)
    grad_normed_one = scatter_lanes(normed_one_part.astype(jnp.bfloat16), levels, lanes, 6)
    grad_tokens = grad_hidden_own + norm_back(grad_normed_one, unit_one, scale_one, gain_attn)
    grad_gain_one = jnp.sum(grad_normed_one * unit_one, axis=0)
    grad_bias_full = lax.dynamic_update_slice_in_dim(
        jnp.zeros((3, model_width), jnp.float32),
        grad_bias_local,
        lax.axis_index(SHARD) * local_width,
        1,
    )
    small = jnp.concatenate(
        [
            grad_router.reshape(-1, model_width),
            grad_gain_one[None],
            grad_gain_two[None],
            grad_gate_vec[None],
            grad_bias_full,
        ]
    )
    small_rows = small.shape[0]
    small = jnp.pad(small, ((0, -small_rows % 16), (0, 0))).reshape(2, -1, model_width)
    qkv_grad_part, wout_grad_part, small, shared_grad_in, shared_grad_down = scatter_last(
        grad_qkv, grad_wout, small, grad_parts, levels, 7
    )
    result = (hidden_own + ffn_own).astype(jnp.bfloat16)
    small = small.reshape(-1, model_width)[:small_rows]
    router_total = small[:-6].reshape(model_width, experts_all)
    gain_one_total, gain_two_total, gate_total = small[-6], small[-5], small[-4]
    bias_total = small[-3:]

    return (
        result,
        grad_tokens,
        gain_one_total,
        qkv_grad_part,
        bias_total,
        wout_grad_part,
        gain_two_total,
        router_total,
        gate_total,
        shared_grad_in,
        shared_grad_down,
        grad_expert_gu[None],
        grad_expert_down[None],
    )


def local_wide(
    tokens,
    gain_attn,
    w_qkv,
    b_qkv,
    w_out,
    gain_ffn,
    w_router,
    shared_gate,
    w_shared_gu,
    w_shared_down,
    w_expert_gu,
    w_expert_down,
    routes,
    grad_out,
):
    own_rows, model_width = tokens.shape
    shard_pos = lax.axis_index(SHARD)
    local_width = w_qkv.shape[2]
    experts_all = w_router.shape[1]
    capacity = 2 * own_rows * TOPK // experts_all
    first_own = shard_pos * own_rows

    def route_rows(block):
        block = block.reshape(experts_all, capacity, model_width)
        block = lax.all_to_all(block, both, split_axis=0, concat_axis=0, tiled=True)
        return block.reshape(-1, model_width)

    def group_rows(rows):
        return lax.all_gather(rows, SHARD, axis=0, tiled=True)

    def own(values):
        return lax.dynamic_slice_in_dim(values, first_own, own_rows, 0)

    full_qkv, full_out, full_sgu, full_sdown = (
        lax.all_gather(w_qkv, EXPERT, axis=1, tiled=True),
        lax.all_gather(w_out, EXPERT, axis=1, tiled=True),
        lax.all_gather(w_shared_gu, EXPERT, axis=1, tiled=True),
        lax.all_gather(w_shared_down, EXPERT, axis=1, tiled=True),
    )
    x_own = tokens.astype(jnp.float32)
    unit_one, scale_one = norm_rows(x_own)
    normed_one = (unit_one * gain_attn).astype(jnp.bfloat16)
    x_group, normed_group = group_rows(tokens), group_rows(normed_one)
    attention = Attention(normed_group, full_qkv, b_qkv)
    attn_group = lax.psum(mul(attention.mixed, full_out, 1, 0), SHARD)
    hidden_group = x_group.astype(jnp.float32) + attn_group
    unit_two, scale_two = norm_rows(hidden_group)
    normed_two = (unit_two * gain_ffn).astype(jnp.bfloat16)
    gate_logit = jnp.dot(normed_two.astype(jnp.float32), shared_gate, precision=highest)
    gate_sig = jax.nn.sigmoid(gate_logit)
    shared_gu = pair_mul(normed_two, full_sgu)
    shared_silu, shared_sig = silu_pair(shared_gu)
    shared_hid = (shared_silu * shared_gu[1]).astype(jnp.bfloat16)
    shared_part = mul(shared_hid, full_sdown, 1, 0)
    shared_own = lax.psum_scatter(
        shared_part.astype(jnp.bfloat16), SHARD, scatter_dimension=0, tiled=True
    ).astype(jnp.float32)
    normed_own, sig_own, hidden_own = own(normed_two), own(gate_sig), own(hidden_group)
    router_exp = jnp.exp(mul(normed_own, w_router, 1, 0))
    router_probs = router_exp / jnp.sum(router_exp, axis=-1, keepdims=True)
    expert_ids = jnp.arange(experts_all, dtype=jnp.int32)
    route_hits = (routes[:, :, None] == expert_ids[None, None, :]).astype(jnp.float32)
    picked = jnp.sum(router_probs[:, None, :] * route_hits, axis=-1)
    flat_routes = routes.reshape(-1)
    matches = (flat_routes[:, None] == expert_ids[None, :]).astype(jnp.int32)
    ranks = jnp.sum((jnp.cumsum(matches, axis=0) - 1) * matches, axis=1)
    targets = flat_routes * capacity + ranks

    def in_slots(rows):
        empty = jnp.zeros((experts_all * capacity, model_width), jnp.bfloat16)
        return empty.at[targets].set(rows)

    def at_slots(rows):
        return rows[targets].reshape(own_rows, TOPK, model_width).astype(jnp.float32)

    received = route_rows(in_slots(jnp.repeat(normed_own, TOPK, axis=0)))
    expert_gu = pair_mul(received, w_expert_gu[0])
    expert_silu, expert_sig = silu_pair(expert_gu)
    expert_hid = (expert_silu * expert_gu[1]).astype(jnp.bfloat16)
    expert_out = mul(expert_hid, w_expert_down[0], 1, 0).astype(jnp.bfloat16)
    route_out = at_slots(route_rows(expert_out))
    routed_own = jnp.sum(route_out * picked[:, :, None], axis=1)
    result = (hidden_own + sig_own[:, None] * shared_own + routed_own).astype(jnp.bfloat16)
    grad_own = grad_out.astype(jnp.float32)
    route_grad = (
        (picked[:, :, None] * grad_own[:, None, :]).reshape(-1, model_width).astype(jnp.bfloat16)
    )
    grad_recv = route_rows(in_slots(route_grad))
    grad_expert_down = mul(expert_hid, grad_recv, 0, 0)
    grad_expert_hid = mul(grad_recv, w_expert_down[0], 1, 1)
    expert_dgu = swiglu_back(grad_expert_hid, expert_gu)
    grad_expert_gu = jnp.stack([mul(received, grad, 0, 0) for grad in expert_dgu])
    expert_din = sum(mul(g, w, 1, 1) for g, w in zip(expert_dgu, w_expert_gu[0]))
    grad_normed_own = jnp.sum(at_slots(route_rows(expert_din.astype(jnp.bfloat16))), axis=1)
    grad_picked = jnp.sum(route_out * grad_own[:, None, :], axis=-1)
    grad_router_probs = jnp.sum(grad_picked[:, :, None] * route_hits, axis=1)
    grad_logits = router_probs * (
        grad_router_probs - jnp.sum(router_probs * grad_router_probs, axis=-1, keepdims=True)
    )
    logits_low = grad_logits.astype(jnp.bfloat16)
    grad_router = mul(normed_own, logits_low, 0, 0)
    grad_normed_own = grad_normed_own + mul(logits_low, w_router, 1, 1)
    grad_gate_logit = jnp.sum(grad_own * shared_own, axis=-1) * sig_own * (1.0 - sig_own)
    grad_gate_vec = jnp.dot(
        grad_gate_logit, normed_own.astype(jnp.float32), precision=highest
    )
    grad_normed_own = grad_normed_own + grad_gate_logit[:, None] * shared_gate[None, :]
    grad_group_f = group_rows(grad_out).astype(jnp.float32)
    grad_shared_out = (gate_sig[:, None] * grad_group_f).astype(jnp.bfloat16)
    grad_sdown = mul(shared_hid, grad_shared_out, 0, 0)
    grad_shared_hid = mul(grad_shared_out, full_sdown, 1, 1)
    shared_dgu = swiglu_back(grad_shared_hid, shared_gu)
    grad_sgu = jnp.stack([mul(normed_two, grad, 0, 0) for grad in shared_dgu])
    normed_part = sum(mul(g, w, 1, 1) for g, w in zip(shared_dgu, full_sgu))
    normed_part = lax.dynamic_update_slice_in_dim(
        normed_part, own(normed_part) + grad_normed_own, first_own, 0
    )
    grad_normed_two = lax.psum(normed_part, SHARD)
    grad_hidden = grad_group_f + norm_back(grad_normed_two, unit_two, scale_two, gain_ffn)
    grad_gain_two = jnp.sum(own(grad_normed_two * unit_two), axis=0)
    grad_hidden_low = grad_hidden.astype(jnp.bfloat16)
    grad_wout = mul(attention.mixed, grad_hidden_low, 0, 0)
    grad_mixed = mul(grad_hidden_low, full_out, 1, 1).astype(jnp.bfloat16)
    grad_bias_local, grad_qkv, normed_one_part = attention.back(grad_mixed)
    grad_normed_one = lax.psum_scatter(
        normed_one_part.astype(jnp.bfloat16), SHARD, scatter_dimension=0, tiled=True
    ).astype(jnp.float32)
    grad_tokens = own(grad_hidden) + norm_back(grad_normed_one, unit_one, scale_one, gain_attn)
    grad_gain_one = jnp.sum(grad_normed_one * unit_one, axis=0)
    grad_bias_full = lax.dynamic_update_slice_in_dim(
        jnp.zeros((3, model_width), jnp.float32), grad_bias_local, shard_pos * local_width, 1
    )

    def weight_sum(grad):
        low = grad.astype(jnp.bfloat16)
        total = lax.psum_scatter(low, EXPERT, scatter_dimension=1, tiled=True)
        return total.astype(jnp.float32)

    router_total, gain_one_total, gain_two_total, gate_total, bias_total = lax.psum(
        (grad_router, grad_gain_one, grad_gain_two, grad_gate_vec, grad_bias_full), both
    )
    return (
        result,
        grad_tokens,
        gain_one_total,
        weight_sum(grad_qkv),
        bias_total,
        weight_sum(grad_wout),
        gain_two_total,
        router_total,
        gate_total,
        weight_sum(grad_sgu),
        weight_sum(grad_sdown),
        grad_expert_gu[None],
        grad_expert_down[None],
    )


def local_by_size(*args):
    spots, lanes = lax.axis_size(EXPERT), lax.axis_size(SHARD)
    w_router, w_shared_down = args[6], args[9]
    units = w_shared_down.shape[0] // spots
    side = units - SIDE + w_router.shape[1] + 3
    fits = lanes == 4 and spots % 2 == 0 and spots * lanes <= 64
    fits = fits and SIDE <= units <= PAIR and side <= PAIR - SIDE
    return local(*args) if fits else local_wide(*args)


def solution(mesh):
    rows, columns = P(both, None), P(None, EXPERT, SHARD)
    weights = P(both, None, None, None), P(both, None, None)
    return jax.shard_map(
        local_by_size,
        mesh=mesh,
        in_specs=(
            rows, P(), columns, P(None, SHARD), P(SHARD, EXPERT), P(), P(), P(),
            columns, P(SHARD, EXPERT), *weights, rows, rows,
        ),
        out_specs=(
            rows, rows, P(), columns, P(), P(SHARD, EXPERT), P(), P(), P(),
            columns, P(SHARD, EXPERT), *weights,
        ),
        check_vma=False,
    )
```
